32 devices in a mesh: gx: 8 (over z, x), gy: 4 (over y, core).
Axes of the slice: x: 2, y: 2, z: 4, core: 2. Of those that a mesh axis runs over, the one named last changes fastest.
Arguments:
- velocity: float32 [3, 128, 128, 256], P(None, 'gx', 'gy'), may hold values from -6 to 6
- owner_block: int32 [65536, 1], P(('gx', 'gy')), may hold values from 0 to 31, as said below
- base_x: int32 [65536], P(('gx', 'gy')), may hold values from 0 to 16
- base_y: int32 [65536], P(('gx', 'gy')), may hold values from 0 to 32
- base_z: int32 [65536], P(('gx', 'gy')), may hold values from 0 to 255
- delta_weights: float32 [12, 65536], P(None, ('gx', 'gy')), may hold values from 0.1 to 1
- marker_offset: float32 [3, 65536], P(None, ('gx', 'gy')), may hold values from -4 to 4
- sphere_motion: float32 [6, 64], P(None, ('gx', 'gy')), may hold values from -6 to 6
- contact_sphere: int32 [128], P(('gx', 'gy')), may hold values from 0 to 63, as said below
- contact_partner: int32 [128], P(('gx', 'gy')), may hold values from 0 to 63
Outputs:
- velocity_star: float32 [3, 128, 128, 256], P(None, 'gx', 'gy')
- new_motion: float32 [6, 64], P(None, ('gx', 'gy'))
The draws below stay inside these ranges and needn't reach their ends.
Inputs may be any that keep to these rules, and one draw needn't show every extreme that they name: `owner_block`: block b stands at gx index b // 4 and gy index b % 4. Each marker's owner block is the block of the device that holds the marker or one of the eight blocks beside it (periodic along gx, none beyond the walls along gy). Among the markers of one device, at most 256 have any one owner block other than that device's own, and in every device exactly 256 have one such block. `contact_sphere`: entry k names one of the 2 spheres k // 4 * 2 and after, those of the device that holds entry k.
All inputs are finite; a program needn't handle non-finite values.
Results may differ from the reference program's by a relative error of at most 0.0003.
Values sent between devices are 32-bit elements; how exact they have to be, the bound alone decides.
A program may use at most 64 MiB of HBM per device.

```python
import math
import jax
import jax.numpy as jnp
from jax import lax

CX = 16
CY = 32
NZ = 256
MK = 1024
S_DEV = 2
CT_DEV = 4
ITERS = 4
NX = 128
NY = 128
SPHERES = 64
MARKERS = 65536
CAP = 256
CONTACTS = 128
N_GX = 8
N_GY = 4


def draw_contact_sphere(key, part):
    entries = jnp.arange(CONTACTS, dtype=jnp.int32)
    picked = jax.random.randint(key, (CONTACTS,), 0, S_DEV, dtype=jnp.int32)
    return entries // CT_DEV * S_DEV + picked


def draw_owner_block(key, part):
    per_device = S_DEV * MK
    devices = N_GX * N_GY
    device = jnp.arange(devices, dtype=jnp.int32)
    column = device // N_GY
    row = device % N_GY
    shift_x = jnp.array([-1, -1, -1, 0, 0, 1, 1, 1], dtype=jnp.int32)
    shift_y = jnp.array([-1, 0, 1, -1, 1, -1, 0, 1], dtype=jnp.int32)
    counts = jax.random.randint(jax.random.fold_in(key, 11), (devices, 8), 1, CAP + 1, dtype=jnp.int32)
    coin = jax.random.randint(jax.random.fold_in(key, 12), (devices,), 0, 2, dtype=jnp.int32)
    full_lane = jnp.where(coin == 0, 1, 6).astype(jnp.int32)
    counts = jnp.where(jnp.arange(8, dtype=jnp.int32)[None, :] == full_lane[:, None], CAP, counts)
    device_keys = jax.random.split(jax.random.fold_in(key, 13), devices)
    position = jax.vmap(lambda one_key: jax.random.permutation(one_key, per_device))(device_keys).astype(jnp.int32)
    lane = jnp.minimum(position // CAP, 7)
    within = position % CAP
    count_here = jnp.take_along_axis(counts, lane, axis=1)
    away = within < count_here
    towards_x = (column[:, None] + shift_x[lane]) % N_GX
    towards_y = row[:, None] + shift_y[lane]
    inside = jnp.logical_and(towards_y >= 0, towards_y < N_GY)
    chosen = jnp.where(jnp.logical_and(away, inside), towards_x * N_GY + towards_y, device[:, None])
    return chosen.reshape(MARKERS, 1).astype(jnp.int32)


def plant(values, stream_key, low, largest):
    shape = values.shape
    index_at = [jax.random.randint(jax.random.fold_in(stream_key, axis), (), 0, shape[axis]) for axis in range(len(shape))]
    values = values.at[tuple(index_at)].set(low)
    longest = shape.index(max(shape))
    index_at[longest] = (index_at[longest] + 1) % shape[longest]
    return values.at[tuple(index_at)].set(largest)


def block_levels(key, extent, shards, smallest, high):
    gain = 1.0
    for axis_at, shards_of in shards:
        heights = jax.random.uniform(jax.random.fold_in(jax.random.fold_in(key, 6), axis_at), (shards_of,), jnp.float32, smallest / len(shards), high / len(shards))
        gain = gain * jnp.repeat(jnp.exp(heights), extent[axis_at] // shards_of).reshape((-1,) + (1,) * (len(extent) - 1 - axis_at))
    return gain


def noise(rng, dims, scale, limit, cuts=(), held_as=jnp.bfloat16):
    level = block_levels(rng, dims, cuts, -0.22, 0.18) if cuts else 1.0
    result = jax.random.normal(rng, dims, jnp.float32) * scale * level
    return jnp.minimum(jnp.maximum(result, -limit), limit).astype(held_as)


def setup_inputs(seed: int = 0) -> dict:
    seeds = jax.random.split(jax.random.key(seed), 11)
    return {
        "velocity": noise(seeds[0], (3, NX, NY, NZ), 1.0, 6.0, ((1, 8), (2, 4)), jnp.float32),
        "owner_block": draw_owner_block(jax.random.fold_in(seeds[10], 71), 0),
        "base_x": plant(jax.random.randint(seeds[2], (MARKERS,), 0, CX + 1), jax.random.fold_in(seeds[2], 1), 0, CX).astype(jnp.int32),
        "base_y": plant(jax.random.randint(seeds[3], (MARKERS,), 0, CY + 1), jax.random.fold_in(seeds[3], 1), 0, CY).astype(jnp.int32),
        "base_z": plant(jax.random.randint(seeds[4], (MARKERS,), 0, NZ), jax.random.fold_in(seeds[4], 1), 0, NZ - 1).astype(jnp.int32),
        "delta_weights": jnp.clip(jnp.exp(math.log(1.0) - 2.3025851 * jax.random.uniform(seeds[5], (12, MARKERS), jnp.float32) ** block_levels(seeds[5], (12, MARKERS), ((1, 32),), -0.2, 0.2)), 0.1, 1.0),
        "marker_offset": noise(seeds[6], (3, MARKERS), 1.0, 4.0, ((1, 32),), jnp.float32),
        "sphere_motion": noise(seeds[7], (6, SPHERES), 1.0, 6.0, ((1, 32),), jnp.float32),
        "contact_sphere": draw_contact_sphere(jax.random.fold_in(seeds[10], 71), 0),
        "contact_partner": plant(jax.random.randint(seeds[9], (CONTACTS,), 0, SPHERES), jax.random.fold_in(seeds[9], 1), 0, SPHERES - 1).astype(jnp.int32),
    }


DIFFUSION = 1.0
RESPONSE = 0.5
DASHPOT = 0.1


def support(start_x, start_y, start_z, weights, stride_y, extent_z):
    offsets = jnp.arange(4, dtype=jnp.int32)
    cells_x = start_x[None, :] + offsets[:, None]
    cells_y = start_y[None, :] + offsets[:, None]
    cells_z = (start_z[None, :] + offsets[:, None]) % extent_z
    where = ((cells_x[:, None, None, :] * stride_y + cells_y[None, :, None, :]) * extent_z + cells_z[None, None, :, :]).reshape(64, -1)
    product = (weights[0:4][:, None, None, :] * weights[4:8][None, :, None, :] * weights[8:12][None, None, :, :]).reshape(64, -1)
    return where, product


def reference(velocity, owner_block, base_x, base_y, base_z, delta_weights, marker_offset, sphere_motion, contact_sphere, contact_partner):
    padded = jnp.pad(velocity, ((0, 0), (2, 2), (0, 0), (0, 0)), mode="wrap")
    padded = jnp.pad(padded, ((0, 0), (0, 0), (2, 2), (0, 0)))
    flat_field = padded.reshape(3, -1)
    owner = owner_block[:, 0]
    start_x = (owner // N_GY) * CX + base_x
    start_y = (owner % N_GY) * CY + base_y
    linear = sphere_motion[0:3]
    angular = sphere_motion[3:6]
    marker_linear = jnp.repeat(linear, MK, axis=1)
    marker_angular = jnp.repeat(angular, MK, axis=1)
    target = marker_linear + jnp.cross(marker_angular, marker_offset, axis=0)
    block_x = start_x.reshape(SPHERES, MK)
    block_y = start_y.reshape(SPHERES, MK)
    block_z = base_z.reshape(SPHERES, MK)
    block_w = delta_weights.reshape(12, SPHERES, MK).transpose(1, 0, 2)
    block_t = target.reshape(3, SPHERES, MK).transpose(1, 0, 2)

    def sample(item):
        where, product = support(item[0], item[1], item[2], item[3], NY + 4, NZ)
        picked = flat_field[:, where]
        return jnp.sum(picked * product[None], axis=1)

    sampled = lax.map(sample, (block_x, block_y, block_z, block_w))
    block_force = block_t - sampled
    force = block_force.transpose(1, 0, 2).reshape(3, MARKERS)
    push = jnp.sum(block_force, axis=-1).T / MK
    twist = jnp.sum(jnp.cross(marker_offset, force, axis=0).reshape(3, SPHERES, MK), axis=-1) / MK
    moved = linear - RESPONSE * push
    turned = angular - RESPONSE * twist
    spring = moved[:, contact_partner] - moved[:, contact_sphere]
    settled = moved + DASHPOT * jax.ops.segment_sum(spring.T, contact_sphere, SPHERES).T
    new_motion = jnp.concatenate([settled, turned], axis=0)

    def deposit(field, item):
        where, product = support(item[0], item[1], item[2], item[3], NY + 4, NZ)
        return field.at[:, where.reshape(-1)].add((product[None] * item[4][:, None, :]).reshape(3, -1)), None

    spread, unused = lax.scan(deposit, jnp.zeros_like(flat_field), (block_x, block_y, block_z, block_w, block_force))
    spread = spread.reshape(padded.shape)
    folded = spread[:, 2:NX + 2]
    folded = folded.at[:, 0:2].add(spread[:, NX + 2:NX + 4])
    folded = folded.at[:, NX - 2:NX].add(spread[:, 0:2])
    source = folded[:, :, 2:NY + 2]
    rhs = velocity + source
    state = rhs
    for sweep in range(ITERS):
        walled = jnp.pad(state, ((0, 0), (0, 0), (1, 1), (0, 0)))
        beside_all = jnp.roll(state, -1, 1) + jnp.roll(state, 1, 1) + walled[:, :, 2:] + walled[:, :, :-2]
        beside_all = beside_all + jnp.roll(state, -1, 3) + jnp.roll(state, 1, 3)
        state = (rhs + DIFFUSION * beside_all) / (1.0 + 6.0 * DIFFUSION)
    return state, new_motion
```

```python
import functools

import jax
import jax.numpy as jnp
import numpy as np
from jax import lax
from jax.experimental import pallas as pl
from jax.experimental.pallas import tpu as pltpu
from jax.sharding import PartitionSpec as P

ITERS = 4
DIFFUSION = 1.0
RESPONSE = 0.5
DASHPOT = 0.1

MESH = pl.DeviceIdType.MESH
TILE_ROWS = 16
TILE_LANES = 128
CHUNK = 256
WINDOW = 8
GROUP = 6
RECORD = 24
X_ROW, Y_ROW, Z_ROW, TARGET, OFFSET, SPHERE, LIVE = 12, 13, 14, 15, 18, 21, 22
DIRECTIONS = ((-1, -1), (-1, 0), (-1, 1), (0, -1), (0, 1), (1, -1), (1, 0), (1, 1))
HALO = 2
RIM = 8


def when(condition, body):
    if condition is True:
        body()
    else:
        pl.when(condition)(body)


def exists(row, rows, dy):
    if dy == 0:
        return True
    return row + dy < rows if dy > 0 else row + dy >= 0


def greet(columns, rows, column, row):
    barrier = pltpu.get_barrier_semaphore()
    for dx, dy in DIRECTIONS:
        peer = (lax.rem(column + dx + columns, columns), row + dy)
        when(
            exists(row, rows, dy),
            lambda peer=peer: pl.semaphore_signal(
                barrier, inc=1, device_id=peer, device_id_type=MESH
            ),
        )
    return barrier


def greeted(rows, row):
    inner = lax.min(row, 1) + lax.min(rows - 1 - row, 1)
    return 2 + 3 * inner


def remote(src, dst, send, recv, k, peer):
    return pltpu.make_async_remote_copy(
        src_ref=src,
        dst_ref=dst,
        send_sem=send.at[k],
        recv_sem=recv.at[k],
        device_id=peer,
        device_id_type=MESH,
    )


def split(value):
    high = value.astype(jnp.bfloat16).astype(jnp.float32)
    return high, value - high


def upper_triangle():
    rows = lax.broadcasted_iota(jnp.int32, (CHUNK, CHUNK), 0)
    lanes = lax.broadcasted_iota(jnp.int32, (CHUNK, CHUNK), 1)
    return (rows <= lanes).astype(jnp.float32).astype(jnp.bfloat16)


def ranks(categories, count):
    rows = lax.broadcasted_iota(jnp.int32, (count, CHUNK), 0).astype(jnp.float32)
    hot = [(rows == block).astype(jnp.float32) for block in categories]
    stacked = jnp.concatenate(hot, axis=0).astype(jnp.bfloat16)
    inside = jnp.dot(stacked, upper_triangle(), preferred_element_type=jnp.float32)
    carry = jnp.zeros((count, 1), jnp.float32)
    upto = []
    for b in range(len(hot)):
        block = inside[b * count : (b + 1) * count]
        upto.append(block + carry)
        carry = carry + block[:, CHUNK - 1 : CHUNK]
    return hot, upto, carry


def place(parts, where_to, groups):
    group = jnp.floor(where_to * (1.0 / CHUNK))
    slot = where_to - group * CHUNK
    rows = lax.broadcasted_iota(jnp.int32, (CHUNK, where_to.shape[1]), 0).astype(jnp.float32)
    hot = (rows == slot).astype(jnp.float32).astype(jnp.bfloat16)
    masked = [parts * (group == g).astype(jnp.float32) for g in groups]
    masked = jnp.concatenate(masked, axis=0).astype(jnp.bfloat16)
    moved = lax.dot_general(
        masked, hot, (((1,), (1,)), ((), ())), preferred_element_type=jnp.float32
    )
    result = []
    for n in range(len(groups)):
        piece = moved[2 * RECORD * n : 2 * RECORD * (n + 1)]
        result.append(piece[:RECORD] + piece[RECORD:])
    return result


def front_kernel(
    columns, rows, ids, weights, offsets, motion, velocity,
    home, arrived, left, right, below, above, corners, slots, send, recv,
):
    column = lax.axis_index("gx")
    row = lax.axis_index("gy")
    span_x, span_y = velocity.shape[1], velocity.shape[2]
    barrier = greet(columns, rows, column, row)

    def peer(dx, dy):
        return (lax.rem(column + dx + columns, columns), row + dy)

    edge = [
        (velocity.at[:, 0:HALO], right, -1, 0),
        (velocity.at[:, span_x - HALO : span_x], left, 1, 0),
        (velocity.at[:, :, 0:RIM], above, 0, -1),
        (velocity.at[:, :, span_y - RIM : span_y], below, 0, 1),
    ]
    for side, halo in enumerate((left, right)):
        edge.append((halo.at[:, :, 0:RIM], corners.at[2 + side], 0, -1))
        edge.append((halo.at[:, :, span_y - RIM : span_y], corners.at[side], 0, 1))
    for g, (dx, dy) in enumerate(DIRECTIONS):
        edge.append((slots.at[g], arrived.at[g], dx, dy))

    def start(k):
        src, dst, dx, dy = edge[k]
        when(
            exists(row, rows, dy),
            lambda: remote(src, dst, send, recv, k, peer(dx, dy)).start(),
        )

    def arrive(k):
        src, dst, dx, dy = edge[k]
        when(
            exists(row, rows, -dy),
            lambda: remote(src, dst, send, recv, k, peer(dx, dy)).wait_recv(),
        )

    def sent(k):
        src, dst, dx, dy = edge[k]
        when(
            exists(row, rows, dy),
            lambda: remote(src, dst, send, recv, k, peer(dx, dy)).wait_send(),
        )

    @pl.when(row == 0)
    def _():
        below[...] = jnp.zeros(below.shape, jnp.float32)
        for n in (0, 1):
            corners[n] = jnp.zeros(corners.shape[1:], jnp.float32)
        for g, (dx, dy) in enumerate(DIRECTIONS):
            if dy > 0:
                arrived[g] = jnp.zeros(arrived.shape[1:], jnp.float32)

    @pl.when(row == rows - 1)
    def _():
        above[...] = jnp.zeros(above.shape, jnp.float32)
        for n in (2, 3):
            corners[n] = jnp.zeros(corners.shape[1:], jnp.float32)
        for g, (dx, dy) in enumerate(DIRECTIONS):
            if dy < 0:
                arrived[g] = jnp.zeros(arrived.shape[1:], jnp.float32)

    pl.semaphore_wait(barrier, greeted(rows, row))
    for k in range(4):
        start(k)

    markers = ids.shape[1]
    spheres = motion.shape[1]
    per_sphere = markers // spheres
    owner = ids[0:1]
    owner_x = jnp.floor((owner + 0.5) * (1.0 / rows))
    owner_y = owner - owner_x * rows
    step_x = owner_x - column.astype(jnp.float32)
    step_x = jnp.where(step_x > 1.5, step_x - columns, step_x)
    step_x = jnp.where(step_x < -1.5, step_x + columns, step_x)
    step_y = owner_y - row.astype(jnp.float32)
    lane = (step_x + 1.0) * 3.0 + step_y + 1.0
    at_home = lane == 4.0
    lane = jnp.where(at_home, -1.0, jnp.where(lane > 4.0, lane - 1.0, lane))
    offset = offsets[...]
    targets = []
    for s in range(spheres):
        o = offset[:, s * per_sphere : (s + 1) * per_sphere]
        m = [motion[c : c + 1, s : s + 1] for c in range(6)]
        targets.append(
            jnp.concatenate(
                [
                    m[0] + (m[4] * o[2:3] - m[5] * o[1:2]),
                    m[1] + (m[5] * o[0:1] - m[3] * o[2:3]),
                    m[2] + (m[3] * o[1:2] - m[4] * o[0:1]),
                ],
                axis=0,
            )
        )
    home[0:12] = weights[...]
    home[X_ROW : Z_ROW + 1] = ids[1:4]
    home[TARGET : TARGET + 3] = jnp.concatenate(targets, axis=1)
    home[OFFSET : OFFSET + 3] = offset
    position = lax.broadcasted_iota(jnp.int32, (1, markers), 1)
    sphere = jnp.zeros((1, markers), jnp.float32)
    for s in range(1, spheres):
        sphere = sphere + (position >= s * per_sphere).astype(jnp.float32)
    home[SPHERE : SPHERE + 1] = sphere
    home[LIVE : LIVE + 1] = jnp.ones((1, markers), jnp.float32)
    home[LIVE + 1 : LIVE + 2] = jnp.zeros((1, markers), jnp.float32)

    lanes = len(DIRECTIONS)
    blocks = markers // CHUNK
    hot, upto, totals = ranks([lane[:, b * CHUNK : (b + 1) * CHUNK] for b in range(blocks)], lanes)
    rank = [jnp.sum(h * (u - 1.0), axis=0, keepdims=True) for h, u in zip(hot, upto)]
    where_to = jnp.concatenate(rank, axis=1) + lane * CHUNK
    where_to = jnp.where(at_home, -1.0, where_to)
    parts = jnp.concatenate(split(home[...]), axis=0)
    for g, piece in enumerate(place(parts, where_to, range(lanes))):
        slots[g] = piece
    home[LIVE : LIVE + 1] = at_home.astype(jnp.float32)

    arrive(0)
    arrive(1)
    for k in range(8, 8 + lanes):
        start(k)
    for k in range(4, 8):
        start(k)
    for k in range(2, 8 + lanes):
        arrive(k)
    for k in range(8 + lanes):
        sent(k)


def front(ids, weights, offsets, motion, velocity):
    columns, rows = lax.axis_size("gx"), lax.axis_size("gy")
    span_x, span_y, extent_z = velocity.shape[1:]
    markers = ids.shape[1]
    lanes = len(DIRECTIONS)
    f32 = jnp.float32
    copies = 8 + lanes
    vmem = pl.BlockSpec(memory_space=pltpu.VMEM)
    out = [
        (RECORD, markers),
        (lanes, RECORD, CHUNK),
        (3, HALO, span_y, extent_z),
        (3, HALO, span_y, extent_z),
        (3, span_x, RIM, extent_z),
        (3, span_x, RIM, extent_z),
        (4, 3, HALO, RIM, extent_z),
    ]
    return pl.pallas_call(
        functools.partial(front_kernel, columns, rows),
        out_shape=[jax.ShapeDtypeStruct(shape, f32) for shape in out],
        in_specs=[vmem] * 5,
        out_specs=[vmem] * len(out),
        scratch_shapes=[
            pltpu.VMEM((lanes, RECORD, CHUNK), f32),
            pltpu.SemaphoreType.DMA((copies,)),
            pltpu.SemaphoreType.DMA((copies,)),
        ],
        compiler_params=pltpu.CompilerParams(collective_id=0, has_side_effects=True),
        name="front",
    )(ids, weights, offsets, motion, velocity)


def four(distance, weights):
    value = jnp.where(distance == 3.0, weights[3:4], 0.0)
    for n in (2, 1, 0):
        value = jnp.where(distance == float(n), weights[n : n + 1], value)
    return value


def markers_kernel(
    spheres, velocity, left, right, below, above, corners, home, arrived, motion,
    spread, tile, high, low, sorted_refs, parts, sums,
):
    span_x, span_y, extent_z = velocity.shape[1:]
    wide_y = span_y + 2 * ITERS
    lanes = len(DIRECTIONS)
    bf16, f32 = jnp.bfloat16, jnp.float32
    layers = span_x + 2 * HALO

    def layer(x, row_source, below_source, above_source, own):
        for c in range(3):
            rows = row_source(c)
            edge = jnp.zeros((HALO, extent_z), f32)
            value = jnp.concatenate(
                [
                    edge,
                    below_source(c)[RIM - HALO : RIM],
                    rows,
                    above_source(c)[0:HALO],
                    edge,
                ],
                axis=0,
            )
            at = slice(wide_y * c, wide_y * (c + 1))
            first, rest = split(value)
            high[x, at] = first.astype(bf16)
            low[x, at] = rest.astype(bf16)
            if own:
                wide = jnp.zeros((ITERS, extent_z), f32)
                spread[x + HALO, at] = jnp.concatenate([wide, rows, wide], axis=0)
        end = jnp.zeros((high.shape[1] - 3 * wide_y, extent_z), bf16)
        high[x, 3 * wide_y :] = end
        low[x, 3 * wide_y :] = end

    def inner(x, carry):
        layer(
            x + HALO,
            lambda c: velocity[c, x],
            lambda c: below[c, x],
            lambda c: above[c, x],
            True,
        )
        return carry

    lax.fori_loop(0, span_x, inner, 0)
    for side, halo in enumerate((left, right)):
        for x in range(HALO):
            layer(
                x + side * (span_x + HALO),
                lambda c: halo[c, x],
                lambda c: corners[side, c, x],
                lambda c: corners[2 + side, c, x],
                False,
            )
    for x in range(ITERS):
        spread[x] = jnp.zeros(spread.shape[1:], f32)
        spread[span_x + ITERS + x] = jnp.zeros(spread.shape[1:], f32)

    markers = home.shape[1]
    blocks = markers // CHUNK
    total = blocks + lanes
    count = -(-(span_x + 1) // 8) * 8
    categories = []
    live = []
    for b in range(total):
        at = slice(b * CHUNK, (b + 1) * CHUNK)
        if b < blocks:
            record = home[:, at]
            group = lanes * spheres + record[SPHERE : SPHERE + 1]
        else:
            record = arrived[b - blocks]
            group = (b - blocks) * spheres + record[SPHERE : SPHERE + 1]
        alive = record[LIVE : LIVE + 1] > 0.5
        live.append(alive)
        categories.append(jnp.where(alive, record[X_ROW : X_ROW + 1], -1.0))
        first, rest = split(record)
        parts[0:RECORD, at] = first
        parts[RECORD : 2 * RECORD, at] = rest
        parts[SPHERE : SPHERE + 1, at] = group
    hot, upto, totals = ranks(categories, count)
    lower_rows = lax.broadcasted_iota(jnp.int32, (count, count), 0)
    lower_lanes = lax.broadcasted_iota(jnp.int32, (count, count), 1)
    before = (lower_lanes < lower_rows).astype(f32)
    starts = jnp.dot(
        before,
        jnp.broadcast_to(totals, (count, TILE_LANES)),
        precision=lax.Precision.HIGHEST,
        preferred_element_type=f32,
    )[:, 0:1]
    places = []
    for b in range(total):
        rank = jnp.sum(hot[b] * (upto[b] + (starts - 1.0)), axis=0, keepdims=True)
        places.append(jnp.where(live[b], rank, -1.0))
    where_to = jnp.concatenate(places, axis=1)
    alive_count = jnp.sum(totals).astype(jnp.int32)
    for first in range(0, total, GROUP):
        groups = range(first, min(first + GROUP, total))

        @pl.when(alive_count > first * CHUNK)
        def _(groups=groups):
            for g, piece in zip(groups, place(parts[...], where_to, groups)):
                sorted_refs[g] = piece

    sums[...] = jnp.zeros(sums.shape, f32)
    z_cells = lax.broadcasted_iota(jnp.int32, (extent_z, CHUNK), 0).astype(f32)
    y_cells = lax.broadcasted_iota(jnp.int32, (wide_y, CHUNK), 0).astype(f32) - HALO
    x_cells = lax.broadcasted_iota(jnp.int32, (WINDOW, CHUNK), 0).astype(f32)

    def chunk(j, carry):
        record = sorted_refs[j]
        alive = record[LIVE : LIVE + 1]
        cell_x = record[X_ROW : X_ROW + 1]
        distance = z_cells - record[Z_ROW : Z_ROW + 1]
        distance = jnp.where(distance < 0.0, distance + extent_z, distance)
        z_high, z_low = split(four(distance, record[8:12]))
        z_high = z_high.astype(bf16)
        z_low = z_low.astype(bf16)
        y_table = four(y_cells - record[Y_ROW : Y_ROW + 1], record[4:8])
        least = jnp.min(jnp.where(alive > 0.5, cell_x, 1e4)).astype(jnp.int32)
        most = jnp.max(jnp.where(alive > 0.5, cell_x, -1.0)).astype(jnp.int32)
        windows = (most + 4 - least + WINDOW - 1) // WINDOW

        def x_table(k):
            fresh = least + WINDOW * k
            base = jnp.minimum(fresh, layers - WINDOW)
            cells = x_cells + base.astype(f32)
            table = four(cells - cell_x, record[0:4])
            return base, jnp.where(cells >= fresh.astype(f32), table, 0.0)

        z_stack = jnp.concatenate([z_high, z_high, z_low], axis=0)

        def sample(k, total):
            base, table = x_table(k)
            rows = high.shape[1]
            first = high[pl.ds(base, WINDOW)].reshape(WINDOW * rows, extent_z)
            rest = low[pl.ds(base, WINDOW)].reshape(WINDOW * rows, extent_z)
            lines = jnp.dot(
                jnp.concatenate([first, rest, first], axis=1),
                z_stack,
                preferred_element_type=f32,
            )
            for x in range(WINDOW):
                total = total + lines[x * rows : x * rows + 3 * wide_y] * table[x : x + 1]
            return total

        plane = lax.fori_loop(0, windows, sample, jnp.zeros((3 * wide_y, CHUNK), f32))
        forces = []
        for c in range(3):
            got = jnp.sum(plane[c * wide_y : (c + 1) * wide_y] * y_table, axis=0, keepdims=True)
            forces.append((record[TARGET + c : TARGET + c + 1] - got) * alive)
        sheet = jnp.concatenate([force * y_table for force in forces], axis=0)
        z_wide = jnp.concatenate([z_high, z_high, z_low], axis=1)

        def deposit(k, carry):
            base, table = x_table(k)
            value = jnp.concatenate([sheet * table[x : x + 1] for x in range(WINDOW)], axis=0)
            first, rest = split(value)
            first = first.astype(bf16)
            rest = rest.astype(bf16)
            added = lax.dot_general(
                jnp.concatenate([first, rest, first], axis=1),
                z_wide,
                (((1,), (1,)), ((), ())),
                preferred_element_type=f32,
            )
            at = pl.ds(base + HALO, WINDOW)
            spread[at] = spread[at] + added.reshape(WINDOW, 3 * wide_y, extent_z)
            return carry

        lax.fori_loop(0, windows, deposit, 0)
        o = [record[OFFSET + c : OFFSET + c + 1] for c in range(3)]
        f = forces
        moments = jnp.concatenate(
            f
            + [
                o[1] * f[2] - o[2] * f[1],
                o[2] * f[0] - o[0] * f[2],
                o[0] * f[1] - o[1] * f[0],
                jnp.zeros((2, CHUNK), f32),
            ],
            axis=0,
        )
        group = record[SPHERE : SPHERE + 1]
        for g in range((lanes + 1) * spheres):
            sums[g] = sums[g] + jnp.where(group == float(g), moments, 0.0)
        return carry

    chunks = (alive_count + (CHUNK - 1)) // CHUNK
    lax.fori_loop(0, chunks, chunk, 0)
    tile[...] = jnp.sum(sums[...], axis=2)


def markers_stage(spheres, velocity, halos, home, arrived, motion):
    span_x, span_y, extent_z = velocity.shape[1:]
    wide_y = span_y + 2 * ITERS
    lanes = len(DIRECTIONS)
    f32 = jnp.float32
    total = home.shape[1] // CHUNK + lanes
    groups = (lanes + 1) * spheres
    field_rows = -(-3 * wide_y // 16) * 16
    field = (span_x + 2 * HALO, field_rows, extent_z)
    vmem = pl.BlockSpec(memory_space=pltpu.VMEM)
    return pl.pallas_call(
        functools.partial(markers_kernel, spheres),
        out_shape=[
            jax.ShapeDtypeStruct((span_x + 2 * ITERS, 3 * wide_y, extent_z), f32),
            jax.ShapeDtypeStruct((groups, 8), f32),
        ],
        in_specs=[vmem] * 9,
        out_specs=[vmem] * 2,
        scratch_shapes=[
            pltpu.VMEM(field, jnp.bfloat16),
            pltpu.VMEM(field, jnp.bfloat16),
            pltpu.VMEM((total, RECORD, CHUNK), f32),
            pltpu.VMEM((2 * RECORD, total * CHUNK), f32),
            pltpu.VMEM((groups, 8, CHUNK), f32),
        ],
        compiler_params=pltpu.CompilerParams(vmem_limit_bytes=56 * 2**20),
        name="markers",
    )(velocity, *halos, home, arrived, motion)


def combine_matrix(columns, rows, per_sphere):
    matrix = np.zeros((columns, rows, columns, rows, TILE_ROWS), np.float32)
    for i in range(columns):
        for j in range(rows):
            for slot, (dx, dy) in enumerate(DIRECTIONS):
                if 0 <= j - dy < rows:
                    matrix[(i - dx) % columns, j - dy, i, j, slot] -= RESPONSE / per_sphere
            matrix[i, j, i, j, len(DIRECTIONS)] -= RESPONSE / per_sphere
            matrix[i, j, i, j, len(DIRECTIONS) + 1] = 1.0
    return matrix.reshape(columns * rows, -1)


def tail_kernel(
    columns, rows, spread, tile, matrix, links,
    out, motion_out, from_left, from_right, from_below, from_above, corners, held,
    rhs, one, two, mask_ref, own_sem, send, recv, row_send, row_recv, col_send, col_recv,
):
    column = lax.axis_index("gx")
    row = lax.axis_index("gy")
    span_x, span_y, extent_z = out.shape[1:]
    wide_x, wide_y = span_x + 2 * ITERS, span_y + 2 * ITERS
    reach = ITERS + HALO
    row_peers = [lax.rem(row + k, rows) for k in range(1, rows)]
    column_peers = [lax.rem(column + k, columns) for k in range(1, columns)]
    barrier = pltpu.get_barrier_semaphore()
    for other in row_peers:
        pl.semaphore_signal(barrier, inc=1, device_id=(column, other), device_id_type=MESH)
    for other in column_peers:
        pl.semaphore_signal(barrier, inc=1, device_id=(other, row), device_id_type=MESH)
    own = pltpu.make_async_copy(tile, held.at[column, row], own_sem)
    own.start()

    def peer(dx, dy):
        return (lax.rem(column + dx + columns, columns), row + dy)

    edge = []
    for c in range(3):
        low, high = wide_y * c, wide_y * (c + 1)
        inner = slice(HALO, wide_x - HALO)
        edge += [
            (spread.at[span_x : span_x + reach, low:high], from_left.at[c], 1, 0),
            (spread.at[HALO : HALO + reach, low:high], from_right.at[c], -1, 0),
            (spread.at[inner, high - RIM : high], from_below.at[c], 0, 1),
            (spread.at[inner, low : low + RIM], from_above.at[c], 0, -1),
            (from_left.at[c, :, wide_y - RIM :], corners.at[c, 0], 0, 1),
            (from_right.at[c, :, wide_y - RIM :], corners.at[c, 1], 0, 1),
            (from_left.at[c, :, 0:RIM], corners.at[c, 2], 0, -1),
            (from_right.at[c, :, 0:RIM], corners.at[c, 3], 0, -1),
        ]

    def start(k):
        src, dst, dx, dy = edge[k]
        when(
            exists(row, rows, dy),
            lambda: remote(src, dst, send, recv, k, peer(dx, dy)).start(),
        )

    def arrive(k):
        src, dst, dx, dy = edge[k]
        when(
            exists(row, rows, -dy),
            lambda: remote(src, dst, send, recv, k, peer(dx, dy)).wait_recv(),
        )

    def sent(k):
        src, dst, dx, dy = edge[k]
        when(
            exists(row, rows, dy),
            lambda: remote(src, dst, send, recv, k, peer(dx, dy)).wait_send(),
        )

    @pl.when(row == 0)
    def _():
        from_below[...] = jnp.zeros(from_below.shape, jnp.float32)
        for c in range(3):
            corners[c, 0:2] = jnp.zeros((2,) + corners.shape[2:], jnp.float32)

    @pl.when(row == rows - 1)
    def _():
        from_above[...] = jnp.zeros(from_above.shape, jnp.float32)
        for c in range(3):
            corners[c, 2:4] = jnp.zeros((2,) + corners.shape[2:], jnp.float32)

    pl.semaphore_wait(barrier, rows + columns - 2)
    first = [
        pltpu.make_async_remote_copy(
            src_ref=tile,
            dst_ref=held.at[column, row],
            send_sem=row_send.at[k],
            recv_sem=row_recv.at[k],
            device_id=(column, other),
            device_id_type=MESH,
        )
        for k, other in enumerate(row_peers)
    ]
    for copy in first:
        copy.start()
    for k in range(4):
        start(k)
    for c in range(1, 3):
        for k in range(2, 4):
            start(8 * c + k)
    own.wait()
    for copy in first:
        copy.wait()
    second = [
        pltpu.make_async_remote_copy(
            src_ref=held.at[column],
            dst_ref=held.at[column],
            send_sem=col_send.at[k],
            recv_sem=col_recv.at[k],
            device_id=(other, row),
            device_id_type=MESH,
        )
        for k, other in enumerate(column_peers)
    ]
    for copy in second:
        copy.start()
    for c in range(1, 3):
        for k in range(2):
            start(8 * c + k)

    cells = lax.broadcasted_iota(jnp.int32, (wide_y, extent_z), 0) + (row * span_y - ITERS)
    inside = jnp.logical_and(cells >= 0, cells < span_y * rows)
    mask_ref[...] = inside.astype(jnp.float32)
    inverse = 1.0 / (1.0 + 6.0 * DIFFUSION)

    def relaxed(source, x):
        here = source[x]
        beside = source[x - 1] + source[x + 1]
        beside = beside + pltpu.roll(here, 1, 0) + pltpu.roll(here, wide_y - 1, 0)
        beside = beside + pltpu.roll(here, 1, 1) + pltpu.roll(here, extent_z - 1, 1)
        return (rhs[x] + DIFFUSION * beside) * (inverse * mask_ref[...])

    for c in range(3):
        at = slice(wide_y * c, wide_y * (c + 1))
        for k in range(4):
            arrive(8 * c + k)
        for k in range(4, 8):
            start(8 * c + k)

        def build(x, carry, at=at, c=c):
            rhs[x] = spread[x, at]
            return carry

        lax.fori_loop(0, wide_x, build, 0)
        for x in range(reach):
            rhs[x] = rhs[x] + from_left[c, x]
            rhs[x + span_x + HALO] = rhs[x + span_x + HALO] + from_right[c, x]

        def rims(x, carry, c=c):
            y = x + HALO
            rhs[y, 0:RIM] = rhs[y, 0:RIM] + from_below[c, x]
            rhs[y, wide_y - RIM :] = rhs[y, wide_y - RIM :] + from_above[c, x]
            return carry

        lax.fori_loop(0, wide_x - 2 * HALO, rims, 0)
        for k in range(4, 8):
            arrive(8 * c + k)
        for x in range(reach):
            for side, y in enumerate((x, x + span_x + HALO)):
                rhs[y, 0:RIM] = rhs[y, 0:RIM] + corners[c, side, x]
                rhs[y, wide_y - RIM :] = rhs[y, wide_y - RIM :] + corners[c, 2 + side, x]

        def masked(x, carry):
            rhs[x] = rhs[x] * mask_ref[...]
            return carry

        lax.fori_loop(0, wide_x, masked, 0)
        source = rhs
        for sweep in range(ITERS - 1):
            target = one if sweep % 2 == 0 else two

            def step(pair, carry, source=source, target=target, first=sweep + 1):
                x = first + 2 * pair
                new = (relaxed(source, x), relaxed(source, x + 1))
                target[x] = new[0]
                target[x + 1] = new[1]
                return carry

            lax.fori_loop(0, wide_x // 2 - sweep - 1, step, 0)
            source = target

        def last(pair, carry, source=source, c=c):
            x = 2 * pair
            new = (relaxed(source, x + ITERS), relaxed(source, x + ITERS + 1))
            out[c, x] = new[0][ITERS : ITERS + span_y]
            out[c, x + 1] = new[1][ITERS : ITERS + span_y]
            return carry

        lax.fori_loop(0, span_x // 2, last, 0)

    for copy in second:
        copy.wait()
    gathered = held[...].reshape(-1, TILE_LANES)
    moved = jnp.dot(
        matrix[...],
        gathered,
        precision=lax.Precision.HIGHEST,
        preferred_element_type=jnp.float32,
    )
    motion_out[...] = jnp.dot(
        links[...],
        moved,
        precision=lax.Precision.HIGHEST,
        preferred_element_type=jnp.float32,
    )
    for k in range(len(edge)):
        sent(k)


def tail(spread, tile, matrix, links, span_y):
    columns, rows = lax.axis_size("gx"), lax.axis_size("gy")
    wide_x, _, extent_z = spread.shape
    span_x = wide_x - 2 * ITERS
    wide_y = span_y + 2 * ITERS
    reach = ITERS + HALO
    f32 = jnp.float32
    vmem = pl.BlockSpec(memory_space=pltpu.VMEM)
    dma = pltpu.SemaphoreType.DMA
    return pl.pallas_call(
        functools.partial(tail_kernel, columns, rows),
        out_shape=[
            jax.ShapeDtypeStruct((3, span_x, span_y, extent_z), f32),
            jax.ShapeDtypeStruct((links.shape[0], TILE_LANES), f32),
        ],
        in_specs=[vmem] * 4,
        out_specs=[vmem] * 2,
        scratch_shapes=[
            pltpu.VMEM((3, reach, wide_y, extent_z), f32),
            pltpu.VMEM((3, reach, wide_y, extent_z), f32),
            pltpu.VMEM((3, wide_x - 2 * HALO, RIM, extent_z), f32),
            pltpu.VMEM((3, wide_x - 2 * HALO, RIM, extent_z), f32),
            pltpu.VMEM((3, 4, reach, RIM, extent_z), f32),
            pltpu.VMEM((columns, rows) + tile.shape, f32),
            pltpu.VMEM((wide_x, wide_y, extent_z), f32),
            pltpu.VMEM((wide_x, wide_y, extent_z), f32),
            pltpu.VMEM((wide_x, wide_y, extent_z), f32),
            pltpu.VMEM((wide_y, extent_z), f32),
            dma,
            dma((24,)),
            dma((24,)),
            dma((rows - 1,)),
            dma((rows - 1,)),
            dma((columns - 1,)),
            dma((columns - 1,)),
        ],
        compiler_params=pltpu.CompilerParams(
            collective_id=1, has_side_effects=True, vmem_limit_bytes=56 * 2**20
        ),
        name="tail",
    )(spread, tile, matrix, links)


def on_device(
    velocity,
    owner_block,
    base_x,
    base_y,
    base_z,
    delta_weights,
    marker_offset,
    sphere_motion,
    contact_sphere,
    contact_partner,
):
    span_y = velocity.shape[2]
    row_count = lax.axis_size("gy")
    column_count = lax.axis_size("gx")
    here = lax.axis_index(("gx", "gy"))
    devices = row_count * column_count
    spheres = sphere_motion.shape[1]
    per_sphere = base_x.shape[0] // spheres
    lanes = len(DIRECTIONS)
    ids = jnp.stack([owner_block[:, 0], base_x, base_y, base_z]).astype(jnp.float32)
    home, arrived, *halos = front(ids, delta_weights, marker_offset, sphere_motion, velocity)
    spread, sums = markers_stage(spheres, velocity, halos, home, arrived, sphere_motion)
    sums = sums[:, :6].reshape(lanes + 1, spheres * 6)
    tile = jnp.concatenate([sums, sphere_motion.T.reshape(1, spheres * 6)], axis=0)
    tile = jnp.pad(tile, ((0, TILE_ROWS - tile.shape[0]), (0, TILE_LANES - tile.shape[1])))
    mine = here * spheres + jnp.arange(spheres, dtype=jnp.int32)
    known = jnp.arange(devices * spheres, dtype=jnp.int32)
    own = (mine[:, None] == known[None, :]).astype(jnp.float32)
    acts = (contact_sphere[None, :] == mine[:, None]).astype(jnp.float32)
    partner = (contact_partner[:, None] == known[None, :]).astype(jnp.float32)
    linked = jnp.sum(acts[:, :, None] * partner[None], axis=1)
    linked = own + DASHPOT * (linked - jnp.sum(acts, axis=1)[:, None] * own)
    both = jnp.concatenate([linked, own], axis=0)
    links = both.reshape(2 * spheres, devices, spheres).transpose(0, 2, 1)
    links = links.reshape(2 * spheres * spheres, devices)
    matrix = jnp.asarray(combine_matrix(column_count, row_count, per_sphere))
    state, motion = tail(spread, tile, matrix, links, span_y)
    motion = motion.reshape(2, spheres, spheres, TILE_LANES)
    linear = sum(motion[0, :, s, 6 * s : 6 * s + 3] for s in range(spheres))
    angular = sum(motion[1, :, s, 6 * s + 3 : 6 * s + 6] for s in range(spheres))
    return state, jnp.concatenate([linear, angular], axis=1).T


def solution(mesh):
    placed = (
        P(None, "gx", "gy", None),
        P(("gx", "gy"), None),
        P(("gx", "gy")),
        P(("gx", "gy")),
        P(("gx", "gy")),
        P(None, ("gx", "gy")),
        P(None, ("gx", "gy")),
        P(None, ("gx", "gy")),
        P(("gx", "gy")),
        P(("gx", "gy")),
    )
    return jax.shard_map(
        on_device,
        mesh=mesh,
        in_specs=placed,
        out_specs=(P(None, "gx", "gy", None), P(None, ("gx", "gy"))),
        check_vma=False,
    )
```

```python
import functools

import jax
import jax.numpy as jnp
import numpy as np
from jax import lax
from jax.experimental import pallas as pl
from jax.experimental.pallas import tpu as pltpu
from jax.sharding import PartitionSpec as P

ITERS = 4
DIFFUSION = 1.0
RESPONSE = 0.5
DASHPOT = 0.1

MESH = pl.DeviceIdType.MESH
TILE_ROWS = 16
TILE_LANES = 128
CHUNK = 256
WINDOW = 8
GROUP = 6
RECORD = 24
X_ROW, Y_ROW, Z_ROW, TARGET, OFFSET, SPHERE, LIVE = 12, 13, 14, 15, 18, 21, 22
DIRECTIONS = ((-1, -1), (-1, 0), (-1, 1), (0, -1), (0, 1), (1, -1), (1, 0), (1, 1))
HALO = 2
RIM = 8


def when(condition, body):
    if condition is True:
        body()
    else:
        pl.when(condition)(body)


def exists(row, rows, dy):
    if dy == 0:
        return True
    return row + dy < rows if dy > 0 else row + dy >= 0


def greet(columns, rows, column, row):
    barrier = pltpu.get_barrier_semaphore()
    for dx, dy in DIRECTIONS:
        peer = (lax.rem(column + dx + columns, columns), row + dy)
        when(
            exists(row, rows, dy),
            lambda peer=peer: pl.semaphore_signal(
                barrier, inc=1, device_id=peer, device_id_type=MESH
            ),
        )
    return barrier


def greeted(rows, row):
    inner = lax.min(row, 1) + lax.min(rows - 1 - row, 1)
    return 2 + 3 * inner


def remote(src, dst, send, recv, k, peer):
    return pltpu.make_async_remote_copy(
        src_ref=src,
        dst_ref=dst,
        send_sem=send.at[k],
        recv_sem=recv.at[k],
        device_id=peer,
        device_id_type=MESH,
    )


def split(value):
    high = value.astype(jnp.bfloat16).astype(jnp.float32)
    return high, value - high


def upper_triangle():
    rows = lax.broadcasted_iota(jnp.int32, (CHUNK, CHUNK), 0)
    lanes = lax.broadcasted_iota(jnp.int32, (CHUNK, CHUNK), 1)
    return (rows <= lanes).astype(jnp.float32).astype(jnp.bfloat16)


def ranks(categories, count):
    rows = lax.broadcasted_iota(jnp.int32, (count, CHUNK), 0).astype(jnp.float32)
    hot = [(rows == block).astype(jnp.float32) for block in categories]
    stacked = jnp.concatenate(hot, axis=0).astype(jnp.bfloat16)
    inside = jnp.dot(stacked, upper_triangle(), preferred_element_type=jnp.float32)
    carry = jnp.zeros((count, 1), jnp.float32)
    upto = []
    for b in range(len(hot)):
        block = inside[b * count : (b + 1) * count]
        upto.append(block + carry)
        carry = carry + block[:, CHUNK - 1 : CHUNK]
    return hot, upto, carry


def place(parts, where_to, groups):
    group = jnp.floor(where_to * (1.0 / CHUNK))
    slot = where_to - group * CHUNK
    rows = lax.broadcasted_iota(jnp.int32, (CHUNK, where_to.shape[1]), 0).astype(jnp.float32)
    hot = (rows == slot).astype(jnp.float32).astype(jnp.bfloat16)
    masked = [parts * (group == g).astype(jnp.float32) for g in groups]
    masked = jnp.concatenate(masked, axis=0).astype(jnp.bfloat16)
    moved = lax.dot_general(
        masked, hot, (((1,), (1,)), ((), ())), preferred_element_type=jnp.float32
    )
    result = []
    for n in range(len(groups)):
        piece = moved[2 * RECORD * n : 2 * RECORD * (n + 1)]
        result.append(piece[:RECORD] + piece[RECORD:])
    return result


def front_kernel(
    columns, rows, owners, base_x, base_y, base_z, weights, offsets, motion, velocity,
    home, arrived, left, right, below, above, corners, slots, send, recv,
):
    column = lax.axis_index("gx")
    row = lax.axis_index("gy")
    span_x, span_y = velocity.shape[1], velocity.shape[2]
    barrier = greet(columns, rows, column, row)

    def peer(dx, dy):
        return (lax.rem(column + dx + columns, columns), row + dy)

    edge = [
        (velocity.at[:, 0:HALO], right, -1, 0),
        (velocity.at[:, span_x - HALO : span_x], left, 1, 0),
        (velocity.at[:, :, 0:RIM], above, 0, -1),
        (velocity.at[:, :, span_y - RIM : span_y], below, 0, 1),
    ]
    for side, halo in enumerate((left, right)):
        edge.append((halo.at[:, :, 0:RIM], corners.at[2 + side], 0, -1))
        edge.append((halo.at[:, :, span_y - RIM : span_y], corners.at[side], 0, 1))
    for g, (dx, dy) in enumerate(DIRECTIONS):
        edge.append((slots.at[g], arrived.at[g], dx, dy))

    def start(k):
        src, dst, dx, dy = edge[k]
        when(
            exists(row, rows, dy),
            lambda: remote(src, dst, send, recv, k, peer(dx, dy)).start(),
        )

    def arrive(k):
        src, dst, dx, dy = edge[k]
        when(
            exists(row, rows, -dy),
            lambda: remote(src, dst, send, recv, k, peer(dx, dy)).wait_recv(),
        )

    def sent(k):
        src, dst, dx, dy = edge[k]
        when(
            exists(row, rows, dy),
            lambda: remote(src, dst, send, recv, k, peer(dx, dy)).wait_send(),
        )

    @pl.when(row == 0)
    def _():
        below[...] = jnp.zeros(below.shape, jnp.float32)
        for n in (0, 1):
            corners[n] = jnp.zeros(corners.shape[1:], jnp.float32)
        for g, (dx, dy) in enumerate(DIRECTIONS):
            if dy > 0:
                arrived[g] = jnp.zeros(arrived.shape[1:], jnp.float32)

    @pl.when(row == rows - 1)
    def _():
        above[...] = jnp.zeros(above.shape, jnp.float32)
        for n in (2, 3):
            corners[n] = jnp.zeros(corners.shape[1:], jnp.float32)
        for g, (dx, dy) in enumerate(DIRECTIONS):
            if dy < 0:
                arrived[g] = jnp.zeros(arrived.shape[1:], jnp.float32)

    pl.semaphore_wait(barrier, greeted(rows, row))
    for k in range(4):
        start(k)

    markers = owners.shape[1]
    spheres = motion.shape[0]
    per_sphere = markers // spheres
    owner = owners[...].astype(jnp.float32)
    owner_x = jnp.floor((owner + 0.5) * (1.0 / rows))
    owner_y = owner - owner_x * rows
    step_x = owner_x - column.astype(jnp.float32)
    step_x = jnp.where(step_x > 1.5, step_x - columns, step_x)
    step_x = jnp.where(step_x < -1.5, step_x + columns, step_x)
    step_y = owner_y - row.astype(jnp.float32)
    lane = (step_x + 1.0) * 3.0 + step_y + 1.0
    at_home = lane == 4.0
    lane = jnp.where(at_home, -1.0, jnp.where(lane > 4.0, lane - 1.0, lane))
    offset = offsets[...]
    targets = []
    for s in range(spheres):
        o = offset[:, s * per_sphere : (s + 1) * per_sphere]
        m = [motion[s : s + 1, c : c + 1] for c in range(6)]
        targets.append(
            jnp.concatenate(
                [
                    m[0] + (m[4] * o[2:3] - m[5] * o[1:2]),
                    m[1] + (m[5] * o[0:1] - m[3] * o[2:3]),
                    m[2] + (m[3] * o[1:2] - m[4] * o[0:1]),
                ],
                axis=0,
            )
        )
    home[0:12] = weights[...]
    for line, base in ((X_ROW, base_x), (Y_ROW, base_y), (Z_ROW, base_z)):
        home[line : line + 1] = base[...].astype(jnp.float32)
    home[TARGET : TARGET + 3] = jnp.concatenate(targets, axis=1)
    home[OFFSET : OFFSET + 3] = offset
    position = lax.broadcasted_iota(jnp.int32, (1, markers), 1)
    sphere = jnp.zeros((1, markers), jnp.float32)
    for s in range(1, spheres):
        sphere = sphere + (position >= s * per_sphere).astype(jnp.float32)
    home[SPHERE : SPHERE + 1] = sphere
    home[LIVE : LIVE + 1] = jnp.ones((1, markers), jnp.float32)
    home[LIVE + 1 : LIVE + 2] = jnp.zeros((1, markers), jnp.float32)

    lanes = len(DIRECTIONS)
    blocks = markers // CHUNK
    hot, upto, totals = ranks([lane[:, b * CHUNK : (b + 1) * CHUNK] for b in range(blocks)], lanes)
    rank = [jnp.sum(h * (u - 1.0), axis=0, keepdims=True) for h, u in zip(hot, upto)]
    where_to = jnp.concatenate(rank, axis=1) + lane * CHUNK
    where_to = jnp.where(at_home, -1.0, where_to)
    parts = jnp.concatenate(split(home[...]), axis=0)
    for g, piece in enumerate(place(parts, where_to, range(lanes))):
        slots[g] = piece
    home[LIVE : LIVE + 1] = at_home.astype(jnp.float32)

    for k in range(8, 8 + lanes):
        start(k)
    arrive(0)
    arrive(1)
    for k in range(4, 8):
        start(k)
    for k in range(2, 8 + lanes):
        arrive(k)
    for k in range(8 + lanes):
        sent(k)


def front(owners, bases, weights, offsets, motion, velocity):
    columns, rows = lax.axis_size("gx"), lax.axis_size("gy")
    span_x, span_y, extent_z = velocity.shape[1:]
    markers = owners.shape[1]
    lanes = len(DIRECTIONS)
    f32 = jnp.float32
    copies = 8 + lanes
    vmem = pl.BlockSpec(memory_space=pltpu.VMEM)
    out = [
        (RECORD, markers),
        (lanes, RECORD, CHUNK),
        (3, HALO, span_y, extent_z),
        (3, HALO, span_y, extent_z),
        (3, span_x, RIM, extent_z),
        (3, span_x, RIM, extent_z),
        (4, 3, HALO, RIM, extent_z),
    ]
    return pl.pallas_call(
        functools.partial(front_kernel, columns, rows),
        out_shape=[jax.ShapeDtypeStruct(shape, f32) for shape in out],
        in_specs=[vmem] * 8,
        out_specs=[vmem] * len(out),
        scratch_shapes=[
            pltpu.VMEM((lanes, RECORD, CHUNK), f32),
            pltpu.SemaphoreType.DMA((copies,)),
            pltpu.SemaphoreType.DMA((copies,)),
        ],
        compiler_params=pltpu.CompilerParams(collective_id=0, has_side_effects=True),
        name="front",
    )(owners, *bases, weights, offsets, motion, velocity)


def four(distance, weights):
    value = jnp.where(distance == 3.0, weights[3:4], 0.0)
    for n in (2, 1, 0):
        value = jnp.where(distance == float(n), weights[n : n + 1], value)
    return value


def markers_kernel(
    spheres, velocity, left, right, below, above, corners, home, arrived, motion,
    spread, edges, tile, high, low, sorted_refs, parts, sums,
):
    span_x, span_y, extent_z = velocity.shape[1:]
    wide_y = span_y + 2 * ITERS
    lanes = len(DIRECTIONS)
    bf16, f32 = jnp.bfloat16, jnp.float32
    layers = span_x + 2 * HALO

    def layer(x, row_source, below_source, above_source, own):
        for c in range(3):
            rows = row_source(c)
            edge = jnp.zeros((HALO, extent_z), f32)
            value = jnp.concatenate(
                [
                    edge,
                    below_source(c)[RIM - HALO : RIM],
                    rows,
                    above_source(c)[0:HALO],
                    edge,
                ],
                axis=0,
            )
            at = slice(wide_y * c, wide_y * (c + 1))
            first, rest = split(value)
            high[x, at] = first.astype(bf16)
            low[x, at] = rest.astype(bf16)
            if own:
                wide = jnp.zeros((ITERS, extent_z), f32)
                spread[x + HALO, at] = jnp.concatenate([wide, rows, wide], axis=0)
        end = jnp.zeros((high.shape[1] - 3 * wide_y, extent_z), bf16)
        high[x, 3 * wide_y :] = end
        low[x, 3 * wide_y :] = end

    def inner(x, carry):
        layer(
            x + HALO,
            lambda c: velocity[c, x],
            lambda c: below[c, x],
            lambda c: above[c, x],
            True,
        )
        return carry

    lax.fori_loop(0, span_x, inner, 0)
    for side, halo in enumerate((left, right)):
        for x in range(HALO):
            layer(
                x + side * (span_x + HALO),
                lambda c: halo[c, x],
                lambda c: corners[side, c, x],
                lambda c: corners[2 + side, c, x],
                False,
            )
    for x in range(ITERS):
        spread[x] = jnp.zeros(spread.shape[1:], f32)
        spread[span_x + ITERS + x] = jnp.zeros(spread.shape[1:], f32)

    markers = home.shape[1]
    blocks = markers // CHUNK
    total = blocks + lanes
    count = -(-(span_x + 1) // 8) * 8
    categories = []
    live = []
    for b in range(total):
        at = slice(b * CHUNK, (b + 1) * CHUNK)
        if b < blocks:
            record = home[:, at]
            group = lanes + record[SPHERE : SPHERE + 1] * (lanes + 1)
        else:
            record = arrived[b - blocks]
            group = (b - blocks) + record[SPHERE : SPHERE + 1] * (lanes + 1)
        alive = record[LIVE : LIVE + 1] > 0.5
        live.append(alive)
        categories.append(jnp.where(alive, record[X_ROW : X_ROW + 1], -1.0))
        first, rest = split(record)
        parts[0:RECORD, at] = first
        parts[RECORD : 2 * RECORD, at] = rest
        parts[SPHERE : SPHERE + 1, at] = group
    hot, upto, totals = ranks(categories, count)
    lower_rows = lax.broadcasted_iota(jnp.int32, (count, count), 0)
    lower_lanes = lax.broadcasted_iota(jnp.int32, (count, count), 1)
    before = (lower_lanes < lower_rows).astype(f32)
    starts = jnp.dot(
        before,
        jnp.broadcast_to(totals, (count, TILE_LANES)),
        precision=lax.Precision.HIGHEST,
        preferred_element_type=f32,
    )[:, 0:1]
    places = []
    for b in range(total):
        rank = jnp.sum(hot[b] * (upto[b] + (starts - 1.0)), axis=0, keepdims=True)
        places.append(jnp.where(live[b], rank, -1.0))
    where_to = jnp.concatenate(places, axis=1)
    alive_count = jnp.sum(totals).astype(jnp.int32)
    for first in range(0, total, GROUP):
        groups = range(first, min(first + GROUP, total))

        @pl.when(alive_count > first * CHUNK)
        def _(groups=groups):
            for g, piece in zip(groups, place(parts[...], where_to, groups)):
                sorted_refs[g] = piece

    sums[...] = jnp.zeros(sums.shape, f32)
    z_cells = lax.broadcasted_iota(jnp.int32, (extent_z, CHUNK), 0).astype(f32)
    y_cells = lax.broadcasted_iota(jnp.int32, (wide_y, CHUNK), 0).astype(f32) - HALO
    x_cells = lax.broadcasted_iota(jnp.int32, (WINDOW, CHUNK), 0).astype(f32)

    def chunk(j, carry):
        record = sorted_refs[j]
        alive = record[LIVE : LIVE + 1]
        cell_x = record[X_ROW : X_ROW + 1]
        distance = z_cells - record[Z_ROW : Z_ROW + 1]
        distance = jnp.where(distance < 0.0, distance + extent_z, distance)
        z_high, z_low = split(four(distance, record[8:12]))
        z_high = z_high.astype(bf16)
        z_low = z_low.astype(bf16)
        y_table = four(y_cells - record[Y_ROW : Y_ROW + 1], record[4:8])
        least = jnp.min(jnp.where(alive > 0.5, cell_x, 1e4)).astype(jnp.int32)
        most = jnp.max(jnp.where(alive > 0.5, cell_x, -1.0)).astype(jnp.int32)
        windows = (most + 4 - least + WINDOW - 1) // WINDOW

        def x_table(k):
            fresh = least + WINDOW * k
            base = jnp.minimum(fresh, layers - WINDOW)
            cells = x_cells + base.astype(f32)
            table = four(cells - cell_x, record[0:4])
            return base, jnp.where(cells >= fresh.astype(f32), table, 0.0)

        z_stack = jnp.concatenate([z_high, z_high, z_low], axis=0)

        def sample(k, total):
            base, table = x_table(k)
            rows = high.shape[1]
            first = high[pl.ds(base, WINDOW)].reshape(WINDOW * rows, extent_z)
            rest = low[pl.ds(base, WINDOW)].reshape(WINDOW * rows, extent_z)
            lines = jnp.dot(
                jnp.concatenate([first, rest, first], axis=1),
                z_stack,
                preferred_element_type=f32,
            )
            for x in range(WINDOW):
                total = total + lines[x * rows : x * rows + 3 * wide_y] * table[x : x + 1]
            return total

        plane = lax.fori_loop(0, windows, sample, jnp.zeros((3 * wide_y, CHUNK), f32))
        forces = []
        for c in range(3):
            got = jnp.sum(plane[c * wide_y : (c + 1) * wide_y] * y_table, axis=0, keepdims=True)
            forces.append((record[TARGET + c : TARGET + c + 1] - got) * alive)
        sheet = jnp.concatenate([force * y_table for force in forces], axis=0)
        z_wide = jnp.concatenate([z_high, z_high, z_low], axis=1)

        def deposit(k, carry):
            base, table = x_table(k)
            value = jnp.concatenate([sheet * table[x : x + 1] for x in range(WINDOW)], axis=0)
            first, rest = split(value)
            first = first.astype(bf16)
            rest = rest.astype(bf16)
            added = lax.dot_general(
                jnp.concatenate([first, rest, first], axis=1),
                z_wide,
                (((1,), (1,)), ((), ())),
                preferred_element_type=f32,
            )
            at = pl.ds(base + HALO, WINDOW)
            spread[at] = spread[at] + added.reshape(WINDOW, 3 * wide_y, extent_z)
            return carry

        lax.fori_loop(0, windows, deposit, 0)
        o = [record[OFFSET + c : OFFSET + c + 1] for c in range(3)]
        f = forces
        moments = jnp.concatenate(
            f
            + [
                o[1] * f[2] - o[2] * f[1],
                o[2] * f[0] - o[0] * f[2],
                o[0] * f[1] - o[1] * f[0],
                jnp.zeros((2, CHUNK), f32),
            ],
            axis=0,
        )
        group = record[SPHERE : SPHERE + 1]
        for g in range((lanes + 1) * spheres):
            sums[g] = sums[g] + jnp.where(group == float(g), moments, 0.0)
        return carry

    chunks = (alive_count + (CHUNK - 1)) // CHUNK
    lax.fori_loop(0, chunks, chunk, 0)
    columns = jnp.sum(sums[...], axis=2)
    tile[...] = jnp.zeros(tile.shape, f32)
    for s in range(spheres):
        at = slice(6 * s, 6 * (s + 1))
        tile[0 : lanes + 1, at] = columns[(lanes + 1) * s : (lanes + 1) * (s + 1), 0:6]
        tile[lanes + 1 : lanes + 2, at] = motion[s : s + 1]
    reach = ITERS + HALO
    depth = span_y + 2 * HALO
    for side, first in enumerate((span_x, HALO)):
        for c in range(3):
            for x in range(reach):
                edges[side, c, depth * x : depth * (x + 1)] = spread[
                    first + x, wide_y * c + HALO : wide_y * (c + 1) - HALO
                ]


def markers_stage(spheres, velocity, halos, home, arrived, motion):
    span_x, span_y, extent_z = velocity.shape[1:]
    wide_y = span_y + 2 * ITERS
    lanes = len(DIRECTIONS)
    f32 = jnp.float32
    total = home.shape[1] // CHUNK + lanes
    groups = (lanes + 1) * spheres
    field_rows = -(-3 * wide_y // 16) * 16
    field = (span_x + 2 * HALO, field_rows, extent_z)
    vmem = pl.BlockSpec(memory_space=pltpu.VMEM)
    return pl.pallas_call(
        functools.partial(markers_kernel, spheres),
        out_shape=[
            jax.ShapeDtypeStruct((span_x + 2 * ITERS, 3 * wide_y, extent_z), f32),
            jax.ShapeDtypeStruct((2, 3, (ITERS + HALO) * (span_y + 2 * HALO), extent_z), f32),
            jax.ShapeDtypeStruct((TILE_ROWS, TILE_LANES), f32),
        ],
        in_specs=[vmem] * 9,
        out_specs=[vmem] * 3,
        scratch_shapes=[
            pltpu.VMEM(field, jnp.bfloat16),
            pltpu.VMEM(field, jnp.bfloat16),
            pltpu.VMEM((total, RECORD, CHUNK), f32),
            pltpu.VMEM((2 * RECORD, total * CHUNK), f32),
            pltpu.VMEM((groups, 8, CHUNK), f32),
        ],
        compiler_params=pltpu.CompilerParams(vmem_limit_bytes=56 * 2**20),
        name="markers",
    )(velocity, *halos, home, arrived, motion)


def combine_matrix(columns, rows, per_sphere):
    matrix = np.zeros((columns, rows, columns, rows, TILE_ROWS), np.float32)
    for i in range(columns):
        for j in range(rows):
            for slot, (dx, dy) in enumerate(DIRECTIONS):
                if 0 <= j - dy < rows:
                    matrix[(i - dx) % columns, j - dy, i, j, slot] -= RESPONSE / per_sphere
            matrix[i, j, i, j, len(DIRECTIONS)] -= RESPONSE / per_sphere
            matrix[i, j, i, j, len(DIRECTIONS) + 1] = 1.0
    return matrix.reshape(columns * rows, -1)


def tail_kernel(
    columns, rows, spread, edges, tile, matrix, contact_sphere, contact_partner,
    out, motion_out, from_left, from_right, from_below, from_above, given, corners, held,
    rhs, one, two, mask_ref, own_sem, send, recv, row_send, row_recv, col_send, col_recv,
):
    column = lax.axis_index("gx")
    row = lax.axis_index("gy")
    span_x, span_y, extent_z = out.shape[1:]
    wide_x, wide_y = span_x + 2 * ITERS, span_y + 2 * ITERS
    reach = ITERS + HALO
    depth = span_y + 2 * HALO
    row_peers = [lax.rem(row + k, rows) for k in range(1, rows)]
    column_peers = [lax.rem(column + k, columns) for k in range(1, columns)]
    barrier = pltpu.get_barrier_semaphore()
    for other in row_peers:
        pl.semaphore_signal(barrier, inc=1, device_id=(column, other), device_id_type=MESH)
    for other in column_peers:
        pl.semaphore_signal(barrier, inc=1, device_id=(other, row), device_id_type=MESH)
    own = pltpu.make_async_copy(tile, held.at[column, row], own_sem)
    own.start()

    def peer(dx, dy):
        return (lax.rem(column + dx + columns, columns), row + dy)

    edge = []
    for c in range(3):
        low, high = wide_y * c, wide_y * (c + 1)
        inner = slice(HALO, wide_x - HALO)
        edge += [
            (edges.at[0, c], from_left.at[c], 1, 0),
            (edges.at[1, c], from_right.at[c], -1, 0),
            (spread.at[inner, high - RIM : high], from_below.at[c], 0, 1),
            (spread.at[inner, low : low + RIM], from_above.at[c], 0, -1),
            (given.at[c, 0], corners.at[c, 0], 0, 1),
            (given.at[c, 1], corners.at[c, 1], 0, 1),
            (given.at[c, 2], corners.at[c, 2], 0, -1),
            (given.at[c, 3], corners.at[c, 3], 0, -1),
        ]

    def start(k):
        src, dst, dx, dy = edge[k]
        when(
            exists(row, rows, dy),
            lambda: remote(src, dst, send, recv, k, peer(dx, dy)).start(),
        )

    def arrive(k):
        src, dst, dx, dy = edge[k]
        when(
            exists(row, rows, -dy),
            lambda: remote(src, dst, send, recv, k, peer(dx, dy)).wait_recv(),
        )

    def sent(k):
        src, dst, dx, dy = edge[k]
        when(
            exists(row, rows, dy),
            lambda: remote(src, dst, send, recv, k, peer(dx, dy)).wait_send(),
        )

    @pl.when(row == 0)
    def _():
        from_below[...] = jnp.zeros(from_below.shape, jnp.float32)
        for c in range(3):
            corners[c, 0:2] = jnp.zeros((2,) + corners.shape[2:], jnp.float32)

    @pl.when(row == rows - 1)
    def _():
        from_above[...] = jnp.zeros(from_above.shape, jnp.float32)
        for c in range(3):
            corners[c, 2:4] = jnp.zeros((2,) + corners.shape[2:], jnp.float32)

    pl.semaphore_wait(barrier, rows + columns - 2)
    first = [
        pltpu.make_async_remote_copy(
            src_ref=tile,
            dst_ref=held.at[column, row],
            send_sem=row_send.at[k],
            recv_sem=row_recv.at[k],
            device_id=(column, other),
            device_id_type=MESH,
        )
        for k, other in enumerate(row_peers)
    ]
    for copy in first:
        copy.start()
    for k in range(4):
        start(k)
    for c in range(1, 3):
        for k in range(2, 4):
            start(8 * c + k)

    cells = lax.broadcasted_iota(jnp.int32, (wide_y, extent_z), 0) + (row * span_y - ITERS)
    inside = jnp.logical_and(cells >= 0, cells < span_y * rows)
    inverse = 1.0 / (1.0 + 6.0 * DIFFUSION)
    mask_ref[0] = inside.astype(jnp.float32)
    mask_ref[1] = inside.astype(jnp.float32) * inverse

    own.wait()
    for copy in first:
        copy.wait()
    second = [
        pltpu.make_async_remote_copy(
            src_ref=held.at[column],
            dst_ref=held.at[column],
            send_sem=col_send.at[k],
            recv_sem=col_recv.at[k],
            device_id=(other, row),
            device_id_type=MESH,
        )
        for k, other in enumerate(column_peers)
    ]
    for copy in second:
        copy.start()
    for c in range(1, 3):
        for k in range(2):
            start(8 * c + k)

    def relaxed(c, source, x):
        here = source[c, x]
        beside = source[c, x - 1] + source[c, x + 1]
        beside = beside + pltpu.roll(here, 1, 0) + pltpu.roll(here, wide_y - 1, 0)
        beside = beside + pltpu.roll(here, 1, 1) + pltpu.roll(here, extent_z - 1, 1)
        return (rhs[c, x] + DIFFUSION * beside) * mask_ref[1]

    buffers = (rhs, one, two, one)

    def sweeps(c, starts, length):
        for sweep in range(ITERS):
            source = buffers[sweep]
            for first, shift in starts:
                begin = first + sweep * shift
                for x in range(begin, begin + length(sweep)):
                    new = relaxed(c, source, x)
                    if sweep == ITERS - 1:
                        out[c, x - ITERS] = new[ITERS : ITERS + span_y]
                    else:
                        buffers[sweep + 1][c, x] = new

    def base(c, carry):
        for x in range(wide_x):
            rhs[c, x] = spread[x, pl.ds(pl.multiple_of(wide_y * c, 8), wide_y)]
        for x in range(wide_x - 2 * HALO):
            y = x + HALO
            rhs[c, y, 0:RIM] = rhs[c, y, 0:RIM] + from_below[c, x]
            rhs[c, y, wide_y - RIM :] = rhs[c, y, wide_y - RIM :] + from_above[c, x]
        for x in range(reach, wide_x - reach):
            rhs[c, x] = rhs[c, x] * mask_ref[0]
        sweeps(c, ((reach + 1, 1),), lambda sweep: span_x - 2 * HALO - 2 - 2 * sweep)
        return carry

    for c in range(3):
        arrive(8 * c + 2)
        arrive(8 * c + 3)
    lax.fori_loop(0, 3, base, 0)

    def outer(c):
        for x in range(reach):
            for side, y in enumerate((x, x + span_x + HALO)):
                at = slice(6 * x, 6 * (x + 1))
                rhs[c, y, 0:6] = rhs[c, y, 0:6] + corners[c, side, at]
                rhs[c, y, wide_y - 6 :] = rhs[c, y, wide_y - 6 :] + corners[c, 2 + side, at]
                rhs[c, y] = rhs[c, y] * mask_ref[0]
        sweeps(c, ((1, 1), (span_x + 1, -1)), lambda sweep: reach)

    for c in range(3):
        arrive(8 * c)
        arrive(8 * c + 1)
        for side, halo in enumerate((from_left, from_right)):
            for up, first in ((0, depth - reach), (2, 0)):
                pieces = [
                    halo[c, depth * x + first : depth * x + first + reach] for x in range(reach)
                ]
                given[c, up + side, 0 : reach * reach] = jnp.concatenate(pieces, axis=0)
        for x in range(reach):
            for halo, y in ((from_left, x), (from_right, x + span_x + HALO)):
                rhs[c, y, HALO : wide_y - HALO] = (
                    rhs[c, y, HALO : wide_y - HALO] + halo[c, depth * x : depth * (x + 1)]
                )
        for k in range(4, 8):
            start(8 * c + k)
        for k in range(4, 8):
            arrive(8 * c + k)
        outer(c)

    for copy in second:
        copy.wait()
    gathered = held[...].reshape(-1, TILE_LANES)
    moved = jnp.dot(
        matrix[...],
        gathered,
        precision=lax.Precision.HIGHEST,
        preferred_element_type=jnp.float32,
    )
    spheres = motion_out.shape[0]
    device = lax.broadcasted_iota(jnp.int32, (1, columns * rows), 1)
    here = column * rows + row
    linked, owned = [], []
    for s in range(spheres):
        mine = here * spheres + s
        for other in range(spheres):
            own_row = (device * spheres + other == mine).astype(jnp.float32)
            line = own_row
            for k in range(contact_sphere.shape[0]):
                acts = contact_sphere[k] == mine
                partner = (device * spheres + other == contact_partner[k]).astype(jnp.float32)
                line = line + jnp.where(acts, DASHPOT * (partner - own_row), 0.0)
            linked.append(line)
            owned.append(own_row)
    links = jnp.concatenate(linked + owned, axis=0)
    result = jnp.dot(
        links, moved, precision=lax.Precision.HIGHEST, preferred_element_type=jnp.float32
    )
    for s in range(spheres):
        for part in range(2):
            total = 0.0
            for other in range(spheres):
                line = (part * spheres + s) * spheres + other
                at = 6 * other + 3 * part
                total = total + result[line : line + 1, at : at + 3]
            motion_out[s : s + 1, 3 * part : 3 * part + 3] = total
    for k in range(len(edge)):
        sent(k)


def tail(spread, edges, tile, matrix, contact_sphere, contact_partner, span_y, spheres):
    columns, rows = lax.axis_size("gx"), lax.axis_size("gy")
    wide_x, _, extent_z = spread.shape
    span_x = wide_x - 2 * ITERS
    wide_y = span_y + 2 * ITERS
    reach = ITERS + HALO
    f32 = jnp.float32
    vmem = pl.BlockSpec(memory_space=pltpu.VMEM)
    smem = pl.BlockSpec(memory_space=pltpu.SMEM)
    dma = pltpu.SemaphoreType.DMA
    corner = (3, 4, -(-reach * reach // 8) * 8, extent_z)
    frame = (3, wide_x, wide_y, extent_z)
    return pl.pallas_call(
        functools.partial(tail_kernel, columns, rows),
        out_shape=[
            jax.ShapeDtypeStruct((3, span_x, span_y, extent_z), f32),
            jax.ShapeDtypeStruct((spheres, 6), f32),
        ],
        in_specs=[vmem] * 4 + [smem] * 2,
        out_specs=[vmem] * 2,
        scratch_shapes=[
            pltpu.VMEM(edges.shape[1:], f32),
            pltpu.VMEM(edges.shape[1:], f32),
            pltpu.VMEM((3, wide_x - 2 * HALO, RIM, extent_z), f32),
            pltpu.VMEM((3, wide_x - 2 * HALO, RIM, extent_z), f32),
            pltpu.VMEM(corner, f32),
            pltpu.VMEM(corner, f32),
            pltpu.VMEM((columns, rows) + tile.shape, f32),
            pltpu.VMEM(frame, f32),
            pltpu.VMEM(frame, f32),
            pltpu.VMEM(frame, f32),
            pltpu.VMEM((2, wide_y, extent_z), f32),
            dma,
            dma((24,)),
            dma((24,)),
            dma((rows - 1,)),
            dma((rows - 1,)),
            dma((columns - 1,)),
            dma((columns - 1,)),
        ],
        compiler_params=pltpu.CompilerParams(
            collective_id=1, has_side_effects=True, vmem_limit_bytes=56 * 2**20
        ),
        name="tail",
    )(spread, edges, tile, matrix, contact_sphere, contact_partner)


def on_device(
    velocity,
    owner_block,
    base_x,
    base_y,
    base_z,
    delta_weights,
    marker_offset,
    sphere_motion,
    contact_sphere,
    contact_partner,
):
    span_y = velocity.shape[2]
    markers = base_x.shape[0]
    spheres = sphere_motion.shape[1]
    bases = [base.reshape(1, markers) for base in (base_x, base_y, base_z)]
    owners = owner_block.reshape(1, markers)
    motion = sphere_motion.T
    home, arrived, *halos = front(owners, bases, delta_weights, marker_offset, motion, velocity)
    spread, edges, tile = markers_stage(spheres, velocity, halos, home, arrived, motion)
    columns, rows = lax.axis_size("gx"), lax.axis_size("gy")
    matrix = jnp.asarray(combine_matrix(columns, rows, markers // spheres))
    state, moved = tail(
        spread, edges, tile, matrix, contact_sphere, contact_partner, span_y, spheres
    )
    return state, moved.T


def solution(mesh):
    placed = (
        P(None, "gx", "gy", None),
        P(("gx", "gy"), None),
        P(("gx", "gy")),
        P(("gx", "gy")),
        P(("gx", "gy")),
        P(None, ("gx", "gy")),
        P(None, ("gx", "gy")),
        P(None, ("gx", "gy")),
        P(("gx", "gy")),
        P(("gx", "gy")),
    )
    return jax.shard_map(
        on_device,
        mesh=mesh,
        in_specs=placed,
        out_specs=(P(None, "gx", "gy", None), P(None, ("gx", "gy"))),
        check_vma=False,
    )
```

```python
import functools
import math

import jax
import jax.numpy as jnp
import numpy as np
from jax import lax
from jax.experimental import pallas as pl
from jax.experimental.pallas import tpu as pltpu
from jax.sharding import PartitionSpec as P

ITERS = 4
DIFFUSION = 1.0
RESPONSE = 0.5
DASHPOT = 0.1

MESH = pl.DeviceIdType.MESH
TILE_ROWS = 16
TILE_LANES = 128
CHUNK = 256
WINDOW = 8
GROUP = 6
RECORD = 24
X_ROW, Y_ROW, Z_ROW, TARGET, OFFSET, SPHERE, LIVE = 12, 13, 14, 15, 18, 21, 22
DIRECTIONS = ((-1, -1), (-1, 0), (-1, 1), (0, -1), (0, 1), (1, -1), (1, 0), (1, 1))
HALO = 2
RIM = 8


def when(condition, body):
    if condition is True:
        body()
    else:
        pl.when(condition)(body)


def exists(row, rows, dy):
    if dy == 0:
        return True
    return row + dy < rows if dy > 0 else row + dy >= 0


def greet(columns, rows, column, row):
    barrier = pltpu.get_barrier_semaphore()
    for dx, dy in DIRECTIONS:
        peer = (lax.rem(column + dx + columns, columns), row + dy)
        when(
            exists(row, rows, dy),
            lambda peer=peer: pl.semaphore_signal(
                barrier, inc=1, device_id=peer, device_id_type=MESH
            ),
        )
    return barrier


def greeted(rows, row):
    inner = lax.min(row, 1) + lax.min(rows - 1 - row, 1)
    return 2 + 3 * inner


def remote(src, dst, send, recv, k, peer):
    return pltpu.make_async_remote_copy(
        src_ref=src,
        dst_ref=dst,
        send_sem=send.at[k],
        recv_sem=recv.at[k],
        device_id=peer,
        device_id_type=MESH,
    )


def split(value):
    high = value.astype(jnp.bfloat16).astype(jnp.float32)
    return high, value - high


def upper_triangle():
    rows = lax.broadcasted_iota(jnp.int32, (CHUNK, CHUNK), 0)
    lanes = lax.broadcasted_iota(jnp.int32, (CHUNK, CHUNK), 1)
    return (rows <= lanes).astype(jnp.float32).astype(jnp.bfloat16)


def ranks(categories, count):
    rows = lax.broadcasted_iota(jnp.int32, (count, CHUNK), 0).astype(jnp.float32)
    hot = [(rows == block).astype(jnp.float32) for block in categories]
    stacked = jnp.concatenate(hot, axis=0).astype(jnp.bfloat16)
    inside = jnp.dot(stacked, upper_triangle(), preferred_element_type=jnp.float32)
    carry = jnp.zeros((count, 1), jnp.float32)
    upto = []
    for b in range(len(hot)):
        block = inside[b * count : (b + 1) * count]
        upto.append(block + carry)
        carry = carry + block[:, CHUNK - 1 : CHUNK]
    return hot, upto, carry


def place(parts, where_to, groups):
    group = jnp.floor(where_to * (1.0 / CHUNK))
    slot = where_to - group * CHUNK
    rows = lax.broadcasted_iota(jnp.int32, (CHUNK, where_to.shape[1]), 0).astype(jnp.float32)
    hot = (rows == slot).astype(jnp.float32).astype(jnp.bfloat16)
    masked = [parts * (group == g).astype(jnp.float32) for g in groups]
    masked = jnp.concatenate(masked, axis=0).astype(jnp.bfloat16)
    moved = lax.dot_general(
        masked, hot, (((1,), (1,)), ((), ())), preferred_element_type=jnp.float32
    )
    result = []
    for n in range(len(groups)):
        piece = moved[2 * RECORD * n : 2 * RECORD * (n + 1)]
        result.append(piece[:RECORD] + piece[RECORD:])
    return result


def front_kernel(
    columns, rows, *refs
):
    inputs, refs = refs[:8], refs[8:]
    staged, load = refs[-9:-1], refs[-1]
    loads = [
        pltpu.make_async_copy(src, dst, load.at[n])
        for n, (src, dst) in enumerate(zip(inputs, staged))
    ]
    for copy in loads:
        copy.start()
    front_body(columns, rows, loads, *staged, *refs[:-9])


def front_body(
    columns, rows, loads, owners, base_x, base_y, base_z, weights, offsets, motion, velocity,
    placed, alive, high, low, spread,
    home, slots, arrived, left, right, below, above, corners, parts, send, recv,
):
    column = lax.axis_index("gx")
    row = lax.axis_index("gy")
    span_x, span_y, extent_z = velocity.shape[1:]
    wide_y = span_y + 2 * ITERS
    lanes = len(DIRECTIONS)
    f32, bf16 = jnp.float32, jnp.bfloat16
    barrier = greet(columns, rows, column, row)

    def peer(dx, dy):
        return (lax.rem(column + dx + columns, columns), row + dy)

    edge = [(slots.at[g], arrived.at[g], dx, dy) for g, (dx, dy) in enumerate(DIRECTIONS)]
    rims = (slice(0, RIM), slice(span_y - RIM, span_y))
    for at in rims + (slice(RIM, span_y - RIM),):
        edge.append((velocity.at[:, 0:HALO, at], right.at[:, :, at], -1, 0))
        edge.append((velocity.at[:, span_x - HALO : span_x, at], left.at[:, :, at], 1, 0))
    edge.append((velocity.at[:, :, rims[0]], above, 0, -1))
    edge.append((velocity.at[:, :, rims[1]], below, 0, 1))
    for side, halo in enumerate((left, right)):
        edge.append((halo.at[:, :, rims[0]], corners.at[2 + side], 0, -1))
        edge.append((halo.at[:, :, rims[1]], corners.at[side], 0, 1))

    def start(k):
        src, dst, dx, dy = edge[k]
        when(
            exists(row, rows, dy),
            lambda: remote(src, dst, send, recv, k, peer(dx, dy)).start(),
        )

    def arrive(k):
        src, dst, dx, dy = edge[k]
        when(
            exists(row, rows, -dy),
            lambda: remote(src, dst, send, recv, k, peer(dx, dy)).wait_recv(),
        )

    def sent(k):
        src, dst, dx, dy = edge[k]
        when(
            exists(row, rows, dy),
            lambda: remote(src, dst, send, recv, k, peer(dx, dy)).wait_send(),
        )

    @pl.when(row == 0)
    def _():
        below[...] = jnp.zeros(below.shape, f32)
        for n in (0, 1):
            corners[n] = jnp.zeros(corners.shape[1:], f32)
        for g, (dx, dy) in enumerate(DIRECTIONS):
            if dy > 0:
                arrived[g] = jnp.zeros(arrived.shape[1:], f32)

    @pl.when(row == rows - 1)
    def _():
        above[...] = jnp.zeros(above.shape, f32)
        for n in (2, 3):
            corners[n] = jnp.zeros(corners.shape[1:], f32)
        for g, (dx, dy) in enumerate(DIRECTIONS):
            if dy < 0:
                arrived[g] = jnp.zeros(arrived.shape[1:], f32)

    for copy in loads[:7]:
        copy.wait()
    markers = owners.shape[1]
    spheres = motion.shape[0]
    per_sphere = markers // spheres
    owner = owners[...].astype(f32)
    owner_x = jnp.floor((owner + 0.5) * (1.0 / rows))
    owner_y = owner - owner_x * rows
    step_x = owner_x - column.astype(f32)
    step_x = jnp.where(step_x > 1.5, step_x - columns, step_x)
    step_x = jnp.where(step_x < -1.5, step_x + columns, step_x)
    step_y = owner_y - row.astype(f32)
    lane = (step_x + 1.0) * 3.0 + step_y + 1.0
    at_home = lane == 4.0
    lane = jnp.where(at_home, -1.0, jnp.where(lane > 4.0, lane - 1.0, lane))
    offset = offsets[...]
    targets = []
    for s in range(spheres):
        o = offset[:, s * per_sphere : (s + 1) * per_sphere]
        m = [motion[s : s + 1, c : c + 1] for c in range(6)]
        targets.append(
            jnp.concatenate(
                [
                    m[0] + (m[4] * o[2:3] - m[5] * o[1:2]),
                    m[1] + (m[5] * o[0:1] - m[3] * o[2:3]),
                    m[2] + (m[3] * o[1:2] - m[4] * o[0:1]),
                ],
                axis=0,
            )
        )
    home[0:12] = weights[...]
    for line, base in ((X_ROW, base_x), (Y_ROW, base_y), (Z_ROW, base_z)):
        home[line : line + 1] = base[...].astype(f32)
    home[TARGET : TARGET + 3] = jnp.concatenate(targets, axis=1)
    home[OFFSET : OFFSET + 3] = offset
    position = lax.broadcasted_iota(jnp.int32, (1, markers), 1)
    sphere = jnp.zeros((1, markers), f32)
    for s in range(1, spheres):
        sphere = sphere + (position >= s * per_sphere).astype(f32)
    home[SPHERE : SPHERE + 1] = sphere
    home[LIVE : LIVE + 1] = jnp.ones((1, markers), f32)
    home[LIVE + 1 : LIVE + 2] = jnp.zeros((1, markers), f32)

    blocks = markers // CHUNK
    hot, upto, totals = ranks([lane[:, b * CHUNK : (b + 1) * CHUNK] for b in range(blocks)], lanes)
    rank = [jnp.sum(h * (u - 1.0), axis=0, keepdims=True) for h, u in zip(hot, upto)]
    where_to = jnp.concatenate(rank, axis=1) + lane * CHUNK
    where_to = jnp.where(at_home, -1.0, where_to)
    pair = jnp.concatenate(split(home[...]), axis=0)
    for g, piece in enumerate(place(pair, where_to, range(lanes))):
        slots[g] = piece
    home[LIVE : LIVE + 1] = at_home.astype(f32)

    loads[7].wait()
    pl.semaphore_wait(barrier, greeted(rows, row))
    for k in range(len(edge) - 4):
        start(k)

    for k in range(lanes):
        arrive(k)
    total = blocks + lanes
    count = -(-(span_x + 1) // 8) * 8
    categories = []
    living = []
    for b in range(total):
        at = slice(b * CHUNK, (b + 1) * CHUNK)
        if b < blocks:
            record = home[:, at]
            group = lanes + record[SPHERE : SPHERE + 1] * (lanes + 1)
        else:
            record = arrived[b - blocks]
            group = (b - blocks) + record[SPHERE : SPHERE + 1] * (lanes + 1)
        lives = record[LIVE : LIVE + 1] > 0.5
        living.append(lives)
        categories.append(jnp.where(lives, record[X_ROW : X_ROW + 1], -1.0))
        first, rest = split(record)
        parts[0:RECORD, at] = first
        parts[RECORD : 2 * RECORD, at] = rest
        parts[SPHERE : SPHERE + 1, at] = group
    hot, upto, totals = ranks(categories, count)
    lower_rows = lax.broadcasted_iota(jnp.int32, (count, count), 0)
    lower_lanes = lax.broadcasted_iota(jnp.int32, (count, count), 1)
    before = (lower_lanes < lower_rows).astype(f32)
    wide = jnp.broadcast_to(totals, (count, TILE_LANES))
    starts = jnp.dot(
        before, wide, precision=lax.Precision.HIGHEST, preferred_element_type=f32
    )[:, 0:1]
    places = []
    for b in range(total):
        rank = jnp.sum(hot[b] * (upto[b] + (starts - 1.0)), axis=0, keepdims=True)
        places.append(jnp.where(living[b], rank, -1.0))
    where_to = jnp.concatenate(places, axis=1)
    alive[...] = jnp.broadcast_to(jnp.sum(wide, axis=0, keepdims=True), alive.shape)
    for first in range(0, total, GROUP):
        groups = range(first, min(first + GROUP, total))
        for g, piece in zip(groups, place(parts[...], where_to, groups)):
            placed[g] = piece

    def layer(x, row_source, below_source, above_source, own):
        for c in range(3):
            lines = row_source(c)
            margin = jnp.zeros((HALO, extent_z), f32)
            value = jnp.concatenate(
                [
                    margin,
                    below_source(c)[RIM - HALO : RIM],
                    lines,
                    above_source(c)[0:HALO],
                    margin,
                ],
                axis=0,
            )
            at = slice(wide_y * c, wide_y * (c + 1))
            first, rest = split(value)
            high[x, at] = first.astype(bf16)
            low[x, at] = rest.astype(bf16)
            if own:
                margin = jnp.zeros((ITERS, extent_z), f32)
                spread[x + HALO, at] = jnp.concatenate([margin, lines, margin], axis=0)
        end = jnp.zeros((high.shape[1] - 3 * wide_y, extent_z), bf16)
        high[x, 3 * wide_y :] = end
        low[x, 3 * wide_y :] = end

    arrive(len(edge) - 6)
    arrive(len(edge) - 5)

    def inner(x, carry):
        layer(
            x + HALO,
            lambda c: velocity[c, x],
            lambda c: below[c, x],
            lambda c: above[c, x],
            True,
        )
        return carry

    for k in range(lanes, lanes + 4):
        arrive(k)
    for k in range(len(edge) - 4, len(edge)):
        start(k)
    lax.fori_loop(0, span_x, inner, 0)
    for x in range(ITERS):
        spread[x] = jnp.zeros(spread.shape[1:], f32)
        spread[span_x + ITERS + x] = jnp.zeros(spread.shape[1:], f32)
    arrive(lanes + 4)
    arrive(lanes + 5)
    for k in range(len(edge) - 4, len(edge)):
        arrive(k)
    for side, halo in enumerate((left, right)):
        for x in range(HALO):
            layer(
                x + side * (span_x + HALO),
                lambda c: halo[c, x],
                lambda c: corners[side, c, x],
                lambda c: corners[2 + side, c, x],
                False,
            )
    for k in range(len(edge)):
        sent(k)


def front(owners, bases, weights, offsets, motion, velocity):
    columns, rows = lax.axis_size("gx"), lax.axis_size("gy")
    span_x, span_y, extent_z = velocity.shape[1:]
    wide_y = span_y + 2 * ITERS
    markers = owners.shape[1]
    lanes = len(DIRECTIONS)
    f32, bf16 = jnp.float32, jnp.bfloat16
    copies = lanes + 12
    inputs = (owners, *bases, weights, offsets, motion, velocity)
    total = markers // CHUNK + lanes
    field = (span_x + 2 * HALO, -(-3 * wide_y // 16) * 16, extent_z)
    vmem = pl.BlockSpec(memory_space=pltpu.VMEM)
    out = [
        pltpu.VMEM((total, RECORD, CHUNK), f32),
        pltpu.VMEM((8, TILE_LANES), f32),
        pltpu.VMEM(field, bf16),
        pltpu.VMEM(field, bf16),
        pltpu.VMEM((span_x + 2 * ITERS, 3 * wide_y, extent_z), f32),
    ]
    room = 67_043_328 - sum(math.prod(ref.shape) * ref.dtype.itemsize for ref in out) - 2**15
    return pl.pallas_call(
        functools.partial(front_kernel, columns, rows),
        out_shape=out,
        in_specs=[pl.BlockSpec(memory_space=pltpu.HBM)] * 8,
        out_specs=[vmem] * len(out),
        scratch_shapes=[
            pltpu.VMEM((RECORD, markers), f32),
            pltpu.VMEM((lanes, RECORD, CHUNK), f32),
            pltpu.VMEM((lanes, RECORD, CHUNK), f32),
            pltpu.VMEM((3, HALO, span_y, extent_z), f32),
            pltpu.VMEM((3, HALO, span_y, extent_z), f32),
            pltpu.VMEM((3, span_x, RIM, extent_z), f32),
            pltpu.VMEM((3, span_x, RIM, extent_z), f32),
            pltpu.VMEM((4, 3, HALO, RIM, extent_z), f32),
            pltpu.VMEM((2 * RECORD, total * CHUNK), f32),
            pltpu.SemaphoreType.DMA((copies,)),
            pltpu.SemaphoreType.DMA((copies,)),
        ]
        + [pltpu.VMEM(array.shape, array.dtype) for array in inputs]
        + [pltpu.SemaphoreType.DMA((len(inputs),))],
        compiler_params=pltpu.CompilerParams(
            collective_id=0, has_side_effects=True, vmem_limit_bytes=room
        ),
        name="front",
    )(*inputs)


def four(distance, weights):
    value = jnp.where(distance == 3.0, weights[3:4], 0.0)
    for n in (2, 1, 0):
        value = jnp.where(distance == float(n), weights[n : n + 1], value)
    return value


def markers_kernel(
    spheres, span_y, sorted_refs, alive_ref, high, low, frame, motion, spread, edges, tile, sums
):
    layers, _, extent_z = high.shape
    span_x = layers - 2 * HALO
    wide_y = span_y + 2 * ITERS
    lanes = len(DIRECTIONS)
    bf16, f32 = jnp.bfloat16, jnp.float32
    alive_count = jnp.max(alive_ref[0:1, :]).astype(jnp.int32)

    sums[...] = jnp.zeros(sums.shape, f32)
    z_cells = lax.broadcasted_iota(jnp.int32, (extent_z, CHUNK), 0).astype(f32)
    y_cells = lax.broadcasted_iota(jnp.int32, (wide_y, CHUNK), 0).astype(f32) - HALO
    x_cells = lax.broadcasted_iota(jnp.int32, (WINDOW, CHUNK), 0).astype(f32)

    def chunk(j, carry):
        record = sorted_refs[j]
        alive = record[LIVE : LIVE + 1]
        cell_x = record[X_ROW : X_ROW + 1]
        distance = z_cells - record[Z_ROW : Z_ROW + 1]
        distance = jnp.where(distance < 0.0, distance + extent_z, distance)
        z_high, z_low = split(four(distance, record[8:12]))
        z_high = z_high.astype(bf16)
        z_low = z_low.astype(bf16)
        y_table = four(y_cells - record[Y_ROW : Y_ROW + 1], record[4:8])
        least = jnp.min(jnp.where(alive > 0.5, cell_x, 1e4)).astype(jnp.int32)
        most = jnp.max(jnp.where(alive > 0.5, cell_x, -1.0)).astype(jnp.int32)
        windows = (most + 4 - least + WINDOW - 1) // WINDOW

        def x_table(k):
            fresh = least + WINDOW * k
            base = jnp.minimum(fresh, layers - WINDOW)
            cells = x_cells + base.astype(f32)
            table = four(cells - cell_x, record[0:4])
            return base, jnp.where(cells >= fresh.astype(f32), table, 0.0)

        z_stack = jnp.concatenate([z_high, z_high, z_low], axis=0)

        def sample(k, total):
            base, table = x_table(k)
            rows = high.shape[1]
            first = high[pl.ds(base, WINDOW)].reshape(WINDOW * rows, extent_z)
            rest = low[pl.ds(base, WINDOW)].reshape(WINDOW * rows, extent_z)
            lines = jnp.dot(
                jnp.concatenate([first, rest, first], axis=1),
                z_stack,
                preferred_element_type=f32,
            )
            for x in range(WINDOW):
                total = total + lines[x * rows : x * rows + 3 * wide_y] * table[x : x + 1]
            return total

        plane = lax.fori_loop(0, windows, sample, jnp.zeros((3 * wide_y, CHUNK), f32))
        forces = []
        for c in range(3):
            got = jnp.sum(plane[c * wide_y : (c + 1) * wide_y] * y_table, axis=0, keepdims=True)
            forces.append((record[TARGET + c : TARGET + c + 1] - got) * alive)
        sheet = jnp.concatenate([force * y_table for force in forces], axis=0)
        z_wide = jnp.concatenate([z_high, z_high, z_low], axis=1)

        def deposit(k, carry):
            base, table = x_table(k)
            value = jnp.concatenate([sheet * table[x : x + 1] for x in range(WINDOW)], axis=0)
            first, rest = split(value)
            first = first.astype(bf16)
            rest = rest.astype(bf16)
            added = lax.dot_general(
                jnp.concatenate([first, rest, first], axis=1),
                z_wide,
                (((1,), (1,)), ((), ())),
                preferred_element_type=f32,
            )
            at = pl.ds(base + HALO, WINDOW)
            spread[at] = spread[at] + added.reshape(WINDOW, 3 * wide_y, extent_z)
            return carry

        lax.fori_loop(0, windows, deposit, 0)
        o = [record[OFFSET + c : OFFSET + c + 1] for c in range(3)]
        f = forces
        moments = jnp.concatenate(
            f
            + [
                o[1] * f[2] - o[2] * f[1],
                o[2] * f[0] - o[0] * f[2],
                o[0] * f[1] - o[1] * f[0],
                jnp.zeros((2, CHUNK), f32),
            ],
            axis=0,
        )
        group = record[SPHERE : SPHERE + 1]
        for g in range((lanes + 1) * spheres):
            sums[g] = sums[g] + jnp.where(group == float(g), moments, 0.0)
        return carry

    chunks = (alive_count + (CHUNK - 1)) // CHUNK
    lax.fori_loop(0, chunks, chunk, 0)
    columns = jnp.sum(sums[...], axis=2)
    tile[...] = jnp.zeros(tile.shape, f32)
    for s in range(spheres):
        at = slice(6 * s, 6 * (s + 1))
        tile[0 : lanes + 1, at] = columns[(lanes + 1) * s : (lanes + 1) * (s + 1), 0:6]
        tile[lanes + 1 : lanes + 2, at] = motion[s : s + 1]
    reach = ITERS + HALO
    depth = span_y + 2 * HALO
    for side, first in enumerate((span_x, HALO)):
        for c in range(3):
            for x in range(reach):
                edges[side, c, depth * x : depth * (x + 1)] = spread[
                    first + x, wide_y * c + HALO : wide_y * (c + 1) - HALO
                ]


def markers_stage(spheres, span_y, placed, alive, high, low, frame, motion):
    wide_x, lines, extent_z = frame.shape
    lanes = len(DIRECTIONS)
    f32 = jnp.float32
    groups = (lanes + 1) * spheres
    vmem = pl.BlockSpec(memory_space=pltpu.VMEM)
    return pl.pallas_call(
        functools.partial(markers_kernel, spheres, span_y),
        out_shape=[
            pltpu.VMEM(frame.shape, f32),
            pltpu.VMEM((2, 3, (ITERS + HALO) * (span_y + 2 * HALO), extent_z), f32),
            jax.ShapeDtypeStruct((TILE_ROWS, TILE_LANES), f32),
        ],
        in_specs=[vmem] * 6,
        out_specs=[vmem] * 3,
        scratch_shapes=[pltpu.VMEM((groups, 8, CHUNK), f32)],
        input_output_aliases={4: 0},
        compiler_params=pltpu.CompilerParams(vmem_limit_bytes=40 * 2**20),
        name="markers",
    )(placed, alive, high, low, frame, motion)


def combine_matrix(columns, rows, per_sphere):
    matrix = np.zeros((columns, rows, columns, rows, TILE_ROWS), np.float32)
    for i in range(columns):
        for j in range(rows):
            for slot, (dx, dy) in enumerate(DIRECTIONS):
                if 0 <= j - dy < rows:
                    matrix[(i - dx) % columns, j - dy, i, j, slot] -= RESPONSE / per_sphere
            matrix[i, j, i, j, len(DIRECTIONS)] -= RESPONSE / per_sphere
            matrix[i, j, i, j, len(DIRECTIONS) + 1] = 1.0
    return matrix.reshape(columns * rows, -1)


def tail_kernel(
    columns, rows, spread, edges, tile, matrix, contact_sphere, contact_partner,
    out, motion_out, from_left, from_right, from_below, from_above, given, corners, held,
    rhs, one, two, mask_ref, own_sem, send, recv, row_send, row_recv, col_send, col_recv,
):
    column = lax.axis_index("gx")
    row = lax.axis_index("gy")
    span_x, span_y, extent_z = out.shape[1:]
    wide_x, wide_y = span_x + 2 * ITERS, span_y + 2 * ITERS
    reach = ITERS + HALO
    depth = span_y + 2 * HALO
    row_peers = [lax.rem(row + k, rows) for k in range(1, rows)]
    column_peers = [lax.rem(column + k, columns) for k in range(1, columns)]
    barrier = pltpu.get_barrier_semaphore()
    for other in row_peers:
        pl.semaphore_signal(barrier, inc=1, device_id=(column, other), device_id_type=MESH)
    for other in column_peers:
        pl.semaphore_signal(barrier, inc=1, device_id=(other, row), device_id_type=MESH)
    own = pltpu.make_async_copy(tile, held.at[column, row], own_sem)
    own.start()

    def peer(dx, dy):
        return (lax.rem(column + dx + columns, columns), row + dy)

    edge = []
    for c in range(3):
        low, high = wide_y * c, wide_y * (c + 1)
        inner = slice(HALO, wide_x - HALO)
        edge += [
            (edges.at[0, c], from_left.at[c], 1, 0),
            (edges.at[1, c], from_right.at[c], -1, 0),
            (spread.at[inner, high - RIM : high], from_below.at[c], 0, 1),
            (spread.at[inner, low : low + RIM], from_above.at[c], 0, -1),
            (given.at[c, 0], corners.at[c, 0], 0, 1),
            (given.at[c, 1], corners.at[c, 1], 0, 1),
            (given.at[c, 2], corners.at[c, 2], 0, -1),
            (given.at[c, 3], corners.at[c, 3], 0, -1),
        ]

    def start(k):
        src, dst, dx, dy = edge[k]
        when(
            exists(row, rows, dy),
            lambda: remote(src, dst, send, recv, k, peer(dx, dy)).start(),
        )

    def arrive(k):
        src, dst, dx, dy = edge[k]
        when(
            exists(row, rows, -dy),
            lambda: remote(src, dst, send, recv, k, peer(dx, dy)).wait_recv(),
        )

    def sent(k):
        src, dst, dx, dy = edge[k]
        when(
            exists(row, rows, dy),
            lambda: remote(src, dst, send, recv, k, peer(dx, dy)).wait_send(),
        )

    @pl.when(row == 0)
    def _():
        from_below[...] = jnp.zeros(from_below.shape, jnp.float32)
        for c in range(3):
            corners[c, 0:2] = jnp.zeros((2,) + corners.shape[2:], jnp.float32)

    @pl.when(row == rows - 1)
    def _():
        from_above[...] = jnp.zeros(from_above.shape, jnp.float32)
        for c in range(3):
            corners[c, 2:4] = jnp.zeros((2,) + corners.shape[2:], jnp.float32)

    pl.semaphore_wait(barrier, rows + columns - 2)
    first = [
        pltpu.make_async_remote_copy(
            src_ref=tile,
            dst_ref=held.at[column, row],
            send_sem=row_send.at[k],
            recv_sem=row_recv.at[k],
            device_id=(column, other),
            device_id_type=MESH,
        )
        for k, other in enumerate(row_peers)
    ]
    for copy in first:
        copy.start()
    for k in range(4):
        start(k)
    for c in range(1, 3):
        for k in range(2, 4):
            start(8 * c + k)

    cells = lax.broadcasted_iota(jnp.int32, (wide_y, extent_z), 0) + (row * span_y - ITERS)
    inside = jnp.logical_and(cells >= 0, cells < span_y * rows)
    inverse = 1.0 / (1.0 + 6.0 * DIFFUSION)
    mask_ref[0] = inside.astype(jnp.float32)
    mask_ref[1] = inside.astype(jnp.float32) * inverse

    own.wait()
    for copy in first:
        copy.wait()
    second = [
        pltpu.make_async_remote_copy(
            src_ref=held.at[column],
            dst_ref=held.at[column],
            send_sem=col_send.at[k],
            recv_sem=col_recv.at[k],
            device_id=(other, row),
            device_id_type=MESH,
        )
        for k, other in enumerate(column_peers)
    ]
    for copy in second:
        copy.start()
    for c in range(1, 3):
        for k in range(2):
            start(8 * c + k)

    def relaxed(c, source, x):
        here = source[c, x]
        beside = source[c, x - 1] + source[c, x + 1]
        beside = beside + pltpu.roll(here, 1, 0) + pltpu.roll(here, wide_y - 1, 0)
        beside = beside + pltpu.roll(here, 1, 1) + pltpu.roll(here, extent_z - 1, 1)
        return (rhs[c, x] + DIFFUSION * beside) * mask_ref[1]

    buffers = (rhs, one, two, one)

    def sweeps(c, starts, length):
        for sweep in range(ITERS):
            source = buffers[sweep]
            for first, shift in starts:
                begin = first + sweep * shift
                for x in range(begin, begin + length(sweep)):
                    new = relaxed(c, source, x)
                    if sweep == ITERS - 1:
                        out[c, x - ITERS] = new[ITERS : ITERS + span_y]
                    else:
                        buffers[sweep + 1][c, x] = new

    def base(c, carry):
        for x in range(wide_x):
            rhs[c, x] = spread[x, pl.ds(pl.multiple_of(wide_y * c, 8), wide_y)]
        for x in range(wide_x - 2 * HALO):
            y = x + HALO
            rhs[c, y, 0:RIM] = rhs[c, y, 0:RIM] + from_below[c, x]
            rhs[c, y, wide_y - RIM :] = rhs[c, y, wide_y - RIM :] + from_above[c, x]
        for x in range(reach, wide_x - reach):
            rhs[c, x] = rhs[c, x] * mask_ref[0]
        sweeps(c, ((reach + 1, 1),), lambda sweep: span_x - 2 * HALO - 2 - 2 * sweep)
        return carry

    for c in range(3):
        arrive(8 * c + 2)
        arrive(8 * c + 3)
    lax.fori_loop(0, 3, base, 0)

    def outer(c):
        for x in range(reach):
            for side, y in enumerate((x, x + span_x + HALO)):
                at = slice(6 * x, 6 * (x + 1))
                rhs[c, y, 0:6] = rhs[c, y, 0:6] + corners[c, side, at]
                rhs[c, y, wide_y - 6 :] = rhs[c, y, wide_y - 6 :] + corners[c, 2 + side, at]
                rhs[c, y] = rhs[c, y] * mask_ref[0]
        sweeps(c, ((1, 1), (span_x + 1, -1)), lambda sweep: reach)

    for c in range(3):
        arrive(8 * c)
        arrive(8 * c + 1)
        for side, halo in enumerate((from_left, from_right)):
            for up, first in ((0, depth - reach), (2, 0)):
                pieces = [
                    halo[c, depth * x + first : depth * x + first + reach] for x in range(reach)
                ]
                given[c, up + side, 0 : reach * reach] = jnp.concatenate(pieces, axis=0)
        for x in range(reach):
            for halo, y in ((from_left, x), (from_right, x + span_x + HALO)):
                rhs[c, y, HALO : wide_y - HALO] = (
                    rhs[c, y, HALO : wide_y - HALO] + halo[c, depth * x : depth * (x + 1)]
                )
        for k in range(4, 8):
            start(8 * c + k)
        for k in range(4, 8):
            arrive(8 * c + k)
        outer(c)

    for copy in second:
        copy.wait()
    gathered = held[...].reshape(-1, TILE_LANES)
    moved = jnp.dot(
        matrix[...],
        gathered,
        precision=lax.Precision.HIGHEST,
        preferred_element_type=jnp.float32,
    )
    spheres = motion_out.shape[0]
    device = lax.broadcasted_iota(jnp.int32, (1, columns * rows), 1)
    here = column * rows + row
    linked, owned = [], []
    for s in range(spheres):
        mine = here * spheres + s
        for other in range(spheres):
            own_row = (device * spheres + other == mine).astype(jnp.float32)
            line = own_row
            for k in range(contact_sphere.shape[0]):
                acts = contact_sphere[k] == mine
                partner = (device * spheres + other == contact_partner[k]).astype(jnp.float32)
                line = line + jnp.where(acts, DASHPOT * (partner - own_row), 0.0)
            linked.append(line)
            owned.append(own_row)
    links = jnp.concatenate(linked + owned, axis=0)
    result = jnp.dot(
        links, moved, precision=lax.Precision.HIGHEST, preferred_element_type=jnp.float32
    )
    for s in range(spheres):
        for part in range(2):
            total = 0.0
            for other in range(spheres):
                line = (part * spheres + s) * spheres + other
                at = 6 * other + 3 * part
                total = total + result[line : line + 1, at : at + 3]
            motion_out[s : s + 1, 3 * part : 3 * part + 3] = total
    for k in range(len(edge)):
        sent(k)


def tail(spread, edges, tile, matrix, contact_sphere, contact_partner, span_y, spheres):
    columns, rows = lax.axis_size("gx"), lax.axis_size("gy")
    wide_x, _, extent_z = spread.shape
    span_x = wide_x - 2 * ITERS
    wide_y = span_y + 2 * ITERS
    reach = ITERS + HALO
    f32 = jnp.float32
    vmem = pl.BlockSpec(memory_space=pltpu.VMEM)
    smem = pl.BlockSpec(memory_space=pltpu.SMEM)
    dma = pltpu.SemaphoreType.DMA
    corner = (3, 4, -(-reach * reach // 8) * 8, extent_z)
    frame = (3, wide_x, wide_y, extent_z)
    return pl.pallas_call(
        functools.partial(tail_kernel, columns, rows),
        out_shape=[
            pltpu.VMEM((3, span_x, span_y, extent_z), f32),
            jax.ShapeDtypeStruct((spheres, 6), f32),
        ],
        in_specs=[vmem] * 4 + [smem] * 2,
        out_specs=[vmem] * 2,
        scratch_shapes=[
            pltpu.VMEM(edges.shape[1:], f32),
            pltpu.VMEM(edges.shape[1:], f32),
            pltpu.VMEM((3, wide_x - 2 * HALO, RIM, extent_z), f32),
            pltpu.VMEM((3, wide_x - 2 * HALO, RIM, extent_z), f32),
            pltpu.VMEM(corner, f32),
            pltpu.VMEM(corner, f32),
            pltpu.VMEM((columns, rows) + tile.shape, f32),
            pltpu.VMEM(frame, f32),
            pltpu.VMEM(frame, f32),
            pltpu.VMEM(frame, f32),
            pltpu.VMEM((2, wide_y, extent_z), f32),
            dma,
            dma((24,)),
            dma((24,)),
            dma((rows - 1,)),
            dma((rows - 1,)),
            dma((columns - 1,)),
            dma((columns - 1,)),
        ],
        compiler_params=pltpu.CompilerParams(
            collective_id=1, has_side_effects=True, vmem_limit_bytes=40 * 2**20
        ),
        name="tail",
    )(spread, edges, tile, matrix, contact_sphere, contact_partner)


def on_device(
    velocity,
    owner_block,
    base_x,
    base_y,
    base_z,
    delta_weights,
    marker_offset,
    sphere_motion,
    contact_sphere,
    contact_partner,
):
    span_y = velocity.shape[2]
    markers = base_x.shape[0]
    spheres = sphere_motion.shape[1]
    bases = [base.reshape(1, markers) for base in (base_x, base_y, base_z)]
    owners = owner_block.reshape(1, markers)
    motion = sphere_motion.T
    staged = front(owners, bases, delta_weights, marker_offset, motion, velocity)
    spread, edges, tile = markers_stage(spheres, span_y, *staged, motion)
    columns, rows = lax.axis_size("gx"), lax.axis_size("gy")
    matrix = jnp.asarray(combine_matrix(columns, rows, markers // spheres))
    state, moved = tail(
        spread, edges, tile, matrix, contact_sphere, contact_partner, span_y, spheres
    )
    return state, moved.T


def solution(mesh):
    placed = (
        P(None, "gx", "gy", None),
        P(("gx", "gy"), None),
        P(("gx", "gy")),
        P(("gx", "gy")),
        P(("gx", "gy")),
        P(None, ("gx", "gy")),
        P(None, ("gx", "gy")),
        P(None, ("gx", "gy")),
        P(("gx", "gy")),
        P(("gx", "gy")),
    )
    return jax.shard_map(
        on_device,
        mesh=mesh,
        in_specs=placed,
        out_specs=(P(None, "gx", "gy", None), P(None, ("gx", "gy"))),
        check_vma=False,
    )
```

```python
import functools
import math

import jax
import jax.numpy as jnp
import numpy as np
from jax import lax
from jax.experimental import pallas as pl
from jax.experimental.pallas import tpu as pltpu
from jax.sharding import PartitionSpec as P

ITERS = 4
DIFFUSION = 1.0
RESPONSE = 0.5
DASHPOT = 0.1

MESH = pl.DeviceIdType.MESH
TILE_LANES = 128
CHUNK = 256
WINDOW = 8
GROUP = 6
RECORD = 24
X_ROW, Y_ROW, Z_ROW, TARGET, OFFSET, SPHERE, LIVE = 12, 13, 14, 15, 18, 21, 22
DIRECTIONS = ((-1, -1), (-1, 0), (-1, 1), (0, -1), (0, 1), (1, -1), (1, 0), (1, 1))
HALO = 2
RIM = 8


def when(condition, body):
    if condition is True:
        body()
    else:
        pl.when(condition)(body)


def exists(row, rows, dy):
    if dy == 0:
        return True
    return row + dy < rows if dy > 0 else row + dy >= 0


def greet(columns, rows, column, row):
    barrier = pltpu.get_barrier_semaphore()
    for dx, dy in DIRECTIONS:
        peer = (lax.rem(column + dx + columns, columns), row + dy)
        when(
            exists(row, rows, dy),
            lambda peer=peer: pl.semaphore_signal(
                barrier, inc=1, device_id=peer, device_id_type=MESH
            ),
        )
    return barrier


def greeted(rows, row):
    inner = lax.min(row, 1) + lax.min(rows - 1 - row, 1)
    return 2 + 3 * inner


def remote(src, dst, send, recv, k, peer):
    return pltpu.make_async_remote_copy(
        src_ref=src,
        dst_ref=dst,
        send_sem=send.at[k],
        recv_sem=recv.at[k],
        device_id=peer,
        device_id_type=MESH,
    )


def split(value):
    high = value.astype(jnp.bfloat16).astype(jnp.float32)
    return high, value - high


def upper_triangle():
    rows = lax.broadcasted_iota(jnp.int32, (CHUNK, CHUNK), 0)
    lanes = lax.broadcasted_iota(jnp.int32, (CHUNK, CHUNK), 1)
    return (rows <= lanes).astype(jnp.float32).astype(jnp.bfloat16)


def ranks(categories, count):
    rows = lax.broadcasted_iota(jnp.int32, (count, CHUNK), 0).astype(jnp.float32)
    hot = [(rows == block).astype(jnp.float32) for block in categories]
    stacked = jnp.concatenate(hot, axis=0).astype(jnp.bfloat16)
    inside = jnp.dot(stacked, upper_triangle(), preferred_element_type=jnp.float32)
    carry = jnp.zeros((count, 1), jnp.float32)
    upto = []
    for b in range(len(hot)):
        block = inside[b * count : (b + 1) * count]
        upto.append(block + carry)
        carry = carry + block[:, CHUNK - 1 : CHUNK]
    return hot, upto, carry


def place(parts, where_to, groups):
    group = jnp.floor(where_to * (1.0 / CHUNK))
    slot = where_to - group * CHUNK
    rows = lax.broadcasted_iota(jnp.int32, (CHUNK, where_to.shape[1]), 0).astype(jnp.float32)
    hot = (rows == slot).astype(jnp.float32).astype(jnp.bfloat16)
    masked = [parts * (group == g).astype(jnp.float32) for g in groups]
    masked = jnp.concatenate(masked, axis=0).astype(jnp.bfloat16)
    moved = lax.dot_general(
        masked, hot, (((1,), (1,)), ((), ())), preferred_element_type=jnp.float32
    )
    result = []
    for n in range(len(groups)):
        piece = moved[2 * RECORD * n : 2 * RECORD * (n + 1)]
        result.append(piece[:RECORD] + piece[RECORD:])
    return result


def front_kernel(
    columns, rows, *refs
):
    inputs, refs = refs[:8], refs[8:]
    staged, load = refs[-9:-1], refs[-1]
    loads = [
        pltpu.make_async_copy(src, dst, load.at[n])
        for n, (src, dst) in enumerate(zip(inputs, staged))
    ]
    for copy in loads:
        copy.start()
    front_body(columns, rows, loads, *staged, *refs[:-9])


def front_body(
    columns, rows, loads, owners, base_x, base_y, base_z, weights, offsets, motion, velocity,
    placed, alive, high, low, spread,
    home, slots, arrived, left, right, below, above, corners, parts, send, recv,
):
    column = lax.axis_index("gx")
    row = lax.axis_index("gy")
    span_x, span_y, extent_z = velocity.shape[1:]
    wide_y = span_y + 2 * ITERS
    lanes = len(DIRECTIONS)
    f32, bf16 = jnp.float32, jnp.bfloat16
    barrier = greet(columns, rows, column, row)

    def peer(dx, dy):
        return (lax.rem(column + dx + columns, columns), row + dy)

    edge = [(slots.at[g], arrived.at[g], dx, dy) for g, (dx, dy) in enumerate(DIRECTIONS)]
    rims = (slice(0, RIM), slice(span_y - RIM, span_y))
    for at in rims + (slice(RIM, span_y - RIM),):
        edge.append((velocity.at[:, 0:HALO, at], right.at[:, :, at], -1, 0))
        edge.append((velocity.at[:, span_x - HALO : span_x, at], left.at[:, :, at], 1, 0))
    edge.append((velocity.at[:, :, rims[0]], above, 0, -1))
    edge.append((velocity.at[:, :, rims[1]], below, 0, 1))
    for side, halo in enumerate((left, right)):
        edge.append((halo.at[:, :, rims[0]], corners.at[2 + side], 0, -1))
        edge.append((halo.at[:, :, rims[1]], corners.at[side], 0, 1))

    def start(k):
        src, dst, dx, dy = edge[k]
        when(
            exists(row, rows, dy),
            lambda: remote(src, dst, send, recv, k, peer(dx, dy)).start(),
        )

    def arrive(k):
        src, dst, dx, dy = edge[k]
        when(
            exists(row, rows, -dy),
            lambda: remote(src, dst, send, recv, k, peer(dx, dy)).wait_recv(),
        )

    def sent(k):
        src, dst, dx, dy = edge[k]
        when(
            exists(row, rows, dy),
            lambda: remote(src, dst, send, recv, k, peer(dx, dy)).wait_send(),
        )

    @pl.when(row == 0)
    def _():
        below[...] = jnp.zeros(below.shape, f32)
        for n in (0, 1):
            corners[n] = jnp.zeros(corners.shape[1:], f32)
        for g, (dx, dy) in enumerate(DIRECTIONS):
            if dy > 0:
                arrived[g] = jnp.zeros(arrived.shape[1:], f32)

    @pl.when(row == rows - 1)
    def _():
        above[...] = jnp.zeros(above.shape, f32)
        for n in (2, 3):
            corners[n] = jnp.zeros(corners.shape[1:], f32)
        for g, (dx, dy) in enumerate(DIRECTIONS):
            if dy < 0:
                arrived[g] = jnp.zeros(arrived.shape[1:], f32)

    for copy in loads[:7]:
        copy.wait()
    markers = owners.shape[1]
    spheres = motion.shape[0]
    per_sphere = markers // spheres
    owner = owners[...].astype(f32)
    owner_x = jnp.floor((owner + 0.5) * (1.0 / rows))
    owner_y = owner - owner_x * rows
    step_x = owner_x - column.astype(f32)
    step_x = jnp.where(step_x > 1.5, step_x - columns, step_x)
    step_x = jnp.where(step_x < -1.5, step_x + columns, step_x)
    step_y = owner_y - row.astype(f32)
    lane = (step_x + 1.0) * 3.0 + step_y + 1.0
    at_home = lane == 4.0
    lane = jnp.where(at_home, -1.0, jnp.where(lane > 4.0, lane - 1.0, lane))
    offset = offsets[...]
    targets = []
    for s in range(spheres):
        o = offset[:, s * per_sphere : (s + 1) * per_sphere]
        m = [motion[s : s + 1, c : c + 1] for c in range(6)]
        targets.append(
            jnp.concatenate(
                [
                    m[0] + (m[4] * o[2:3] - m[5] * o[1:2]),
                    m[1] + (m[5] * o[0:1] - m[3] * o[2:3]),
                    m[2] + (m[3] * o[1:2] - m[4] * o[0:1]),
                ],
                axis=0,
            )
        )
    home[0:12] = weights[...]
    for line, base in ((X_ROW, base_x), (Y_ROW, base_y), (Z_ROW, base_z)):
        home[line : line + 1] = base[...].astype(f32)
    home[TARGET : TARGET + 3] = jnp.concatenate(targets, axis=1)
    home[OFFSET : OFFSET + 3] = offset
    position = lax.broadcasted_iota(jnp.int32, (1, markers), 1)
    sphere = jnp.zeros((1, markers), f32)
    for s in range(1, spheres):
        sphere = sphere + (position >= s * per_sphere).astype(f32)
    home[SPHERE : SPHERE + 1] = sphere
    home[LIVE : LIVE + 1] = jnp.ones((1, markers), f32)
    home[LIVE + 1 : LIVE + 2] = jnp.zeros((1, markers), f32)

    blocks = markers // CHUNK
    hot, upto, totals = ranks([lane[:, b * CHUNK : (b + 1) * CHUNK] for b in range(blocks)], lanes)
    rank = [jnp.sum(h * (u - 1.0), axis=0, keepdims=True) for h, u in zip(hot, upto)]
    where_to = jnp.concatenate(rank, axis=1) + lane * CHUNK
    where_to = jnp.where(at_home, -1.0, where_to)
    pair = jnp.concatenate(split(home[...]), axis=0)
    for g, piece in enumerate(place(pair, where_to, range(lanes))):
        slots[g] = piece
    home[LIVE : LIVE + 1] = at_home.astype(f32)

    loads[7].wait()
    pl.semaphore_wait(barrier, greeted(rows, row))
    for k in range(len(edge) - 4):
        start(k)

    for k in range(lanes):
        arrive(k)
    total = blocks + lanes
    count = -(-(span_x + 1) // 8) * 8
    categories = []
    living = []
    for b in range(total):
        at = slice(b * CHUNK, (b + 1) * CHUNK)
        if b < blocks:
            record = home[:, at]
            group = lanes + record[SPHERE : SPHERE + 1] * (lanes + 1)
        else:
            record = arrived[b - blocks]
            group = (b - blocks) + record[SPHERE : SPHERE + 1] * (lanes + 1)
        lives = record[LIVE : LIVE + 1] > 0.5
        living.append(lives)
        categories.append(jnp.where(lives, record[X_ROW : X_ROW + 1], -1.0))
        first, rest = split(record)
        parts[0:RECORD, at] = first
        parts[RECORD : 2 * RECORD, at] = rest
        parts[SPHERE : SPHERE + 1, at] = group
    hot, upto, totals = ranks(categories, count)
    lower_rows = lax.broadcasted_iota(jnp.int32, (count, count), 0)
    lower_lanes = lax.broadcasted_iota(jnp.int32, (count, count), 1)
    before = (lower_lanes < lower_rows).astype(f32)
    wide = jnp.broadcast_to(totals, (count, TILE_LANES))
    starts = jnp.dot(
        before, wide, precision=lax.Precision.HIGHEST, preferred_element_type=f32
    )[:, 0:1]
    places = []
    for b in range(total):
        rank = jnp.sum(hot[b] * (upto[b] + (starts - 1.0)), axis=0, keepdims=True)
        places.append(jnp.where(living[b], rank, -1.0))
    where_to = jnp.concatenate(places, axis=1)
    alive[...] = jnp.broadcast_to(jnp.sum(wide, axis=0, keepdims=True), alive.shape)
    for first in range(0, total, GROUP):
        groups = range(first, min(first + GROUP, total))
        for g, piece in zip(groups, place(parts[...], where_to, groups)):
            placed[g] = piece

    def layer(x, row_source, below_source, above_source, own):
        for c in range(3):
            lines = row_source(c)
            margin = jnp.zeros((HALO, extent_z), f32)
            value = jnp.concatenate(
                [
                    margin,
                    below_source(c)[RIM - HALO : RIM],
                    lines,
                    above_source(c)[0:HALO],
                    margin,
                ],
                axis=0,
            )
            at = slice(wide_y * c, wide_y * (c + 1))
            first, rest = split(value)
            high[x, at] = first.astype(bf16)
            low[x, at] = rest.astype(bf16)
            if own:
                margin = jnp.zeros((ITERS, extent_z), f32)
                spread[x + HALO, at] = jnp.concatenate([margin, lines, margin], axis=0)
        end = jnp.zeros((high.shape[1] - 3 * wide_y, extent_z), bf16)
        high[x, 3 * wide_y :] = end
        low[x, 3 * wide_y :] = end

    arrive(len(edge) - 6)
    arrive(len(edge) - 5)

    def inner(x, carry):
        layer(
            x + HALO,
            lambda c: velocity[c, x],
            lambda c: below[c, x],
            lambda c: above[c, x],
            True,
        )
        return carry

    for k in range(lanes, lanes + 4):
        arrive(k)
    for k in range(len(edge) - 4, len(edge)):
        start(k)
    lax.fori_loop(0, span_x, inner, 0)
    for x in range(ITERS):
        spread[x] = jnp.zeros(spread.shape[1:], f32)
        spread[span_x + ITERS + x] = jnp.zeros(spread.shape[1:], f32)
    arrive(lanes + 4)
    arrive(lanes + 5)
    for k in range(len(edge) - 4, len(edge)):
        arrive(k)
    for side, halo in enumerate((left, right)):
        for x in range(HALO):
            layer(
                x + side * (span_x + HALO),
                lambda c: halo[c, x],
                lambda c: corners[side, c, x],
                lambda c: corners[2 + side, c, x],
                False,
            )
    for k in range(len(edge)):
        sent(k)


def front(owners, bases, weights, offsets, motion, velocity):
    columns, rows = lax.axis_size("gx"), lax.axis_size("gy")
    span_x, span_y, extent_z = velocity.shape[1:]
    wide_y = span_y + 2 * ITERS
    markers = owners.shape[1]
    lanes = len(DIRECTIONS)
    f32, bf16 = jnp.float32, jnp.bfloat16
    copies = lanes + 12
    inputs = (owners, *bases, weights, offsets, motion, velocity)
    total = markers // CHUNK + lanes
    field = (span_x + 2 * HALO, -(-3 * wide_y // 16) * 16, extent_z)
    vmem = pl.BlockSpec(memory_space=pltpu.VMEM)
    out = [
        pltpu.VMEM((total, RECORD, CHUNK), f32),
        pltpu.VMEM((8, TILE_LANES), f32),
        pltpu.VMEM(field, bf16),
        pltpu.VMEM(field, bf16),
        pltpu.VMEM((span_x + 2 * ITERS, 3 * wide_y, extent_z), f32),
    ]
    room = 67_043_328 - sum(math.prod(ref.shape) * ref.dtype.itemsize for ref in out) - 2**15
    return pl.pallas_call(
        functools.partial(front_kernel, columns, rows),
        out_shape=out,
        in_specs=[pl.BlockSpec(memory_space=pltpu.HBM)] * 8,
        out_specs=[vmem] * len(out),
        scratch_shapes=[
            pltpu.VMEM((RECORD, markers), f32),
            pltpu.VMEM((lanes, RECORD, CHUNK), f32),
            pltpu.VMEM((lanes, RECORD, CHUNK), f32),
            pltpu.VMEM((3, HALO, span_y, extent_z), f32),
            pltpu.VMEM((3, HALO, span_y, extent_z), f32),
            pltpu.VMEM((3, span_x, RIM, extent_z), f32),
            pltpu.VMEM((3, span_x, RIM, extent_z), f32),
            pltpu.VMEM((4, 3, HALO, RIM, extent_z), f32),
            pltpu.VMEM((2 * RECORD, total * CHUNK), f32),
            pltpu.SemaphoreType.DMA((copies,)),
            pltpu.SemaphoreType.DMA((copies,)),
        ]
        + [pltpu.VMEM(array.shape, array.dtype) for array in inputs]
        + [pltpu.SemaphoreType.DMA((len(inputs),))],
        compiler_params=pltpu.CompilerParams(
            collective_id=0, has_side_effects=True, vmem_limit_bytes=room
        ),
        name="front",
    )(*inputs)


def four(distance, weights):
    value = jnp.where(distance == 3.0, weights[3:4], 0.0)
    for n in (2, 1, 0):
        value = jnp.where(distance == float(n), weights[n : n + 1], value)
    return value


def markers_kernel(
    spheres, span_y, sorted_refs, alive_ref, high, low, frame, motion, spread, edges, tile, sums
):
    layers, _, extent_z = high.shape
    span_x = layers - 2 * HALO
    wide_y = span_y + 2 * ITERS
    lanes = len(DIRECTIONS)
    bf16, f32 = jnp.bfloat16, jnp.float32
    alive_count = jnp.max(alive_ref[0:1, :]).astype(jnp.int32)

    sums[...] = jnp.zeros(sums.shape, f32)
    z_cells = lax.broadcasted_iota(jnp.int32, (extent_z, CHUNK), 0).astype(f32)
    y_cells = lax.broadcasted_iota(jnp.int32, (wide_y, CHUNK), 0).astype(f32) - HALO
    x_cells = lax.broadcasted_iota(jnp.int32, (WINDOW, CHUNK), 0).astype(f32)

    def chunk(j, carry):
        record = sorted_refs[j]
        alive = record[LIVE : LIVE + 1]
        cell_x = record[X_ROW : X_ROW + 1]
        distance = z_cells - record[Z_ROW : Z_ROW + 1]
        distance = jnp.where(distance < 0.0, distance + extent_z, distance)
        z_high, z_low = split(four(distance, record[8:12]))
        z_high = z_high.astype(bf16)
        z_low = z_low.astype(bf16)
        y_table = four(y_cells - record[Y_ROW : Y_ROW + 1], record[4:8])
        least = jnp.min(jnp.where(alive > 0.5, cell_x, 1e4)).astype(jnp.int32)
        most = jnp.max(jnp.where(alive > 0.5, cell_x, -1.0)).astype(jnp.int32)
        windows = (most + 4 - least + WINDOW - 1) // WINDOW

        def x_table(k):
            fresh = least + WINDOW * k
            base = jnp.minimum(fresh, layers - WINDOW)
            cells = x_cells + base.astype(f32)
            table = four(cells - cell_x, record[0:4])
            return base, jnp.where(cells >= fresh.astype(f32), table, 0.0)

        z_stack = jnp.concatenate([z_high, z_high, z_low], axis=0)

        def sample(k, total):
            base, table = x_table(k)
            rows = high.shape[1]
            first = high[pl.ds(base, WINDOW)].reshape(WINDOW * rows, extent_z)
            rest = low[pl.ds(base, WINDOW)].reshape(WINDOW * rows, extent_z)
            lines = jnp.dot(
                jnp.concatenate([first, rest, first], axis=1),
                z_stack,
                preferred_element_type=f32,
            )
            for x in range(WINDOW):
                total = total + lines[x * rows : x * rows + 3 * wide_y] * table[x : x + 1]
            return total

        plane = lax.fori_loop(0, windows, sample, jnp.zeros((3 * wide_y, CHUNK), f32))
        forces = []
        for c in range(3):
            got = jnp.sum(plane[c * wide_y : (c + 1) * wide_y] * y_table, axis=0, keepdims=True)
            forces.append((record[TARGET + c : TARGET + c + 1] - got) * alive)
        sheet = jnp.concatenate([force * y_table for force in forces], axis=0)
        z_wide = jnp.concatenate([z_high, z_high, z_low], axis=1)

        def deposit(k, carry):
            base, table = x_table(k)
            value = jnp.concatenate([sheet * table[x : x + 1] for x in range(WINDOW)], axis=0)
            first, rest = split(value)
            first = first.astype(bf16)
            rest = rest.astype(bf16)
            added = lax.dot_general(
                jnp.concatenate([first, rest, first], axis=1),
                z_wide,
                (((1,), (1,)), ((), ())),
                preferred_element_type=f32,
            )
            at = pl.ds(base + HALO, WINDOW)
            spread[at] = spread[at] + added.reshape(WINDOW, 3 * wide_y, extent_z)
            return carry

        lax.fori_loop(0, windows, deposit, 0)
        o = [record[OFFSET + c : OFFSET + c + 1] for c in range(3)]
        f = forces
        moments = jnp.concatenate(
            f
            + [
                o[1] * f[2] - o[2] * f[1],
                o[2] * f[0] - o[0] * f[2],
                o[0] * f[1] - o[1] * f[0],
                jnp.zeros((2, CHUNK), f32),
            ],
            axis=0,
        )
        group = record[SPHERE : SPHERE + 1]
        for g in range((lanes + 1) * spheres):
            sums[g] = sums[g] + jnp.where(group == float(g), moments, 0.0)
        return carry

    chunks = (alive_count + (CHUNK - 1)) // CHUNK
    lax.fori_loop(0, chunks, chunk, 0)
    columns = jnp.sum(sums[...], axis=2)
    tile[...] = jnp.zeros(tile.shape, f32)
    for s in range(spheres):
        for slot in range(lanes + 1):
            at = 6 * (slot * spheres + s)
            line = (lanes + 1) * s + slot
            tile[0:1, at : at + 6] = columns[line : line + 1, 0:6]
        at = 6 * ((lanes + 1) * spheres + s)
        tile[0:1, at : at + 6] = motion[s : s + 1]
    reach = ITERS + HALO
    middle = span_y + 2 * HALO - 2 * reach
    for side, first in enumerate((span_x, HALO)):
        for c in range(3):
            for x in range(reach):
                low_rim = wide_y * c + HALO
                high_rim = wide_y * (c + 1) - HALO - reach
                done = 0
                for start, length in (
                    (low_rim, reach),
                    (high_rim, reach),
                    (low_rim + reach, middle),
                ):
                    to = done + length * x
                    edges[side, c, to : to + length] = spread[first + x, start : start + length]
                    done += length * reach


def markers_stage(spheres, span_y, placed, alive, high, low, frame, motion):
    wide_x, lines, extent_z = frame.shape
    lanes = len(DIRECTIONS)
    f32 = jnp.float32
    groups = (lanes + 1) * spheres
    vmem = pl.BlockSpec(memory_space=pltpu.VMEM)
    return pl.pallas_call(
        functools.partial(markers_kernel, spheres, span_y),
        out_shape=[
            pltpu.VMEM(frame.shape, f32),
            pltpu.VMEM((2, 3, (ITERS + HALO) * (span_y + 2 * HALO), extent_z), f32),
            jax.ShapeDtypeStruct((1, TILE_LANES), f32),
        ],
        in_specs=[vmem] * 6,
        out_specs=[vmem] * 3,
        scratch_shapes=[pltpu.VMEM((groups, 8, CHUNK), f32)],
        input_output_aliases={4: 0},
        compiler_params=pltpu.CompilerParams(vmem_limit_bytes=40 * 2**20),
        name="markers",
    )(placed, alive, high, low, frame, motion)


def combine_matrix(columns, rows, per_sphere):
    slots = len(DIRECTIONS) + 2
    matrix = np.zeros((slots, columns, rows, columns, rows), np.float32)
    for i in range(columns):
        for j in range(rows):
            for slot, (dx, dy) in enumerate(DIRECTIONS):
                if 0 <= j - dy < rows:
                    matrix[slot, (i - dx) % columns, j - dy, i, j] -= RESPONSE / per_sphere
            matrix[slots - 2, i, j, i, j] -= RESPONSE / per_sphere
            matrix[slots - 1, i, j, i, j] = 1.0
    return matrix.reshape(slots * columns * rows, -1)


def tail_kernel(
    columns, rows, spread, edges, tile, matrix, contact_sphere, contact_partner,
    out, motion_out, from_left, from_right, from_below, from_above, corners, held,
    rhs, one, two, mask_ref, own_sem, send, recv, row_send, row_recv, col_send, col_recv,
):
    column = lax.axis_index("gx")
    row = lax.axis_index("gy")
    span_x, span_y, extent_z = out.shape[1:]
    wide_x, wide_y = span_x + 2 * ITERS, span_y + 2 * ITERS
    reach = ITERS + HALO
    depth = span_y + 2 * HALO
    row_peers = [lax.rem(row + k, rows) for k in range(1, rows)]
    column_peers = [lax.rem(column + k, columns) for k in range(1, columns)]
    barrier = pltpu.get_barrier_semaphore()
    for other in row_peers:
        pl.semaphore_signal(barrier, inc=1, device_id=(column, other), device_id_type=MESH)
    for other in column_peers:
        pl.semaphore_signal(barrier, inc=1, device_id=(other, row), device_id_type=MESH)
    own = pltpu.make_async_copy(tile, held.at[column, row], own_sem)
    own.start()

    def peer(dx, dy):
        return (lax.rem(column + dx + columns, columns), row + dy)

    edge = []
    rim = 2 * reach * reach
    part = corners.shape[2]
    for c in range(3):
        low, high = wide_y * c, wide_y * (c + 1)
        inner = slice(HALO, wide_x - HALO)
        edge += [
            (edges.at[0, c, 0:rim], from_left.at[c, 0:rim], 1, 0),
            (edges.at[1, c, 0:rim], from_right.at[c, 0:rim], -1, 0),
            (edges.at[0, c, rim:], from_left.at[c, rim:], 1, 0),
            (edges.at[1, c, rim:], from_right.at[c, rim:], -1, 0),
            (spread.at[inner, high - RIM : high], from_below.at[c], 0, 1),
            (spread.at[inner, low : low + RIM], from_above.at[c], 0, -1),
            (from_left.at[c, rim - part : rim], corners.at[c, 0], 0, 1),
            (from_right.at[c, rim - part : rim], corners.at[c, 1], 0, 1),
            (from_left.at[c, 0:part], corners.at[c, 2], 0, -1),
            (from_right.at[c, 0:part], corners.at[c, 3], 0, -1),
        ]
    each = 10

    def start(k):
        src, dst, dx, dy = edge[k]
        when(
            exists(row, rows, dy),
            lambda: remote(src, dst, send, recv, k, peer(dx, dy)).start(),
        )

    def arrive(k):
        src, dst, dx, dy = edge[k]
        when(
            exists(row, rows, -dy),
            lambda: remote(src, dst, send, recv, k, peer(dx, dy)).wait_recv(),
        )

    def sent(k):
        src, dst, dx, dy = edge[k]
        when(
            exists(row, rows, dy),
            lambda: remote(src, dst, send, recv, k, peer(dx, dy)).wait_send(),
        )

    @pl.when(row == 0)
    def _():
        from_below[...] = jnp.zeros(from_below.shape, jnp.float32)
        for c in range(3):
            corners[c, 0:2] = jnp.zeros((2,) + corners.shape[2:], jnp.float32)

    @pl.when(row == rows - 1)
    def _():
        from_above[...] = jnp.zeros(from_above.shape, jnp.float32)
        for c in range(3):
            corners[c, 2:4] = jnp.zeros((2,) + corners.shape[2:], jnp.float32)

    pl.semaphore_wait(barrier, rows + columns - 2)
    first = [
        pltpu.make_async_remote_copy(
            src_ref=tile,
            dst_ref=held.at[column, row],
            send_sem=row_send.at[k],
            recv_sem=row_recv.at[k],
            device_id=(column, other),
            device_id_type=MESH,
        )
        for k, other in enumerate(row_peers)
    ]
    for copy in first:
        copy.start()
    for k in range(6):
        start(k)
    for c in range(1, 3):
        for k in range(4, 6):
            start(each * c + k)

    cells = lax.broadcasted_iota(jnp.int32, (wide_y, extent_z), 0) + (row * span_y - ITERS)
    inside = jnp.logical_and(cells >= 0, cells < span_y * rows)
    inverse = 1.0 / (1.0 + 6.0 * DIFFUSION)
    mask_ref[0] = inside.astype(jnp.float32)
    mask_ref[1] = inside.astype(jnp.float32) * inverse

    own.wait()
    for copy in first:
        copy.wait()
    second = [
        pltpu.make_async_remote_copy(
            src_ref=held.at[column],
            dst_ref=held.at[column],
            send_sem=col_send.at[k],
            recv_sem=col_recv.at[k],
            device_id=(other, row),
            device_id_type=MESH,
        )
        for k, other in enumerate(column_peers)
    ]
    for copy in second:
        copy.start()
    for c in range(1, 3):
        for k in range(4):
            start(each * c + k)

    def relaxed(c, source, x):
        here = source[c, x]
        beside = source[c, x - 1] + source[c, x + 1]
        beside = beside + pltpu.roll(here, 1, 0) + pltpu.roll(here, wide_y - 1, 0)
        beside = beside + pltpu.roll(here, 1, 1) + pltpu.roll(here, extent_z - 1, 1)
        return (rhs[c, x] + DIFFUSION * beside) * mask_ref[1]

    buffers = (rhs, one, two, one)

    def sweeps(c, starts, length):
        for sweep in range(ITERS):
            source = buffers[sweep]
            for first, shift in starts:
                begin = first + sweep * shift
                for x in range(begin, begin + length(sweep)):
                    new = relaxed(c, source, x)
                    if sweep == ITERS - 1:
                        out[c, x - ITERS] = new[ITERS : ITERS + span_y]
                    else:
                        buffers[sweep + 1][c, x] = new

    def base(c, carry):
        for x in range(wide_x):
            rhs[c, x] = spread[x, pl.ds(pl.multiple_of(wide_y * c, 8), wide_y)]
        for x in range(wide_x - 2 * HALO):
            y = x + HALO
            rhs[c, y, 0:RIM] = rhs[c, y, 0:RIM] + from_below[c, x]
            rhs[c, y, wide_y - RIM :] = rhs[c, y, wide_y - RIM :] + from_above[c, x]
        for x in range(reach, wide_x - reach):
            rhs[c, x] = rhs[c, x] * mask_ref[0]
        sweeps(c, ((reach + 1, 1),), lambda sweep: span_x - 2 * HALO - 2 - 2 * sweep)
        return carry

    for c in range(3):
        arrive(each * c + 4)
        arrive(each * c + 5)
    lax.fori_loop(0, 3, base, 0)

    middle = depth - 2 * reach
    upper = wide_y - HALO - reach

    def outer(c):
        for x in range(reach):
            for side, (halo, y) in enumerate(((from_left, x), (from_right, x + span_x + HALO))):
                low = slice(reach * x, reach * (x + 1))
                high = slice(reach * (reach + x), reach * (reach + x + 1))
                late = slice(part - rim // 2 + reach * x, part - rim // 2 + reach * (x + 1))
                inside = slice(rim + middle * x, rim + middle * (x + 1))
                rhs[c, y, HALO : HALO + reach] = rhs[c, y, HALO : HALO + reach] + halo[c, low]
                rhs[c, y, upper : upper + reach] = rhs[c, y, upper : upper + reach] + halo[c, high]
                rhs[c, y, HALO + reach : upper] = rhs[c, y, HALO + reach : upper] + halo[c, inside]
                rhs[c, y, 0:reach] = rhs[c, y, 0:reach] + corners[c, side, late]
                rhs[c, y, wide_y - reach :] = rhs[c, y, wide_y - reach :] + corners[c, 2 + side, low]
                rhs[c, y] = rhs[c, y] * mask_ref[0]
        sweeps(c, ((1, 1), (span_x + 1, -1)), lambda sweep: reach)

    def settle():
        for copy in second:
            copy.wait()
        gathered = held[...].reshape(-1, TILE_LANES)
        devices = columns * rows
        pieces = jnp.dot(
            matrix[...],
            gathered,
            precision=lax.Precision.HIGHEST,
            preferred_element_type=jnp.float32,
        )
        spheres = motion_out.shape[0]
        moved = 0.0
        for slot in range(len(DIRECTIONS) + 2):
            at = 6 * spheres * slot
            moved = moved + pieces[devices * slot : devices * (slot + 1), at : at + 6 * spheres]
        device = lax.broadcasted_iota(jnp.int32, (1, devices), 1)
        here = column * rows + row
        linked, owned = [], []
        for s in range(spheres):
            mine = here * spheres + s
            for other in range(spheres):
                own_row = (device * spheres + other == mine).astype(jnp.float32)
                line = own_row
                for k in range(contact_sphere.shape[0]):
                    acts = contact_sphere[k] == mine
                    partner = (device * spheres + other == contact_partner[k]).astype(jnp.float32)
                    line = line + jnp.where(acts, DASHPOT * (partner - own_row), 0.0)
                linked.append(line)
                owned.append(own_row)
        links = jnp.concatenate(linked + owned, axis=0)
        result = jnp.dot(
            links, moved, precision=lax.Precision.HIGHEST, preferred_element_type=jnp.float32
        )
        for s in range(spheres):
            for half in range(2):
                total = 0.0
                for other in range(spheres):
                    line = (half * spheres + s) * spheres + other
                    at = 6 * other + 3 * half
                    total = total + result[line : line + 1, at : at + 3]
                motion_out[s : s + 1, 3 * half : 3 * half + 3] = total

    for c in range(3):
        arrive(each * c)
        arrive(each * c + 1)
        for k in range(6, each):
            start(each * c + k)
        if c == 2:
            settle()
        for k in range(2, 4):
            arrive(each * c + k)
        for k in range(6, each):
            arrive(each * c + k)
        outer(c)

    for k in range(len(edge)):
        sent(k)


def tail(spread, edges, tile, matrix, contact_sphere, contact_partner, span_y, spheres):
    columns, rows = lax.axis_size("gx"), lax.axis_size("gy")
    wide_x, _, extent_z = spread.shape
    span_x = wide_x - 2 * ITERS
    wide_y = span_y + 2 * ITERS
    reach = ITERS + HALO
    f32 = jnp.float32
    vmem = pl.BlockSpec(memory_space=pltpu.VMEM)
    smem = pl.BlockSpec(memory_space=pltpu.SMEM)
    dma = pltpu.SemaphoreType.DMA
    corner = (3, 4, -(-reach * reach // 8) * 8, extent_z)
    frame = (3, wide_x, wide_y, extent_z)
    return pl.pallas_call(
        functools.partial(tail_kernel, columns, rows),
        out_shape=[
            pltpu.VMEM((3, span_x, span_y, extent_z), f32),
            jax.ShapeDtypeStruct((spheres, 6), f32),
        ],
        in_specs=[vmem] * 4 + [smem] * 2,
        out_specs=[vmem] * 2,
        scratch_shapes=[
            pltpu.VMEM(edges.shape[1:], f32),
            pltpu.VMEM(edges.shape[1:], f32),
            pltpu.VMEM((3, wide_x - 2 * HALO, RIM, extent_z), f32),
            pltpu.VMEM((3, wide_x - 2 * HALO, RIM, extent_z), f32),
            pltpu.VMEM(corner, f32),
            pltpu.VMEM((columns, rows) + tile.shape, f32),
            pltpu.VMEM(frame, f32),
            pltpu.VMEM(frame, f32),
            pltpu.VMEM(frame, f32),
            pltpu.VMEM((2, wide_y, extent_z), f32),
            dma,
            dma((30,)),
            dma((30,)),
            dma((rows - 1,)),
            dma((rows - 1,)),
            dma((columns - 1,)),
            dma((columns - 1,)),
        ],
        compiler_params=pltpu.CompilerParams(
            collective_id=1, has_side_effects=True, vmem_limit_bytes=40 * 2**20
        ),
        name="tail",
    )(spread, edges, tile, matrix, contact_sphere, contact_partner)


def on_device(
    velocity,
    owner_block,
    base_x,
    base_y,
    base_z,
    delta_weights,
    marker_offset,
    sphere_motion,
    contact_sphere,
    contact_partner,
):
    span_y = velocity.shape[2]
    markers = base_x.shape[0]
    spheres = sphere_motion.shape[1]
    bases = [base.reshape(1, markers) for base in (base_x, base_y, base_z)]
    owners = owner_block.reshape(1, markers)
    motion = sphere_motion.T
    staged = front(owners, bases, delta_weights, marker_offset, motion, velocity)
    spread, edges, tile = markers_stage(spheres, span_y, *staged, motion)
    columns, rows = lax.axis_size("gx"), lax.axis_size("gy")
    matrix = jnp.asarray(combine_matrix(columns, rows, markers // spheres))
    state, moved = tail(
        spread, edges, tile, matrix, contact_sphere, contact_partner, span_y, spheres
    )
    return state, moved.T


def solution(mesh):
    placed = (
        P(None, "gx", "gy", None),
        P(("gx", "gy"), None),
        P(("gx", "gy")),
        P(("gx", "gy")),
        P(("gx", "gy")),
        P(None, ("gx", "gy")),
        P(None, ("gx", "gy")),
        P(None, ("gx", "gy")),
        P(("gx", "gy")),
        P(("gx", "gy")),
    )
    return jax.shard_map(
        on_device,
        mesh=mesh,
        in_specs=placed,
        out_specs=(P(None, "gx", "gy", None), P(None, ("gx", "gy"))),
        check_vma=False,
    )
```

```python
import functools
import math

import jax
import jax.numpy as jnp
import numpy as np
from jax import lax
from jax.experimental import pallas as pl
from jax.experimental.pallas import tpu as pltpu
from jax.sharding import PartitionSpec as P

ITERS = 4
DIFFUSION = 1.0
RESPONSE = 0.5
DASHPOT = 0.1

MESH = pl.DeviceIdType.MESH
TILE_LANES = 128
CHUNK = 256
WINDOW = 6
TOGETHER = 2
GROUP = 6
RECORD = 24
X_ROW, Y_ROW, Z_ROW, TARGET, OFFSET, SPHERE, LIVE = 12, 13, 14, 15, 18, 21, 22
DIRECTIONS = ((-1, -1), (-1, 0), (-1, 1), (0, -1), (0, 1), (1, -1), (1, 0), (1, 1))
HALO = 2
RIM = 8


def when(condition, body):
    if condition is True:
        body()
    else:
        pl.when(condition)(body)


def exists(row, rows, dy):
    if dy == 0:
        return True
    return row + dy < rows if dy > 0 else row + dy >= 0


def greet(columns, rows, column, row):
    barrier = pltpu.get_barrier_semaphore()
    for dx, dy in DIRECTIONS:
        peer = (lax.rem(column + dx + columns, columns), row + dy)
        when(
            exists(row, rows, dy),
            lambda peer=peer: pl.semaphore_signal(
                barrier, inc=1, device_id=peer, device_id_type=MESH
            ),
        )
    return barrier


def greeted(rows, row):
    inner = lax.min(row, 1) + lax.min(rows - 1 - row, 1)
    return 2 + 3 * inner


def remote(src, dst, send, recv, k, peer):
    return pltpu.make_async_remote_copy(
        src_ref=src,
        dst_ref=dst,
        send_sem=send.at[k],
        recv_sem=recv.at[k],
        device_id=peer,
        device_id_type=MESH,
    )


def split(value):
    high = value.astype(jnp.bfloat16).astype(jnp.float32)
    return high, value - high


def upper_triangle():
    rows = lax.broadcasted_iota(jnp.int32, (CHUNK, CHUNK), 0)
    lanes = lax.broadcasted_iota(jnp.int32, (CHUNK, CHUNK), 1)
    return (rows <= lanes).astype(jnp.float32).astype(jnp.bfloat16)


def ranks(categories, count):
    rows = lax.broadcasted_iota(jnp.int32, (count, CHUNK), 0).astype(jnp.float32)
    hot = [(rows == block).astype(jnp.float32) for block in categories]
    stacked = jnp.concatenate(hot, axis=0).astype(jnp.bfloat16)
    inside = jnp.dot(stacked, upper_triangle(), preferred_element_type=jnp.float32)
    carry = jnp.zeros((count, 1), jnp.float32)
    upto = []
    for b in range(len(hot)):
        block = inside[b * count : (b + 1) * count]
        upto.append(block + carry)
        carry = carry + block[:, CHUNK - 1 : CHUNK]
    return hot, upto, carry


def place(parts, where_to, groups):
    group = jnp.floor(where_to * (1.0 / CHUNK))
    slot = where_to - group * CHUNK
    rows = lax.broadcasted_iota(jnp.int32, (CHUNK, where_to.shape[1]), 0).astype(jnp.float32)
    hot = (rows == slot).astype(jnp.float32).astype(jnp.bfloat16)
    masked = [parts * (group == g).astype(jnp.float32) for g in groups]
    masked = jnp.concatenate(masked, axis=0).astype(jnp.bfloat16)
    moved = lax.dot_general(
        masked, hot, (((1,), (1,)), ((), ())), preferred_element_type=jnp.float32
    )
    result = []
    for n in range(len(groups)):
        piece = moved[2 * RECORD * n : 2 * RECORD * (n + 1)]
        result.append(piece[:RECORD] + piece[RECORD:])
    return result


def front_kernel(
    columns, rows, *refs
):
    inputs, refs = refs[:8], refs[8:]
    staged, load = refs[-9:-1], refs[-1]
    loads = [
        pltpu.make_async_copy(src, dst, load.at[n])
        for n, (src, dst) in enumerate(zip(inputs, staged))
    ]
    for copy in loads:
        copy.start()
    front_body(columns, rows, loads, *staged, *refs[:-9])


def front_body(
    columns, rows, loads, owners, base_x, base_y, base_z, weights, offsets, motion, velocity,
    placed, alive, high_0, low_0, frame_0, high_1, low_1, frame_1,
    home, slots, arrived, left, right, below, above, corners, parts, send, recv,
):
    column = lax.axis_index("gx")
    row = lax.axis_index("gy")
    span_x, span_y, extent_z = velocity.shape[1:]
    wide_y = span_y + 2 * ITERS
    lanes = len(DIRECTIONS)
    f32, bf16 = jnp.float32, jnp.bfloat16
    barrier = greet(columns, rows, column, row)

    def peer(dx, dy):
        return (lax.rem(column + dx + columns, columns), row + dy)

    edge = [(slots.at[g], arrived.at[g], dx, dy) for g, (dx, dy) in enumerate(DIRECTIONS)]
    rims = (slice(0, RIM), slice(span_y - RIM, span_y))
    for at in rims + (slice(RIM, span_y - RIM),):
        edge.append((velocity.at[:, 0:HALO, at], right.at[:, :, at], -1, 0))
        edge.append((velocity.at[:, span_x - HALO : span_x, at], left.at[:, :, at], 1, 0))
    edge.append((velocity.at[:, :, rims[0]], above, 0, -1))
    edge.append((velocity.at[:, :, rims[1]], below, 0, 1))
    for side, halo in enumerate((left, right)):
        edge.append((halo.at[:, :, rims[0]], corners.at[2 + side], 0, -1))
        edge.append((halo.at[:, :, rims[1]], corners.at[side], 0, 1))

    def start(k):
        src, dst, dx, dy = edge[k]
        when(
            exists(row, rows, dy),
            lambda: remote(src, dst, send, recv, k, peer(dx, dy)).start(),
        )

    def arrive(k):
        src, dst, dx, dy = edge[k]
        when(
            exists(row, rows, -dy),
            lambda: remote(src, dst, send, recv, k, peer(dx, dy)).wait_recv(),
        )

    def sent(k):
        src, dst, dx, dy = edge[k]
        when(
            exists(row, rows, dy),
            lambda: remote(src, dst, send, recv, k, peer(dx, dy)).wait_send(),
        )

    @pl.when(row == 0)
    def _():
        below[...] = jnp.zeros(below.shape, f32)
        for n in (0, 1):
            corners[n] = jnp.zeros(corners.shape[1:], f32)
        for g, (dx, dy) in enumerate(DIRECTIONS):
            if dy > 0:
                arrived[g] = jnp.zeros(arrived.shape[1:], f32)

    @pl.when(row == rows - 1)
    def _():
        above[...] = jnp.zeros(above.shape, f32)
        for n in (2, 3):
            corners[n] = jnp.zeros(corners.shape[1:], f32)
        for g, (dx, dy) in enumerate(DIRECTIONS):
            if dy < 0:
                arrived[g] = jnp.zeros(arrived.shape[1:], f32)

    for copy in loads[:7]:
        copy.wait()
    markers = owners.shape[1]
    spheres = motion.shape[0]
    per_sphere = markers // spheres
    owner = owners[...].astype(f32)
    owner_x = jnp.floor((owner + 0.5) * (1.0 / rows))
    owner_y = owner - owner_x * rows
    step_x = owner_x - column.astype(f32)
    step_x = jnp.where(step_x > 1.5, step_x - columns, step_x)
    step_x = jnp.where(step_x < -1.5, step_x + columns, step_x)
    step_y = owner_y - row.astype(f32)
    lane = (step_x + 1.0) * 3.0 + step_y + 1.0
    at_home = lane == 4.0
    lane = jnp.where(at_home, -1.0, jnp.where(lane > 4.0, lane - 1.0, lane))
    offset = offsets[...]
    targets = []
    for s in range(spheres):
        o = offset[:, s * per_sphere : (s + 1) * per_sphere]
        m = [motion[s : s + 1, c : c + 1] for c in range(6)]
        targets.append(
            jnp.concatenate(
                [
                    m[0] + (m[4] * o[2:3] - m[5] * o[1:2]),
                    m[1] + (m[5] * o[0:1] - m[3] * o[2:3]),
                    m[2] + (m[3] * o[1:2] - m[4] * o[0:1]),
                ],
                axis=0,
            )
        )
    home[0:12] = weights[...]
    for line, base in ((X_ROW, base_x), (Y_ROW, base_y), (Z_ROW, base_z)):
        home[line : line + 1] = base[...].astype(f32)
    home[TARGET : TARGET + 3] = jnp.concatenate(targets, axis=1)
    home[OFFSET : OFFSET + 3] = offset
    position = lax.broadcasted_iota(jnp.int32, (1, markers), 1)
    sphere = jnp.zeros((1, markers), f32)
    for s in range(1, spheres):
        sphere = sphere + (position >= s * per_sphere).astype(f32)
    home[SPHERE : SPHERE + 1] = sphere
    home[LIVE : LIVE + 1] = jnp.ones((1, markers), f32)
    home[LIVE + 1 : LIVE + 2] = jnp.zeros((1, markers), f32)

    blocks = markers // CHUNK
    hot, upto, totals = ranks([lane[:, b * CHUNK : (b + 1) * CHUNK] for b in range(blocks)], lanes)
    rank = [jnp.sum(h * (u - 1.0), axis=0, keepdims=True) for h, u in zip(hot, upto)]
    where_to = jnp.concatenate(rank, axis=1) + lane * CHUNK
    where_to = jnp.where(at_home, -1.0, where_to)
    pair = jnp.concatenate(split(home[...]), axis=0)
    for g, piece in enumerate(place(pair, where_to, range(lanes))):
        slots[g] = piece
    home[LIVE : LIVE + 1] = at_home.astype(f32)

    loads[7].wait()
    pl.semaphore_wait(barrier, greeted(rows, row))
    for k in range(len(edge) - 4):
        start(k)

    for k in range(lanes):
        arrive(k)
    total = blocks + lanes
    count = -(-(span_x + 1) // 8) * 8
    categories = []
    living = []
    for b in range(total):
        at = slice(b * CHUNK, (b + 1) * CHUNK)
        if b < blocks:
            record = home[:, at]
            group = lanes + record[SPHERE : SPHERE + 1] * (lanes + 1)
        else:
            record = arrived[b - blocks]
            group = (b - blocks) + record[SPHERE : SPHERE + 1] * (lanes + 1)
        lives = record[LIVE : LIVE + 1] > 0.5
        living.append(lives)
        categories.append(jnp.where(lives, record[X_ROW : X_ROW + 1], -1.0))
        first, rest = split(record)
        parts[0:RECORD, at] = first
        parts[RECORD : 2 * RECORD, at] = rest
        parts[SPHERE : SPHERE + 1, at] = group
    hot, upto, totals = ranks(categories, count)
    lower_rows = lax.broadcasted_iota(jnp.int32, (count, count), 0)
    lower_lanes = lax.broadcasted_iota(jnp.int32, (count, count), 1)
    before = (lower_lanes < lower_rows).astype(f32)
    wide = jnp.broadcast_to(totals, (count, TILE_LANES))
    starts = jnp.dot(
        before, wide, precision=lax.Precision.HIGHEST, preferred_element_type=f32
    )[:, 0:1]
    places = []
    for b in range(total):
        rank = jnp.sum(hot[b] * (upto[b] + (starts - 1.0)), axis=0, keepdims=True)
        places.append(jnp.where(living[b], rank, -1.0))
    where_to = jnp.concatenate(places, axis=1)
    alive[...] = jnp.broadcast_to(jnp.sum(wide, axis=0, keepdims=True), alive.shape)
    for first in range(0, total, GROUP):
        groups = range(first, min(first + GROUP, total))
        for g, piece in zip(groups, place(parts[...], where_to, groups)):
            placed[g] = piece

    def layer(x, row_source, below_source, above_source, own):
        for c in range(3):
            lines = row_source(c)
            margin = jnp.zeros((HALO, extent_z), f32)
            value = jnp.concatenate(
                [
                    margin,
                    below_source(c)[RIM - HALO : RIM],
                    lines,
                    above_source(c)[0:HALO],
                    margin,
                ],
                axis=0,
            )
            high, low, frame = (high_0, low_0, frame_0) if c == 0 else (high_1, low_1, frame_1)
            begin = 0 if c == 0 else wide_y * (c - 1)
            at = slice(begin, begin + wide_y)
            first, rest = split(value)
            high[x, at] = first.astype(bf16)
            low[x, at] = rest.astype(bf16)
            if own:
                margin = jnp.zeros((ITERS, extent_z), f32)
                frame[x + HALO, at] = jnp.concatenate([margin, lines, margin], axis=0)
        for ref, used in ((high_0, 1), (low_0, 1), (high_1, 2), (low_1, 2)):
            used = used * wide_y
            if ref.shape[1] > used:
                ref[x, used:] = jnp.zeros((ref.shape[1] - used, extent_z), bf16)

    arrive(len(edge) - 6)
    arrive(len(edge) - 5)

    def inner(x, carry):
        layer(
            x + HALO,
            lambda c: velocity[c, x],
            lambda c: below[c, x],
            lambda c: above[c, x],
            True,
        )
        return carry

    for k in range(lanes, lanes + 4):
        arrive(k)
    for k in range(len(edge) - 4, len(edge)):
        start(k)
    lax.fori_loop(0, span_x, inner, 0)
    for x in range(ITERS):
        for frame in (frame_0, frame_1):
            frame[x] = jnp.zeros(frame.shape[1:], f32)
            frame[span_x + ITERS + x] = jnp.zeros(frame.shape[1:], f32)
    arrive(lanes + 4)
    arrive(lanes + 5)
    for k in range(len(edge) - 4, len(edge)):
        arrive(k)
    for side, halo in enumerate((left, right)):
        for x in range(HALO):
            layer(
                x + side * (span_x + HALO),
                lambda c: halo[c, x],
                lambda c: corners[side, c, x],
                lambda c: corners[2 + side, c, x],
                False,
            )
    for k in range(len(edge)):
        sent(k)


def front(owners, bases, weights, offsets, motion, velocity):
    columns, rows = lax.axis_size("gx"), lax.axis_size("gy")
    span_x, span_y, extent_z = velocity.shape[1:]
    wide_y = span_y + 2 * ITERS
    markers = owners.shape[1]
    lanes = len(DIRECTIONS)
    f32, bf16 = jnp.float32, jnp.bfloat16
    copies = lanes + 12
    inputs = (owners, *bases, weights, offsets, motion, velocity)
    total = markers // CHUNK + lanes
    vmem = pl.BlockSpec(memory_space=pltpu.VMEM)
    out = [
        pltpu.VMEM((total, RECORD, CHUNK), f32),
        pltpu.VMEM((8, TILE_LANES), f32),
    ]
    for lines in (wide_y, 2 * wide_y):
        field = (span_x + 2 * HALO, -(-lines // 16) * 16, extent_z)
        out += [pltpu.VMEM(field, bf16), pltpu.VMEM(field, bf16)]
        out.append(pltpu.VMEM((span_x + 2 * ITERS, lines, extent_z), f32))
    room = 67_043_328 - sum(math.prod(ref.shape) * ref.dtype.itemsize for ref in out) - 2**15
    return pl.pallas_call(
        functools.partial(front_kernel, columns, rows),
        out_shape=out,
        in_specs=[pl.BlockSpec(memory_space=pltpu.HBM)] * 8,
        out_specs=[vmem] * len(out),
        scratch_shapes=[
            pltpu.VMEM((RECORD, markers), f32),
            pltpu.VMEM((lanes, RECORD, CHUNK), f32),
            pltpu.VMEM((lanes, RECORD, CHUNK), f32),
            pltpu.VMEM((3, HALO, span_y, extent_z), f32),
            pltpu.VMEM((3, HALO, span_y, extent_z), f32),
            pltpu.VMEM((3, span_x, RIM, extent_z), f32),
            pltpu.VMEM((3, span_x, RIM, extent_z), f32),
            pltpu.VMEM((4, 3, HALO, RIM, extent_z), f32),
            pltpu.VMEM((2 * RECORD, total * CHUNK), f32),
            pltpu.SemaphoreType.DMA((copies,)),
            pltpu.SemaphoreType.DMA((copies,)),
        ]
        + [pltpu.VMEM(array.shape, array.dtype) for array in inputs]
        + [pltpu.SemaphoreType.DMA((len(inputs),))],
        compiler_params=pltpu.CompilerParams(
            collective_id=0, has_side_effects=True, vmem_limit_bytes=room
        ),
        name="front",
    )(*inputs)


def four(distance, weights):
    value = jnp.where(distance == 3.0, weights[3:4], 0.0)
    for n in (2, 1, 0):
        value = jnp.where(distance == float(n), weights[n : n + 1], value)
    return value


def first_kernel(span_y, placed, alive, high, low, frame, spread, right, left, tables, forces):
    def finish(j, record, got):
        forces[j, 0:1] = got[0]

    each_chunk(span_y, 1, 0, placed, alive, high, low, spread, tables, True, finish)
    for edge, first in ((right, high.shape[0] - 2 * HALO), (left, HALO)):
        pack_edge(edge, spread, first, 0, span_y)


def rest_kernel(
    spheres, span_y, placed, alive, high, low, frame, tables, forces, motion,
    spread, edges, tile, sums,
):
    lanes = len(DIRECTIONS)
    f32 = jnp.float32
    sums[...] = jnp.zeros(sums.shape, f32)

    def finish(j, record, got):
        o = [record[OFFSET + c : OFFSET + c + 1] for c in range(3)]
        f = [forces[j, 0:1]] + got
        moments = jnp.concatenate(
            f
            + [
                o[1] * f[2] - o[2] * f[1],
                o[2] * f[0] - o[0] * f[2],
                o[0] * f[1] - o[1] * f[0],
                jnp.zeros((2, CHUNK), f32),
            ],
            axis=0,
        )
        group = record[SPHERE : SPHERE + 1]
        for g in range((lanes + 1) * spheres):
            sums[g] = sums[g] + jnp.where(group == float(g), moments, 0.0)

    each_chunk(span_y, 2, 1, placed, alive, high, low, spread, tables, False, finish)
    columns = jnp.sum(sums[...], axis=2)
    tile[...] = jnp.zeros(tile.shape, f32)
    for s in range(spheres):
        for slot in range(lanes + 1):
            at = 6 * (slot * spheres + s)
            line = (lanes + 1) * s + slot
            tile[0:1, at : at + 6] = columns[line : line + 1, 0:6]
        at = 6 * ((lanes + 1) * spheres + s)
        tile[0:1, at : at + 6] = motion[s : s + 1]
    for side, first in enumerate((high.shape[0] - 2 * HALO, HALO)):
        for c in range(2):
            pack_edge(edges.at[side, c], spread, first, c, span_y)


def pack_edge(edge, spread, first, c, span_y):
    wide_y = span_y + 2 * ITERS
    reach = ITERS + HALO
    middle = span_y + 2 * HALO - 2 * reach
    low_rim = wide_y * c + HALO
    high_rim = wide_y * (c + 1) - HALO - reach
    for x in range(reach):
        done = 0
        for start, length in ((low_rim, reach), (high_rim, reach), (low_rim + reach, middle)):
            to = done + length * x
            edge[to : to + length] = spread[first + x, start : start + length]
            done += length * reach


def each_chunk(
    span_y, components, component, placed, alive_ref, high, low, spread, tables, build, finish
):
    layers, rows, extent_z = high.shape
    wide_y = span_y + 2 * ITERS
    lines_here = components * wide_y
    bf16, f32 = jnp.bfloat16, jnp.float32
    alive_count = jnp.max(alive_ref[0:1, :]).astype(jnp.int32)
    z_cells = lax.broadcasted_iota(jnp.int32, (extent_z, CHUNK), 0).astype(f32)
    y_cells = lax.broadcasted_iota(jnp.int32, (wide_y, CHUNK), 0).astype(f32) - HALO
    x_cells = lax.broadcasted_iota(jnp.int32, (WINDOW, CHUNK), 0).astype(f32)

    def x_table(record, fresh):
        base = jnp.minimum(fresh, layers - WINDOW)
        cells = x_cells + base.astype(f32)
        table = four(cells - record[X_ROW : X_ROW + 1], record[0:4])
        return base, jnp.where(cells >= fresh.astype(f32), table, 0.0)

    def sample(record, z_stack, fresh, total):
        base, table = x_table(record, fresh)
        first = high[pl.ds(base, WINDOW)].reshape(WINDOW * rows, extent_z)
        rest = low[pl.ds(base, WINDOW)].reshape(WINDOW * rows, extent_z)
        lines = jnp.dot(
            jnp.concatenate([first, rest, first], axis=1),
            z_stack,
            preferred_element_type=f32,
        )
        for x in range(WINDOW):
            part = lines[x * rows : x * rows + lines_here] * table[x : x + 1]
            total = part if total is None else total + part
        return total

    def deposit(record, z_wide, sheet, fresh):
        base, table = x_table(record, fresh)
        value = jnp.concatenate([sheet * table[x : x + 1] for x in range(WINDOW)], axis=0)
        first, rest = split(value)
        first = first.astype(bf16)
        rest = rest.astype(bf16)
        added = lax.dot_general(
            jnp.concatenate([first, rest, first], axis=1),
            z_wide,
            (((1,), (1,)), ((), ())),
            preferred_element_type=f32,
        )
        at = pl.ds(base + HALO, WINDOW)
        spread[at] = spread[at] + added.reshape(WINDOW, lines_here, extent_z)

    def several(step, carry):
        chunks = [step * TOGETHER + n for n in range(TOGETHER)]
        records = [placed[j] for j in chunks]
        high_z, low_z, y_tables, begins, windows, planes = [], [], [], [], [], []
        for j, record in zip(chunks, records):
            if build:
                distance = z_cells - record[Z_ROW : Z_ROW + 1]
                distance = jnp.where(distance < 0.0, distance + extent_z, distance)
                z_high, z_low = split(four(distance, record[8:12]))
                tables[j, 0] = z_high.astype(bf16)
                tables[j, 1] = z_low.astype(bf16)
            alive = record[LIVE : LIVE + 1] > 0.5
            cell_x = record[X_ROW : X_ROW + 1]
            least = jnp.min(jnp.where(alive, cell_x, 1e4)).astype(jnp.int32)
            most = jnp.max(jnp.where(alive, cell_x, -1.0)).astype(jnp.int32)
            begins.append(least)
            windows.append((most + 4 - least + WINDOW - 1) // WINDOW)
            y_tables.append(four(y_cells - record[Y_ROW : Y_ROW + 1], record[4:8]))

        def stack(j, axis):
            return jnp.concatenate([tables[j, 0], tables[j, 0], tables[j, 1]], axis=axis)

        for n, j in enumerate(chunks):
            planes.append(sample(records[n], stack(j, 0), begins[n], None))
        for n, j in enumerate(chunks):
            planes[n] = lax.fori_loop(
                1,
                windows[n],
                lambda k, total, n=n, j=j: sample(
                    placed[j], stack(j, 0), begins[n] + WINDOW * k, total
                ),
                planes[n],
            )
        sheets = []
        for n, j in enumerate(chunks):
            record = records[n]
            got = []
            for c in range(components):
                weighted = planes[n][c * wide_y : (c + 1) * wide_y] * y_tables[n]
                sampled = jnp.sum(weighted, axis=0, keepdims=True)
                line = TARGET + component + c
                got.append((record[line : line + 1] - sampled) * record[LIVE : LIVE + 1])
            sheets.append(jnp.concatenate([force * y_tables[n] for force in got], axis=0))
            finish(j, record, got)
        for n, j in enumerate(chunks):
            deposit(records[n], stack(j, 1), sheets[n], begins[n])
        for n, j in enumerate(chunks):

            @pl.when(windows[n] > 1)
            def _(n=n, j=j):
                def more(k, carry):
                    deposit(placed[j], stack(j, 1), sheets[n], begins[n] + WINDOW * k)
                    return carry

                lax.fori_loop(1, windows[n], more, 0)

        return carry

    steps = (alive_count + (CHUNK * TOGETHER - 1)) // (CHUNK * TOGETHER)
    lax.fori_loop(0, steps, several, 0)


def first_stage(span_y, placed, alive, high, low, frame):
    extent_z = frame.shape[2]
    f32 = jnp.float32
    edge = jax.ShapeDtypeStruct(((ITERS + HALO) * (span_y + 2 * HALO), extent_z), f32)
    vmem = pl.BlockSpec(memory_space=pltpu.VMEM)
    return pl.pallas_call(
        functools.partial(first_kernel, span_y),
        out_shape=[
            pltpu.VMEM(frame.shape, f32),
            edge,
            edge,
            pltpu.VMEM((placed.shape[0], 2, extent_z, CHUNK), jnp.bfloat16),
            pltpu.VMEM((placed.shape[0], 8, CHUNK), f32),
        ],
        in_specs=[vmem] * 5,
        out_specs=[vmem] * 5,
        input_output_aliases={4: 0},
        compiler_params=pltpu.CompilerParams(vmem_limit_bytes=36 * 2**20),
        cost_estimate=pl.CostEstimate(
            flops=10_000_000_000, bytes_accessed=4_000_000, transcendentals=0
        ),
        name="first",
    )(placed, alive, high, low, frame)


def rest_stage(spheres, span_y, placed, alive, high, low, frame, tables, forces, motion):
    extent_z = frame.shape[2]
    f32 = jnp.float32
    groups = (len(DIRECTIONS) + 1) * spheres
    vmem = pl.BlockSpec(memory_space=pltpu.VMEM)
    return pl.pallas_call(
        functools.partial(rest_kernel, spheres, span_y),
        out_shape=[
            pltpu.VMEM(frame.shape, f32),
            pltpu.VMEM((2, 2, (ITERS + HALO) * (span_y + 2 * HALO), extent_z), f32),
            jax.ShapeDtypeStruct((1, TILE_LANES), f32),
        ],
        in_specs=[vmem] * 8,
        out_specs=[vmem] * 3,
        scratch_shapes=[pltpu.VMEM((groups, 8, CHUNK), f32)],
        input_output_aliases={4: 0},
        compiler_params=pltpu.CompilerParams(vmem_limit_bytes=36 * 2**20),
        cost_estimate=pl.CostEstimate(
            flops=20_000_000_000, bytes_accessed=8_000_000, transcendentals=0
        ),
        name="rest",
    )(placed, alive, high, low, frame, tables, forces, motion)


def shift(array, step):
    size = lax.axis_size("gx")
    return lax.ppermute(array, "gx", [(i, (i + step) % size) for i in range(size)])


def combine_matrix(columns, rows, per_sphere):
    slots = len(DIRECTIONS) + 2
    matrix = np.zeros((slots, columns, rows, columns, rows), np.float32)
    for i in range(columns):
        for j in range(rows):
            for slot, (dx, dy) in enumerate(DIRECTIONS):
                if 0 <= j - dy < rows:
                    matrix[slot, (i - dx) % columns, j - dy, i, j] -= RESPONSE / per_sphere
            matrix[slots - 2, i, j, i, j] -= RESPONSE / per_sphere
            matrix[slots - 1, i, j, i, j] = 1.0
    return matrix.reshape(slots * columns * rows, -1)


def tail_kernel(
    columns, rows, frame_0, frame_1, got_left, got_right, edges, tile, matrix,
    contact_sphere, contact_partner, out, motion_out, from_left, from_right, from_below, from_above, corners, held,
    rhs, one, two, mask_ref, own_sem, send, recv, row_send, row_recv, col_send, col_recv,
):
    column = lax.axis_index("gx")
    row = lax.axis_index("gy")
    span_x, span_y, extent_z = out.shape[1:]
    wide_x, wide_y = span_x + 2 * ITERS, span_y + 2 * ITERS
    reach = ITERS + HALO
    depth = span_y + 2 * HALO
    row_peers = [lax.rem(row + k, rows) for k in range(1, rows)]
    column_peers = [lax.rem(column + k, columns) for k in range(1, columns)]
    barrier = pltpu.get_barrier_semaphore()
    for other in row_peers:
        pl.semaphore_signal(barrier, inc=1, device_id=(column, other), device_id_type=MESH)
    for other in column_peers:
        pl.semaphore_signal(barrier, inc=1, device_id=(other, row), device_id_type=MESH)
    own = pltpu.make_async_copy(tile, held.at[column, row], own_sem)
    own.start()

    def peer(dx, dy):
        return (lax.rem(column + dx + columns, columns), row + dy)

    edge = []
    rim = 2 * reach * reach
    part = corners.shape[2]

    def halo(c, side):
        if c == 0:
            return (got_left, got_right)[side]
        return (from_left, from_right)[side].at[c - 1]

    for c in range(3):
        frame = frame_1 if c else frame_0
        low = wide_y * max(c - 1, 0)
        high = low + wide_y
        inner = slice(HALO, wide_x - HALO)
        if c:
            edge += [
                (edges.at[0, c - 1, 0:rim], from_left.at[c - 1, 0:rim], 1, 0),
                (edges.at[1, c - 1, 0:rim], from_right.at[c - 1, 0:rim], -1, 0),
                (edges.at[0, c - 1, rim:], from_left.at[c - 1, rim:], 1, 0),
                (edges.at[1, c - 1, rim:], from_right.at[c - 1, rim:], -1, 0),
            ]
        else:
            edge += [None] * 4
        edge += [
            (frame.at[inner, high - RIM : high], from_below.at[c], 0, 1),
            (frame.at[inner, low : low + RIM], from_above.at[c], 0, -1),
            (halo(c, 0).at[rim - part : rim], corners.at[c, 0], 0, 1),
            (halo(c, 1).at[rim - part : rim], corners.at[c, 1], 0, 1),
            (halo(c, 0).at[0:part], corners.at[c, 2], 0, -1),
            (halo(c, 1).at[0:part], corners.at[c, 3], 0, -1),
        ]
    each = 10

    def start(k):
        src, dst, dx, dy = edge[k]
        when(
            exists(row, rows, dy),
            lambda: remote(src, dst, send, recv, k, peer(dx, dy)).start(),
        )

    def arrive(k):
        src, dst, dx, dy = edge[k]
        when(
            exists(row, rows, -dy),
            lambda: remote(src, dst, send, recv, k, peer(dx, dy)).wait_recv(),
        )

    def sent(k):
        src, dst, dx, dy = edge[k]
        when(
            exists(row, rows, dy),
            lambda: remote(src, dst, send, recv, k, peer(dx, dy)).wait_send(),
        )

    @pl.when(row == 0)
    def _():
        from_below[...] = jnp.zeros(from_below.shape, jnp.float32)
        for c in range(3):
            corners[c, 0:2] = jnp.zeros((2,) + corners.shape[2:], jnp.float32)

    @pl.when(row == rows - 1)
    def _():
        from_above[...] = jnp.zeros(from_above.shape, jnp.float32)
        for c in range(3):
            corners[c, 2:4] = jnp.zeros((2,) + corners.shape[2:], jnp.float32)

    pl.semaphore_wait(barrier, rows + columns - 2)
    first = [
        pltpu.make_async_remote_copy(
            src_ref=tile,
            dst_ref=held.at[column, row],
            send_sem=row_send.at[k],
            recv_sem=row_recv.at[k],
            device_id=(column, other),
            device_id_type=MESH,
        )
        for k, other in enumerate(row_peers)
    ]
    for copy in first:
        copy.start()
    for k in range(4):
        start(each + k)
    for c in range(3):
        for k in range(4, 6):
            start(each * c + k)
    for k in range(6, each):
        start(k)

    cells = lax.broadcasted_iota(jnp.int32, (wide_y, extent_z), 0) + (row * span_y - ITERS)
    inside = jnp.logical_and(cells >= 0, cells < span_y * rows)
    inverse = 1.0 / (1.0 + 6.0 * DIFFUSION)
    mask_ref[0] = inside.astype(jnp.float32)
    mask_ref[1] = inside.astype(jnp.float32) * inverse

    own.wait()
    for copy in first:
        copy.wait()
    second = [
        pltpu.make_async_remote_copy(
            src_ref=held.at[column],
            dst_ref=held.at[column],
            send_sem=col_send.at[k],
            recv_sem=col_recv.at[k],
            device_id=(other, row),
            device_id_type=MESH,
        )
        for k, other in enumerate(column_peers)
    ]
    for copy in second:
        copy.start()
    for k in range(4):
        start(2 * each + k)

    def relaxed(c, source, x):
        here = source[c, x]
        beside = source[c, x - 1] + source[c, x + 1]
        beside = beside + pltpu.roll(here, 1, 0) + pltpu.roll(here, wide_y - 1, 0)
        beside = beside + pltpu.roll(here, 1, 1) + pltpu.roll(here, extent_z - 1, 1)
        return (rhs[c, x] + DIFFUSION * beside) * mask_ref[1]

    buffers = (rhs, one, two, one)

    def sweeps(c, starts, length):
        for sweep in range(ITERS):
            source = buffers[sweep]
            for first, shift in starts:
                begin = first + sweep * shift
                for x in range(begin, begin + length(sweep)):
                    new = relaxed(c, source, x)
                    if sweep == ITERS - 1:
                        out[c, x - ITERS] = new[ITERS : ITERS + span_y]
                    else:
                        buffers[sweep + 1][c, x] = new

    def base(c, load):
        for x in range(wide_x):
            rhs[c, x] = load(x)
        for x in range(wide_x - 2 * HALO):
            y = x + HALO
            rhs[c, y, 0:RIM] = rhs[c, y, 0:RIM] + from_below[c, x]
            rhs[c, y, wide_y - RIM :] = rhs[c, y, wide_y - RIM :] + from_above[c, x]
        for x in range(reach, wide_x - reach):
            rhs[c, x] = rhs[c, x] * mask_ref[0]
        sweeps(c, ((reach + 1, 1),), lambda sweep: span_x - 2 * HALO - 2 - 2 * sweep)

    def later(c, carry):
        base(c, lambda x: frame_1[x, pl.ds(pl.multiple_of(wide_y * (c - 1), 8), wide_y)])
        return carry

    for c in range(3):
        arrive(each * c + 4)
        arrive(each * c + 5)
    base(0, lambda x: frame_0[x])
    lax.fori_loop(1, 3, later, 0)

    middle = depth - 2 * reach
    upper = wide_y - HALO - reach

    def outer(c):
        for x in range(reach):
            for side, y in enumerate((x, x + span_x + HALO)):
                got = halo(c, side)
                low = slice(reach * x, reach * (x + 1))
                high = slice(reach * (reach + x), reach * (reach + x + 1))
                late = slice(part - rim // 2 + reach * x, part - rim // 2 + reach * (x + 1))
                inside = slice(rim + middle * x, rim + middle * (x + 1))
                rhs[c, y, HALO : HALO + reach] = rhs[c, y, HALO : HALO + reach] + got[low]
                rhs[c, y, upper : upper + reach] = rhs[c, y, upper : upper + reach] + got[high]
                rhs[c, y, HALO + reach : upper] = rhs[c, y, HALO + reach : upper] + got[inside]
                rhs[c, y, 0:reach] = rhs[c, y, 0:reach] + corners[c, side, late]
                rhs[c, y, wide_y - reach :] = rhs[c, y, wide_y - reach :] + corners[c, 2 + side, low]
                rhs[c, y] = rhs[c, y] * mask_ref[0]
        sweeps(c, ((1, 1), (span_x + 1, -1)), lambda sweep: reach)

    def settle():
        for copy in second:
            copy.wait()
        gathered = held[...].reshape(-1, TILE_LANES)
        devices = columns * rows
        pieces = jnp.dot(
            matrix[...],
            gathered,
            precision=lax.Precision.HIGHEST,
            preferred_element_type=jnp.float32,
        )
        spheres = motion_out.shape[0]
        moved = 0.0
        for slot in range(len(DIRECTIONS) + 2):
            at = 6 * spheres * slot
            moved = moved + pieces[devices * slot : devices * (slot + 1), at : at + 6 * spheres]
        device = lax.broadcasted_iota(jnp.int32, (1, devices), 1)
        here = column * rows + row
        linked, owned = [], []
        for s in range(spheres):
            mine = here * spheres + s
            for other in range(spheres):
                own_row = (device * spheres + other == mine).astype(jnp.float32)
                line = own_row
                for k in range(contact_sphere.shape[0]):
                    acts = contact_sphere[k] == mine
                    partner = (device * spheres + other == contact_partner[k]).astype(jnp.float32)
                    line = line + jnp.where(acts, DASHPOT * (partner - own_row), 0.0)
                linked.append(line)
                owned.append(own_row)
        links = jnp.concatenate(linked + owned, axis=0)
        result = jnp.dot(
            links, moved, precision=lax.Precision.HIGHEST, preferred_element_type=jnp.float32
        )
        for s in range(spheres):
            for half in range(2):
                total = 0.0
                for other in range(spheres):
                    line = (half * spheres + s) * spheres + other
                    at = 6 * other + 3 * half
                    total = total + result[line : line + 1, at : at + 3]
                motion_out[s : s + 1, 3 * half : 3 * half + 3] = total

    for c in range(3):
        if c:
            arrive(each * c)
            arrive(each * c + 1)
            for k in range(6, each):
                start(each * c + k)
        if c == 2:
            settle()
        if c:
            arrive(each * c + 2)
            arrive(each * c + 3)
        for k in range(6, each):
            arrive(each * c + k)
        outer(c)

    for k in range(4, len(edge)):
        sent(k)


def tail(frames, got, edges, tile, matrix, contact_sphere, contact_partner, span_y, spheres):
    columns, rows = lax.axis_size("gx"), lax.axis_size("gy")
    wide_x, _, extent_z = frames[0].shape
    span_x = wide_x - 2 * ITERS
    wide_y = span_y + 2 * ITERS
    reach = ITERS + HALO
    f32 = jnp.float32
    vmem = pl.BlockSpec(memory_space=pltpu.VMEM)
    smem = pl.BlockSpec(memory_space=pltpu.SMEM)
    dma = pltpu.SemaphoreType.DMA
    corner = (3, 4, -(-reach * reach // 8) * 8, extent_z)
    frame = (3, wide_x, wide_y, extent_z)
    return pl.pallas_call(
        functools.partial(tail_kernel, columns, rows),
        out_shape=[
            pltpu.VMEM((3, span_x, span_y, extent_z), f32),
            jax.ShapeDtypeStruct((spheres, 6), f32),
        ],
        in_specs=[vmem] * 7 + [smem] * 2,
        out_specs=[vmem] * 2,
        scratch_shapes=[
            pltpu.VMEM(edges.shape[1:], f32),
            pltpu.VMEM(edges.shape[1:], f32),
            pltpu.VMEM((3, wide_x - 2 * HALO, RIM, extent_z), f32),
            pltpu.VMEM((3, wide_x - 2 * HALO, RIM, extent_z), f32),
            pltpu.VMEM(corner, f32),
            pltpu.VMEM((columns, rows) + tile.shape, f32),
            pltpu.VMEM(frame, f32),
            pltpu.VMEM(frame, f32),
            pltpu.VMEM(frame, f32),
            pltpu.VMEM((2, wide_y, extent_z), f32),
            dma,
            dma((30,)),
            dma((30,)),
            dma((rows - 1,)),
            dma((rows - 1,)),
            dma((columns - 1,)),
            dma((columns - 1,)),
        ],
        compiler_params=pltpu.CompilerParams(
            collective_id=1, has_side_effects=True, vmem_limit_bytes=36 * 2**20
        ),
        name="tail",
    )(*frames, *got, edges, tile, matrix, contact_sphere, contact_partner)


def on_device(
    velocity,
    owner_block,
    base_x,
    base_y,
    base_z,
    delta_weights,
    marker_offset,
    sphere_motion,
    contact_sphere,
    contact_partner,
):
    span_y = velocity.shape[2]
    markers = base_x.shape[0]
    spheres = sphere_motion.shape[1]
    bases = [base.reshape(1, markers) for base in (base_x, base_y, base_z)]
    owners = owner_block.reshape(1, markers)
    motion = sphere_motion.T
    placed, alive, high_0, low_0, frame_0, high_1, low_1, frame_1 = front(
        owners, bases, delta_weights, marker_offset, motion, velocity
    )
    frame_0, right, left, tables, forces = first_stage(
        span_y, placed, alive, high_0, low_0, frame_0
    )
    got = (shift(right, 1), shift(left, -1))
    frame_1, edges, tile = rest_stage(
        spheres, span_y, placed, alive, high_1, low_1, frame_1, tables, forces, motion
    )
    columns, rows = lax.axis_size("gx"), lax.axis_size("gy")
    matrix = jnp.asarray(combine_matrix(columns, rows, markers // spheres))
    state, moved = tail(
        (frame_0, frame_1), got, edges, tile, matrix, contact_sphere, contact_partner,
        span_y, spheres,
    )
    return state, moved.T


def solution(mesh):
    placed = (
        P(None, "gx", "gy", None),
        P(("gx", "gy"), None),
        P(("gx", "gy")),
        P(("gx", "gy")),
        P(("gx", "gy")),
        P(None, ("gx", "gy")),
        P(None, ("gx", "gy")),
        P(None, ("gx", "gy")),
        P(("gx", "gy")),
        P(("gx", "gy")),
    )
    return jax.shard_map(
        on_device,
        mesh=mesh,
        in_specs=placed,
        out_specs=(P(None, "gx", "gy", None), P(None, ("gx", "gy"))),
        check_vma=False,
    )
```

```python
import functools
import math

import jax
import jax.numpy as jnp
import numpy as np
from jax import lax
from jax.experimental import pallas as pl
from jax.experimental.pallas import tpu as pltpu
from jax.sharding import PartitionSpec as P

ITERS = 4
DIFFUSION = 1.0
RESPONSE = 0.5
DASHPOT = 0.1

MESH = pl.DeviceIdType.MESH
TILE_LANES = 128
CHUNK = 256
WINDOW = 6
TOGETHER = 4
GROUP = 6
RECORD = 24
X_ROW, Y_ROW, Z_ROW, TARGET, OFFSET, SPHERE, LIVE = 12, 13, 14, 15, 18, 21, 22
DIRECTIONS = ((-1, -1), (-1, 0), (-1, 1), (0, -1), (0, 1), (1, -1), (1, 0), (1, 1))
HALO = 2
RIM = 8


def when(condition, body):
    if condition is True:
        body()
    else:
        pl.when(condition)(body)


def exists(row, rows, dy):
    if dy == 0:
        return True
    return row + dy < rows if dy > 0 else row + dy >= 0


def greet(columns, rows, column, row):
    barrier = pltpu.get_barrier_semaphore()
    for dx, dy in DIRECTIONS:
        peer = (lax.rem(column + dx + columns, columns), row + dy)
        when(
            exists(row, rows, dy),
            lambda peer=peer: pl.semaphore_signal(
                barrier, inc=1, device_id=peer, device_id_type=MESH
            ),
        )
    return barrier


def greeted(rows, row):
    inner = lax.min(row, 1) + lax.min(rows - 1 - row, 1)
    return 2 + 3 * inner


def remote(src, dst, send, recv, k, peer):
    return pltpu.make_async_remote_copy(
        src_ref=src,
        dst_ref=dst,
        send_sem=send.at[k],
        recv_sem=recv.at[k],
        device_id=peer,
        device_id_type=MESH,
    )


def split(value):
    high = value.astype(jnp.bfloat16).astype(jnp.float32)
    return high, value - high


def upper_triangle():
    rows = lax.broadcasted_iota(jnp.int32, (CHUNK, CHUNK), 0)
    lanes = lax.broadcasted_iota(jnp.int32, (CHUNK, CHUNK), 1)
    return (rows <= lanes).astype(jnp.float32).astype(jnp.bfloat16)


def ranks(categories, count):
    rows = lax.broadcasted_iota(jnp.int32, (count, CHUNK), 0).astype(jnp.float32)
    hot = [(rows == block).astype(jnp.float32) for block in categories]
    stacked = jnp.concatenate(hot, axis=0).astype(jnp.bfloat16)
    inside = jnp.dot(stacked, upper_triangle(), preferred_element_type=jnp.float32)
    carry = jnp.zeros((count, 1), jnp.float32)
    upto = []
    for b in range(len(hot)):
        block = inside[b * count : (b + 1) * count]
        upto.append(block + carry)
        carry = carry + block[:, CHUNK - 1 : CHUNK]
    return hot, upto, carry


def place(parts, where_to, groups):
    group = jnp.floor(where_to * (1.0 / CHUNK))
    slot = where_to - group * CHUNK
    rows = lax.broadcasted_iota(jnp.int32, (CHUNK, where_to.shape[1]), 0).astype(jnp.float32)
    hot = (rows == slot).astype(jnp.float32).astype(jnp.bfloat16)
    masked = [parts * (group == g).astype(jnp.float32) for g in groups]
    masked = jnp.concatenate(masked, axis=0).astype(jnp.bfloat16)
    moved = lax.dot_general(
        masked, hot, (((1,), (1,)), ((), ())), preferred_element_type=jnp.float32
    )
    result = []
    for n in range(len(groups)):
        piece = moved[2 * RECORD * n : 2 * RECORD * (n + 1)]
        result.append(piece[:RECORD] + piece[RECORD:])
    return result


def front_kernel(
    columns, rows, *refs
):
    inputs, refs = refs[:8], refs[8:]
    staged, load = refs[-9:-1], refs[-1]
    loads = [
        pltpu.make_async_copy(src, dst, load.at[n])
        for n, (src, dst) in enumerate(zip(inputs, staged))
    ]
    for copy in loads:
        copy.start()
    front_body(columns, rows, loads, *staged, *refs[:-9])


def front_body(
    columns, rows, loads, owners, base_x, base_y, base_z, weights, offsets, motion, velocity,
    placed, alive, high_0, low_0, frame_0, high_1, low_1, frame_1,
    home, slots, arrived, left, right, below, above, corners, parts, send, recv,
):
    column = lax.axis_index("gx")
    row = lax.axis_index("gy")
    span_x, span_y, extent_z = velocity.shape[1:]
    wide_y = span_y + 2 * ITERS
    lanes = len(DIRECTIONS)
    f32, bf16 = jnp.float32, jnp.bfloat16
    barrier = greet(columns, rows, column, row)

    def peer(dx, dy):
        return (lax.rem(column + dx + columns, columns), row + dy)

    edge = [(slots.at[g], arrived.at[g], dx, dy) for g, (dx, dy) in enumerate(DIRECTIONS)]
    rims = (slice(0, RIM), slice(span_y - RIM, span_y))
    for at in rims + (slice(RIM, span_y - RIM),):
        edge.append((velocity.at[:, 0:HALO, at], right.at[:, :, at], -1, 0))
        edge.append((velocity.at[:, span_x - HALO : span_x, at], left.at[:, :, at], 1, 0))
    edge.append((velocity.at[:, :, rims[0]], above, 0, -1))
    edge.append((velocity.at[:, :, rims[1]], below, 0, 1))
    for side, halo in enumerate((left, right)):
        edge.append((halo.at[:, :, rims[0]], corners.at[2 + side], 0, -1))
        edge.append((halo.at[:, :, rims[1]], corners.at[side], 0, 1))

    def start(k):
        src, dst, dx, dy = edge[k]
        when(
            exists(row, rows, dy),
            lambda: remote(src, dst, send, recv, k, peer(dx, dy)).start(),
        )

    def arrive(k):
        src, dst, dx, dy = edge[k]
        when(
            exists(row, rows, -dy),
            lambda: remote(src, dst, send, recv, k, peer(dx, dy)).wait_recv(),
        )

    def sent(k):
        src, dst, dx, dy = edge[k]
        when(
            exists(row, rows, dy),
            lambda: remote(src, dst, send, recv, k, peer(dx, dy)).wait_send(),
        )

    @pl.when(row == 0)
    def _():
        below[...] = jnp.zeros(below.shape, f32)
        for n in (0, 1):
            corners[n] = jnp.zeros(corners.shape[1:], f32)
        for g, (dx, dy) in enumerate(DIRECTIONS):
            if dy > 0:
                arrived[g] = jnp.zeros(arrived.shape[1:], f32)

    @pl.when(row == rows - 1)
    def _():
        above[...] = jnp.zeros(above.shape, f32)
        for n in (2, 3):
            corners[n] = jnp.zeros(corners.shape[1:], f32)
        for g, (dx, dy) in enumerate(DIRECTIONS):
            if dy < 0:
                arrived[g] = jnp.zeros(arrived.shape[1:], f32)

    for copy in loads[:7]:
        copy.wait()
    markers = owners.shape[1]
    spheres = motion.shape[0]
    per_sphere = markers // spheres
    owner = owners[...].astype(f32)
    owner_x = jnp.floor((owner + 0.5) * (1.0 / rows))
    owner_y = owner - owner_x * rows
    step_x = owner_x - column.astype(f32)
    step_x = jnp.where(step_x > 1.5, step_x - columns, step_x)
    step_x = jnp.where(step_x < -1.5, step_x + columns, step_x)
    step_y = owner_y - row.astype(f32)
    lane = (step_x + 1.0) * 3.0 + step_y + 1.0
    at_home = lane == 4.0
    lane = jnp.where(at_home, -1.0, jnp.where(lane > 4.0, lane - 1.0, lane))
    offset = offsets[...]
    targets = []
    for s in range(spheres):
        o = offset[:, s * per_sphere : (s + 1) * per_sphere]
        m = [motion[s : s + 1, c : c + 1] for c in range(6)]
        targets.append(
            jnp.concatenate(
                [
                    m[0] + (m[4] * o[2:3] - m[5] * o[1:2]),
                    m[1] + (m[5] * o[0:1] - m[3] * o[2:3]),
                    m[2] + (m[3] * o[1:2] - m[4] * o[0:1]),
                ],
                axis=0,
            )
        )
    home[0:12] = weights[...]
    for line, base in ((X_ROW, base_x), (Y_ROW, base_y), (Z_ROW, base_z)):
        home[line : line + 1] = base[...].astype(f32)
    home[TARGET : TARGET + 3] = jnp.concatenate(targets, axis=1)
    home[OFFSET : OFFSET + 3] = offset
    position = lax.broadcasted_iota(jnp.int32, (1, markers), 1)
    sphere = jnp.zeros((1, markers), f32)
    for s in range(1, spheres):
        sphere = sphere + (position >= s * per_sphere).astype(f32)
    home[SPHERE : SPHERE + 1] = sphere
    home[LIVE : LIVE + 1] = jnp.ones((1, markers), f32)
    home[LIVE + 1 : LIVE + 2] = jnp.zeros((1, markers), f32)

    blocks = markers // CHUNK
    hot, upto, totals = ranks([lane[:, b * CHUNK : (b + 1) * CHUNK] for b in range(blocks)], lanes)
    rank = [jnp.sum(h * (u - 1.0), axis=0, keepdims=True) for h, u in zip(hot, upto)]
    where_to = jnp.concatenate(rank, axis=1) + lane * CHUNK
    where_to = jnp.where(at_home, -1.0, where_to)
    pair = jnp.concatenate(split(home[...]), axis=0)
    for g, piece in enumerate(place(pair, where_to, range(lanes))):
        slots[g] = piece
    home[LIVE : LIVE + 1] = at_home.astype(f32)

    loads[7].wait()
    pl.semaphore_wait(barrier, greeted(rows, row))
    for k in range(len(edge) - 4):
        start(k)

    for k in range(lanes):
        arrive(k)
    total = blocks + lanes
    count = -(-(span_x + 1) // 8) * 8
    categories = []
    living = []
    for b in range(total):
        at = slice(b * CHUNK, (b + 1) * CHUNK)
        if b < blocks:
            record = home[:, at]
            group = lanes + record[SPHERE : SPHERE + 1] * (lanes + 1)
        else:
            record = arrived[b - blocks]
            group = (b - blocks) + record[SPHERE : SPHERE + 1] * (lanes + 1)
        lives = record[LIVE : LIVE + 1] > 0.5
        living.append(lives)
        categories.append(jnp.where(lives, record[X_ROW : X_ROW + 1], -1.0))
        first, rest = split(record)
        parts[0:RECORD, at] = first
        parts[RECORD : 2 * RECORD, at] = rest
        parts[SPHERE : SPHERE + 1, at] = group
    hot, upto, totals = ranks(categories, count)
    lower_rows = lax.broadcasted_iota(jnp.int32, (count, count), 0)
    lower_lanes = lax.broadcasted_iota(jnp.int32, (count, count), 1)
    before = (lower_lanes < lower_rows).astype(f32)
    wide = jnp.broadcast_to(totals, (count, TILE_LANES))
    starts = jnp.dot(
        before, wide, precision=lax.Precision.HIGHEST, preferred_element_type=f32
    )[:, 0:1]
    places = []
    for b in range(total):
        rank = jnp.sum(hot[b] * (upto[b] + (starts - 1.0)), axis=0, keepdims=True)
        places.append(jnp.where(living[b], rank, -1.0))
    where_to = jnp.concatenate(places, axis=1)
    alive[...] = jnp.broadcast_to(jnp.sum(wide, axis=0, keepdims=True), alive.shape)
    for first in range(0, total, GROUP):
        groups = range(first, min(first + GROUP, total))
        for g, piece in zip(groups, place(parts[...], where_to, groups)):
            placed[g] = piece

    def layer(x, row_source, below_source, above_source, own):
        for c in range(3):
            lines = row_source(c)
            margin = jnp.zeros((HALO, extent_z), f32)
            value = jnp.concatenate(
                [
                    margin,
                    below_source(c)[RIM - HALO : RIM],
                    lines,
                    above_source(c)[0:HALO],
                    margin,
                ],
                axis=0,
            )
            high, low, frame = (high_0, low_0, frame_0) if c == 0 else (high_1, low_1, frame_1)
            begin = 0 if c == 0 else wide_y * (c - 1)
            at = slice(begin, begin + wide_y)
            first, rest = split(value)
            high[x, at] = first.astype(bf16)
            low[x, at] = rest.astype(bf16)
            if own:
                margin = jnp.zeros((ITERS, extent_z), f32)
                frame[x + HALO, at] = jnp.concatenate([margin, lines, margin], axis=0)
        for ref, used in ((high_0, 1), (low_0, 1), (high_1, 2), (low_1, 2)):
            used = used * wide_y
            if ref.shape[1] > used:
                ref[x, used:] = jnp.zeros((ref.shape[1] - used, extent_z), bf16)

    arrive(len(edge) - 6)
    arrive(len(edge) - 5)

    def inner(x, carry):
        layer(
            x + HALO,
            lambda c: velocity[c, x],
            lambda c: below[c, x],
            lambda c: above[c, x],
            True,
        )
        return carry

    for k in range(lanes, lanes + 4):
        arrive(k)
    for k in range(len(edge) - 4, len(edge)):
        start(k)
    lax.fori_loop(0, span_x, inner, 0)
    for x in range(ITERS):
        for frame in (frame_0, frame_1):
            frame[x] = jnp.zeros(frame.shape[1:], f32)
            frame[span_x + ITERS + x] = jnp.zeros(frame.shape[1:], f32)
    arrive(lanes + 4)
    arrive(lanes + 5)
    for k in range(len(edge) - 4, len(edge)):
        arrive(k)
    for side, halo in enumerate((left, right)):
        for x in range(HALO):
            layer(
                x + side * (span_x + HALO),
                lambda c: halo[c, x],
                lambda c: corners[side, c, x],
                lambda c: corners[2 + side, c, x],
                False,
            )
    for k in range(len(edge)):
        sent(k)


def front(owners, bases, weights, offsets, motion, velocity):
    columns, rows = lax.axis_size("gx"), lax.axis_size("gy")
    span_x, span_y, extent_z = velocity.shape[1:]
    wide_y = span_y + 2 * ITERS
    markers = owners.shape[1]
    lanes = len(DIRECTIONS)
    f32, bf16 = jnp.float32, jnp.bfloat16
    copies = lanes + 12
    inputs = (owners, *bases, weights, offsets, motion, velocity)
    total = markers // CHUNK + lanes
    vmem = pl.BlockSpec(memory_space=pltpu.VMEM)
    out = [
        pltpu.VMEM((total, RECORD, CHUNK), f32),
        pltpu.VMEM((8, TILE_LANES), f32),
    ]
    for lines in (wide_y, 2 * wide_y):
        field = (span_x + 2 * HALO, -(-lines // 16) * 16, extent_z)
        out += [pltpu.VMEM(field, bf16), pltpu.VMEM(field, bf16)]
        out.append(pltpu.VMEM((span_x + 2 * ITERS, lines, extent_z), f32))
    room = 67_043_328 - sum(math.prod(ref.shape) * ref.dtype.itemsize for ref in out) - 2**15
    return pl.pallas_call(
        functools.partial(front_kernel, columns, rows),
        out_shape=out,
        in_specs=[pl.BlockSpec(memory_space=pltpu.HBM)] * 8,
        out_specs=[vmem] * len(out),
        scratch_shapes=[
            pltpu.VMEM((RECORD, markers), f32),
            pltpu.VMEM((lanes, RECORD, CHUNK), f32),
            pltpu.VMEM((lanes, RECORD, CHUNK), f32),
            pltpu.VMEM((3, HALO, span_y, extent_z), f32),
            pltpu.VMEM((3, HALO, span_y, extent_z), f32),
            pltpu.VMEM((3, span_x, RIM, extent_z), f32),
            pltpu.VMEM((3, span_x, RIM, extent_z), f32),
            pltpu.VMEM((4, 3, HALO, RIM, extent_z), f32),
            pltpu.VMEM((2 * RECORD, total * CHUNK), f32),
            pltpu.SemaphoreType.DMA((copies,)),
            pltpu.SemaphoreType.DMA((copies,)),
        ]
        + [pltpu.VMEM(array.shape, array.dtype) for array in inputs]
        + [pltpu.SemaphoreType.DMA((len(inputs),))],
        compiler_params=pltpu.CompilerParams(
            collective_id=0, has_side_effects=True, vmem_limit_bytes=room
        ),
        name="front",
    )(*inputs)


def four(distance, weights):
    value = jnp.where(distance == 3.0, weights[3:4], 0.0)
    for n in (2, 1, 0):
        value = jnp.where(distance == float(n), weights[n : n + 1], value)
    return value


def first_kernel(span_y, placed, alive, high, low, frame, spread, right, left, tables, forces):
    def finish(j, record, got):
        forces[j, 0:1] = got[0]

    each_chunk(span_y, 1, 0, placed, alive, high, low, spread, tables, True, finish)
    for edge, first in ((right, high.shape[0] - 2 * HALO), (left, HALO)):
        pack_edge(edge, spread, first, 0, span_y)


def rest_kernel(
    spheres, span_y, placed, alive, high, low, frame, tables, forces, motion,
    spread, edges, tile, sums,
):
    lanes = len(DIRECTIONS)
    f32 = jnp.float32
    sums[...] = jnp.zeros(sums.shape, f32)

    def finish(j, record, got):
        o = [record[OFFSET + c : OFFSET + c + 1] for c in range(3)]
        f = [forces[j, 0:1]] + got
        moments = jnp.concatenate(
            f
            + [
                o[1] * f[2] - o[2] * f[1],
                o[2] * f[0] - o[0] * f[2],
                o[0] * f[1] - o[1] * f[0],
                jnp.zeros((2, CHUNK), f32),
            ],
            axis=0,
        )
        group = record[SPHERE : SPHERE + 1]
        for g in range((lanes + 1) * spheres):
            sums[g] = sums[g] + jnp.where(group == float(g), moments, 0.0)

    each_chunk(span_y, 2, 1, placed, alive, high, low, spread, tables, False, finish)
    columns = jnp.sum(sums[...], axis=2)
    tile[...] = jnp.zeros(tile.shape, f32)
    for s in range(spheres):
        for slot in range(lanes + 1):
            at = 6 * (slot * spheres + s)
            line = (lanes + 1) * s + slot
            tile[0:1, at : at + 6] = columns[line : line + 1, 0:6]
        at = 6 * ((lanes + 1) * spheres + s)
        tile[0:1, at : at + 6] = motion[s : s + 1]
    for side, first in enumerate((high.shape[0] - 2 * HALO, HALO)):
        for c in range(2):
            pack_edge(edges.at[side, c], spread, first, c, span_y)


def pack_edge(edge, spread, first, c, span_y):
    wide_y = span_y + 2 * ITERS
    reach = ITERS + HALO
    middle = span_y + 2 * HALO - 2 * reach
    low_rim = wide_y * c + HALO
    high_rim = wide_y * (c + 1) - HALO - reach
    for x in range(reach):
        done = 0
        for start, length in ((low_rim, reach), (high_rim, reach), (low_rim + reach, middle)):
            to = done + length * x
            edge[to : to + length] = spread[first + x, start : start + length]
            done += length * reach


def each_chunk(
    span_y, components, component, placed, alive_ref, high, low, spread, tables, build, finish
):
    layers, rows, extent_z = high.shape
    wide_y = span_y + 2 * ITERS
    lines_here = components * wide_y
    bf16, f32 = jnp.bfloat16, jnp.float32
    alive_count = jnp.max(alive_ref[0:1, :]).astype(jnp.int32)
    z_cells = lax.broadcasted_iota(jnp.int32, (extent_z, CHUNK), 0).astype(f32)
    y_cells = lax.broadcasted_iota(jnp.int32, (wide_y, CHUNK), 0).astype(f32) - HALO
    x_cells = lax.broadcasted_iota(jnp.int32, (WINDOW, CHUNK), 0).astype(f32)

    def x_table(record, fresh):
        base = jnp.minimum(fresh, layers - WINDOW)
        cells = x_cells + base.astype(f32)
        table = four(cells - record[X_ROW : X_ROW + 1], record[0:4])
        return base, jnp.where(cells >= fresh.astype(f32), table, 0.0)

    def sample(record, z_stack, fresh, total):
        base, table = x_table(record, fresh)
        first = high[pl.ds(base, WINDOW)].reshape(WINDOW * rows, extent_z)
        rest = low[pl.ds(base, WINDOW)].reshape(WINDOW * rows, extent_z)
        lines = jnp.dot(
            jnp.concatenate([first, rest, first], axis=1),
            z_stack,
            preferred_element_type=f32,
        )
        for x in range(WINDOW):
            part = lines[x * rows : x * rows + lines_here] * table[x : x + 1]
            total = part if total is None else total + part
        return total

    def deposit(record, z_wide, sheet, fresh):
        base, table = x_table(record, fresh)
        value = jnp.concatenate([sheet * table[x : x + 1] for x in range(WINDOW)], axis=0)
        first, rest = split(value)
        first = first.astype(bf16)
        rest = rest.astype(bf16)
        added = lax.dot_general(
            jnp.concatenate([first, rest, first], axis=1),
            z_wide,
            (((1,), (1,)), ((), ())),
            preferred_element_type=f32,
        )
        at = pl.ds(base + HALO, WINDOW)
        spread[at] = spread[at] + added.reshape(WINDOW, lines_here, extent_z)

    def several(step, carry):
        chunks = [step * TOGETHER + n for n in range(TOGETHER)]
        records = [placed[j] for j in chunks]
        high_z, low_z, y_tables, begins, windows, planes = [], [], [], [], [], []
        for j, record in zip(chunks, records):
            if build:
                distance = z_cells - record[Z_ROW : Z_ROW + 1]
                distance = jnp.where(distance < 0.0, distance + extent_z, distance)
                z_high, z_low = split(four(distance, record[8:12]))
                tables[j, 0] = z_high.astype(bf16)
                tables[j, 1] = z_low.astype(bf16)
            alive = record[LIVE : LIVE + 1] > 0.5
            cell_x = record[X_ROW : X_ROW + 1]
            least = jnp.min(jnp.where(alive, cell_x, 1e4)).astype(jnp.int32)
            most = jnp.max(jnp.where(alive, cell_x, -1.0)).astype(jnp.int32)
            begins.append(least)
            windows.append((most + 4 - least + WINDOW - 1) // WINDOW)
            y_tables.append(four(y_cells - record[Y_ROW : Y_ROW + 1], record[4:8]))

        def stack(j, axis):
            return jnp.concatenate([tables[j, 0], tables[j, 0], tables[j, 1]], axis=axis)

        for n, j in enumerate(chunks):
            planes.append(sample(records[n], stack(j, 0), begins[n], None))
        for n, j in enumerate(chunks):
            planes[n] = lax.fori_loop(
                1,
                windows[n],
                lambda k, total, n=n, j=j: sample(
                    placed[j], stack(j, 0), begins[n] + WINDOW * k, total
                ),
                planes[n],
            )
        sheets = []
        for n, j in enumerate(chunks):
            record = records[n]
            got = []
            for c in range(components):
                weighted = planes[n][c * wide_y : (c + 1) * wide_y] * y_tables[n]
                sampled = jnp.sum(weighted, axis=0, keepdims=True)
                line = TARGET + component + c
                got.append((record[line : line + 1] - sampled) * record[LIVE : LIVE + 1])
            sheets.append(jnp.concatenate([force * y_tables[n] for force in got], axis=0))
            finish(j, record, got)
        for n, j in enumerate(chunks):
            deposit(records[n], stack(j, 1), sheets[n], begins[n])
        for n, j in enumerate(chunks):

            @pl.when(windows[n] > 1)
            def _(n=n, j=j):
                def more(k, carry):
                    deposit(placed[j], stack(j, 1), sheets[n], begins[n] + WINDOW * k)
                    return carry

                lax.fori_loop(1, windows[n], more, 0)

        return carry

    steps = (alive_count + (CHUNK * TOGETHER - 1)) // (CHUNK * TOGETHER)
    lax.fori_loop(0, steps, several, 0)


def first_stage(span_y, placed, alive, high, low, frame):
    extent_z = frame.shape[2]
    f32 = jnp.float32
    edge = jax.ShapeDtypeStruct(((ITERS + HALO) * (span_y + 2 * HALO), extent_z), f32)
    vmem = pl.BlockSpec(memory_space=pltpu.VMEM)
    return pl.pallas_call(
        functools.partial(first_kernel, span_y),
        out_shape=[
            pltpu.VMEM(frame.shape, f32),
            edge,
            edge,
            pltpu.VMEM((placed.shape[0], 2, extent_z, CHUNK), jnp.bfloat16),
            pltpu.VMEM((placed.shape[0], 8, CHUNK), f32),
        ],
        in_specs=[vmem] * 5,
        out_specs=[vmem] * 5,
        input_output_aliases={4: 0},
        compiler_params=pltpu.CompilerParams(vmem_limit_bytes=30 * 2**20),
        cost_estimate=pl.CostEstimate(
            flops=10_000_000_000, bytes_accessed=4_000_000, transcendentals=0
        ),
        name="first",
    )(placed, alive, high, low, frame)


def rest_stage(spheres, span_y, placed, alive, high, low, frame, tables, forces, motion):
    extent_z = frame.shape[2]
    f32 = jnp.float32
    groups = (len(DIRECTIONS) + 1) * spheres
    vmem = pl.BlockSpec(memory_space=pltpu.VMEM)
    return pl.pallas_call(
        functools.partial(rest_kernel, spheres, span_y),
        out_shape=[
            pltpu.VMEM(frame.shape, f32),
            pltpu.VMEM((2, 2, (ITERS + HALO) * (span_y + 2 * HALO), extent_z), f32),
            jax.ShapeDtypeStruct((1, TILE_LANES), f32),
        ],
        in_specs=[vmem] * 8,
        out_specs=[vmem] * 3,
        scratch_shapes=[pltpu.VMEM((groups, 8, CHUNK), f32)],
        input_output_aliases={4: 0},
        compiler_params=pltpu.CompilerParams(vmem_limit_bytes=30 * 2**20),
        cost_estimate=pl.CostEstimate(
            flops=20_000_000_000, bytes_accessed=8_000_000, transcendentals=0
        ),
        name="rest",
    )(placed, alive, high, low, frame, tables, forces, motion)


def shift(array, step):
    size = lax.axis_size("gx")
    return lax.ppermute(array, "gx", [(i, (i + step) % size) for i in range(size)])


def combine_matrix(columns, rows, per_sphere):
    slots = len(DIRECTIONS) + 2
    matrix = np.zeros((slots, columns, rows, columns, rows), np.float32)
    for i in range(columns):
        for j in range(rows):
            for slot, (dx, dy) in enumerate(DIRECTIONS):
                if 0 <= j - dy < rows:
                    matrix[slot, (i - dx) % columns, j - dy, i, j] -= RESPONSE / per_sphere
            matrix[slots - 2, i, j, i, j] -= RESPONSE / per_sphere
            matrix[slots - 1, i, j, i, j] = 1.0
    return matrix.reshape(slots * columns * rows, -1)


def tail_kernel(
    columns, rows, frame_0, frame_1, got_left, got_right, edges, tile, matrix,
    contact_sphere, contact_partner, out, motion_out, from_left, from_right, from_below, from_above, corners, held,
    rhs, one, two, mask_ref, own_sem, send, recv, row_send, row_recv, col_send, col_recv,
):
    column = lax.axis_index("gx")
    row = lax.axis_index("gy")
    span_x, span_y, extent_z = out.shape[1:]
    wide_x, wide_y = span_x + 2 * ITERS, span_y + 2 * ITERS
    reach = ITERS + HALO
    depth = span_y + 2 * HALO
    row_peers = [lax.rem(row + k, rows) for k in range(1, rows)]
    column_peers = [lax.rem(column + k, columns) for k in range(1, columns)]
    barrier = pltpu.get_barrier_semaphore()
    for other in row_peers:
        pl.semaphore_signal(barrier, inc=1, device_id=(column, other), device_id_type=MESH)
    for other in column_peers:
        pl.semaphore_signal(barrier, inc=1, device_id=(other, row), device_id_type=MESH)
    own = pltpu.make_async_copy(tile, held.at[column, row], own_sem)
    own.start()

    def peer(dx, dy):
        return (lax.rem(column + dx + columns, columns), row + dy)

    edge = []
    rim = 2 * reach * reach
    part = corners.shape[2]

    def halo(c, side):
        if c == 0:
            return (got_left, got_right)[side]
        return (from_left, from_right)[side].at[c - 1]

    for c in range(3):
        frame = frame_1 if c else frame_0
        low = wide_y * max(c - 1, 0)
        high = low + wide_y
        inner = slice(HALO, wide_x - HALO)
        if c:
            edge += [
                (edges.at[0, c - 1, 0:rim], from_left.at[c - 1, 0:rim], 1, 0),
                (edges.at[1, c - 1, 0:rim], from_right.at[c - 1, 0:rim], -1, 0),
                (edges.at[0, c - 1, rim:], from_left.at[c - 1, rim:], 1, 0),
                (edges.at[1, c - 1, rim:], from_right.at[c - 1, rim:], -1, 0),
            ]
        else:
            edge += [None] * 4
        edge += [
            (frame.at[inner, high - RIM : high], from_below.at[c], 0, 1),
            (frame.at[inner, low : low + RIM], from_above.at[c], 0, -1),
            (halo(c, 0).at[rim - part : rim], corners.at[c, 0], 0, 1),
            (halo(c, 1).at[rim - part : rim], corners.at[c, 1], 0, 1),
            (halo(c, 0).at[0:part], corners.at[c, 2], 0, -1),
            (halo(c, 1).at[0:part], corners.at[c, 3], 0, -1),
        ]
    each = 10

    def start(k):
        src, dst, dx, dy = edge[k]
        when(
            exists(row, rows, dy),
            lambda: remote(src, dst, send, recv, k, peer(dx, dy)).start(),
        )

    def arrive(k):
        src, dst, dx, dy = edge[k]
        when(
            exists(row, rows, -dy),
            lambda: remote(src, dst, send, recv, k, peer(dx, dy)).wait_recv(),
        )

    def sent(k):
        src, dst, dx, dy = edge[k]
        when(
            exists(row, rows, dy),
            lambda: remote(src, dst, send, recv, k, peer(dx, dy)).wait_send(),
        )

    @pl.when(row == 0)
    def _():
        from_below[...] = jnp.zeros(from_below.shape, jnp.float32)
        for c in range(3):
            corners[c, 0:2] = jnp.zeros((2,) + corners.shape[2:], jnp.float32)

    @pl.when(row == rows - 1)
    def _():
        from_above[...] = jnp.zeros(from_above.shape, jnp.float32)
        for c in range(3):
            corners[c, 2:4] = jnp.zeros((2,) + corners.shape[2:], jnp.float32)

    pl.semaphore_wait(barrier, rows + columns - 2)
    first = [
        pltpu.make_async_remote_copy(
            src_ref=tile,
            dst_ref=held.at[column, row],
            send_sem=row_send.at[k],
            recv_sem=row_recv.at[k],
            device_id=(column, other),
            device_id_type=MESH,
        )
        for k, other in enumerate(row_peers)
    ]
    for copy in first:
        copy.start()
    for k in range(4):
        start(each + k)
    for c in range(3):
        for k in range(4, 6):
            start(each * c + k)
    for k in range(6, each):
        start(k)

    cells = lax.broadcasted_iota(jnp.int32, (wide_y, extent_z), 0) + (row * span_y - ITERS)
    inside = jnp.logical_and(cells >= 0, cells < span_y * rows)
    inverse = 1.0 / (1.0 + 6.0 * DIFFUSION)
    mask_ref[0] = inside.astype(jnp.float32)
    mask_ref[1] = inside.astype(jnp.float32) * inverse

    own.wait()
    for copy in first:
        copy.wait()
    second = [
        pltpu.make_async_remote_copy(
            src_ref=held.at[column],
            dst_ref=held.at[column],
            send_sem=col_send.at[k],
            recv_sem=col_recv.at[k],
            device_id=(other, row),
            device_id_type=MESH,
        )
        for k, other in enumerate(column_peers)
    ]
    for copy in second:
        copy.start()
    for k in range(4):
        start(2 * each + k)

    def relaxed(c, source, x):
        here = source[c, x]
        beside = source[c, x - 1] + source[c, x + 1]
        beside = beside + pltpu.roll(here, 1, 0) + pltpu.roll(here, wide_y - 1, 0)
        beside = beside + pltpu.roll(here, 1, 1) + pltpu.roll(here, extent_z - 1, 1)
        return (rhs[c, x] + DIFFUSION * beside) * mask_ref[1]

    buffers = (rhs, one, two, one)

    def sweeps(c, starts, length):
        for sweep in range(ITERS):
            source = buffers[sweep]
            for first, shift in starts:
                begin = first + sweep * shift
                for x in range(begin, begin + length(sweep)):
                    new = relaxed(c, source, x)
                    if sweep == ITERS - 1:
                        out[c, x - ITERS] = new[ITERS : ITERS + span_y]
                    else:
                        buffers[sweep + 1][c, x] = new

    def base(c, load):
        for x in range(wide_x):
            rhs[c, x] = load(x)
        for x in range(wide_x - 2 * HALO):
            y = x + HALO
            rhs[c, y, 0:RIM] = rhs[c, y, 0:RIM] + from_below[c, x]
            rhs[c, y, wide_y - RIM :] = rhs[c, y, wide_y - RIM :] + from_above[c, x]
        for x in range(reach, wide_x - reach):
            rhs[c, x] = rhs[c, x] * mask_ref[0]
        sweeps(c, ((reach + 1, 1),), lambda sweep: span_x - 2 * HALO - 2 - 2 * sweep)

    def later(c, carry):
        base(c, lambda x: frame_1[x, pl.ds(pl.multiple_of(wide_y * (c - 1), 8), wide_y)])
        return carry

    for c in range(3):
        arrive(each * c + 4)
        arrive(each * c + 5)
    base(0, lambda x: frame_0[x])
    lax.fori_loop(1, 3, later, 0)

    middle = depth - 2 * reach
    upper = wide_y - HALO - reach

    def outer(c):
        for x in range(reach):
            for side, y in enumerate((x, x + span_x + HALO)):
                got = halo(c, side)
                low = slice(reach * x, reach * (x + 1))
                high = slice(reach * (reach + x), reach * (reach + x + 1))
                late = slice(part - rim // 2 + reach * x, part - rim // 2 + reach * (x + 1))
                inside = slice(rim + middle * x, rim + middle * (x + 1))
                rhs[c, y, HALO : HALO + reach] = rhs[c, y, HALO : HALO + reach] + got[low]
                rhs[c, y, upper : upper + reach] = rhs[c, y, upper : upper + reach] + got[high]
                rhs[c, y, HALO + reach : upper] = rhs[c, y, HALO + reach : upper] + got[inside]
                rhs[c, y, 0:reach] = rhs[c, y, 0:reach] + corners[c, side, late]
                rhs[c, y, wide_y - reach :] = rhs[c, y, wide_y - reach :] + corners[c, 2 + side, low]
                rhs[c, y] = rhs[c, y] * mask_ref[0]
        sweeps(c, ((1, 1), (span_x + 1, -1)), lambda sweep: reach)

    def settle():
        for copy in second:
            copy.wait()
        gathered = held[...].reshape(-1, TILE_LANES)
        devices = columns * rows
        pieces = jnp.dot(
            matrix[...],
            gathered,
            precision=lax.Precision.HIGHEST,
            preferred_element_type=jnp.float32,
        )
        spheres = motion_out.shape[0]
        moved = 0.0
        for slot in range(len(DIRECTIONS) + 2):
            at = 6 * spheres * slot
            moved = moved + pieces[devices * slot : devices * (slot + 1), at : at + 6 * spheres]
        device = lax.broadcasted_iota(jnp.int32, (1, devices), 1)
        here = column * rows + row
        linked, owned = [], []
        for s in range(spheres):
            mine = here * spheres + s
            for other in range(spheres):
                own_row = (device * spheres + other == mine).astype(jnp.float32)
                line = own_row
                for k in range(contact_sphere.shape[0]):
                    acts = contact_sphere[k] == mine
                    partner = (device * spheres + other == contact_partner[k]).astype(jnp.float32)
                    line = line + jnp.where(acts, DASHPOT * (partner - own_row), 0.0)
                linked.append(line)
                owned.append(own_row)
        links = jnp.concatenate(linked + owned, axis=0)
        result = jnp.dot(
            links, moved, precision=lax.Precision.HIGHEST, preferred_element_type=jnp.float32
        )
        for s in range(spheres):
            for half in range(2):
                total = 0.0
                for other in range(spheres):
                    line = (half * spheres + s) * spheres + other
                    at = 6 * other + 3 * half
                    total = total + result[line : line + 1, at : at + 3]
                motion_out[s : s + 1, 3 * half : 3 * half + 3] = total

    for c in range(3):
        if c:
            arrive(each * c)
            arrive(each * c + 1)
            for k in range(6, each):
                start(each * c + k)
        if c == 2:
            settle()
        if c:
            arrive(each * c + 2)
            arrive(each * c + 3)
        for k in range(6, each):
            arrive(each * c + k)
        outer(c)

    for k in range(4, len(edge)):
        sent(k)


def tail(frames, got, edges, tile, matrix, contact_sphere, contact_partner, span_y, spheres):
    columns, rows = lax.axis_size("gx"), lax.axis_size("gy")
    wide_x, _, extent_z = frames[0].shape
    span_x = wide_x - 2 * ITERS
    wide_y = span_y + 2 * ITERS
    reach = ITERS + HALO
    f32 = jnp.float32
    vmem = pl.BlockSpec(memory_space=pltpu.VMEM)
    smem = pl.BlockSpec(memory_space=pltpu.SMEM)
    dma = pltpu.SemaphoreType.DMA
    corner = (3, 4, -(-reach * reach // 8) * 8, extent_z)
    frame = (3, wide_x, wide_y, extent_z)
    return pl.pallas_call(
        functools.partial(tail_kernel, columns, rows),
        out_shape=[
            pltpu.VMEM((3, span_x, span_y, extent_z), f32),
            jax.ShapeDtypeStruct((spheres, 6), f32),
        ],
        in_specs=[vmem] * 7 + [smem] * 2,
        out_specs=[vmem] * 2,
        scratch_shapes=[
            pltpu.VMEM(edges.shape[1:], f32),
            pltpu.VMEM(edges.shape[1:], f32),
            pltpu.VMEM((3, wide_x - 2 * HALO, RIM, extent_z), f32),
            pltpu.VMEM((3, wide_x - 2 * HALO, RIM, extent_z), f32),
            pltpu.VMEM(corner, f32),
            pltpu.VMEM((columns, rows) + tile.shape, f32),
            pltpu.VMEM(frame, f32),
            pltpu.VMEM(frame, f32),
            pltpu.VMEM(frame, f32),
            pltpu.VMEM((2, wide_y, extent_z), f32),
            dma,
            dma((30,)),
            dma((30,)),
            dma((rows - 1,)),
            dma((rows - 1,)),
            dma((columns - 1,)),
            dma((columns - 1,)),
        ],
        compiler_params=pltpu.CompilerParams(
            collective_id=1, has_side_effects=True, vmem_limit_bytes=36 * 2**20
        ),
        name="tail",
    )(*frames, *got, edges, tile, matrix, contact_sphere, contact_partner)


def on_device(
    velocity,
    owner_block,
    base_x,
    base_y,
    base_z,
    delta_weights,
    marker_offset,
    sphere_motion,
    contact_sphere,
    contact_partner,
):
    span_y = velocity.shape[2]
    markers = base_x.shape[0]
    spheres = sphere_motion.shape[1]
    bases = [base.reshape(1, markers) for base in (base_x, base_y, base_z)]
    owners = owner_block.reshape(1, markers)
    motion = sphere_motion.T
    placed, alive, high_0, low_0, frame_0, high_1, low_1, frame_1 = front(
        owners, bases, delta_weights, marker_offset, motion, velocity
    )
    frame_0, right, left, tables, forces = first_stage(
        span_y, placed, alive, high_0, low_0, frame_0
    )
    got = (shift(right, 1), shift(left, -1))
    frame_1, edges, tile = rest_stage(
        spheres, span_y, placed, alive, high_1, low_1, frame_1, tables, forces, motion
    )
    columns, rows = lax.axis_size("gx"), lax.axis_size("gy")
    matrix = jnp.asarray(combine_matrix(columns, rows, markers // spheres))
    state, moved = tail(
        (frame_0, frame_1), got, edges, tile, matrix, contact_sphere, contact_partner,
        span_y, spheres,
    )
    return state, moved.T


def solution(mesh):
    placed = (
        P(None, "gx", "gy", None),
        P(("gx", "gy"), None),
        P(("gx", "gy")),
        P(("gx", "gy")),
        P(("gx", "gy")),
        P(None, ("gx", "gy")),
        P(None, ("gx", "gy")),
        P(None, ("gx", "gy")),
        P(("gx", "gy")),
        P(("gx", "gy")),
    )
    return jax.shard_map(
        on_device,
        mesh=mesh,
        in_specs=placed,
        out_specs=(P(None, "gx", "gy", None), P(None, ("gx", "gy"))),
        check_vma=False,
    )
```
